32 devices in a mesh: gx: 4 (over x, core), gy: 2 (over y), gz: 4 (over z).
Axes of the slice: x: 2, y: 2, z: 4, core: 2. Of those that a mesh axis runs over, the one named last changes fastest.
Arguments:
- opening_warmth_field: float32 [32, 32, 512], P('gx', 'gy', 'gz'), may hold values from -42 to 42
- cellwise_warming_source: float32 [32, 32, 512], P('gx', 'gy', 'gz'), may hold values from -6 to 6
- substance_category_per_voxel: int32 [32, 32, 512], P('gx', 'gy', 'gz'), may hold values from 0 to 15
- thermal_coefficient_table: float32 [16], replicated, may hold values from 0.2 to 5
- boundary_cooling_flags: int32 [32, 32, 512], P('gx', 'gy', 'gz'), may hold values 0 or 1
Outputs:
- closing_warmth_field: float32 [32, 32, 512], P('gx', 'gy', 'gz')
- remaining_mismatch: float32 [32, 32, 512], P('gx', 'gy', 'gz')
The draws below stay inside these ranges and needn't reach their ends.
All inputs are finite; a program needn't handle non-finite values. No bound on the sum of `boundary_cooling_flags` on one device may be relied on, other than what follows from the above.
Results may differ from the reference program's by a relative error of at most 0.00055.
Values sent between devices are 32-bit elements; how exact they have to be, the bound alone decides.
A program may use at most 64 MiB of HBM per device.

```python
import math
import jax
import jax.numpy as jnp
from jax import lax

ITERS = 4
TSTEPS = 1
CLASSES = 16
NX = 32
NY = 32
NZ = 512


def draw_opening_warmth_field(key, part):
    keys = jax.random.split(key, 1)
    ramp = (1.0 + 2.0 * jnp.arange(NX, dtype=jnp.float32) / (NX - 1))[:, None, None]
    values = jax.random.truncated_normal(keys[0], -5.0, 5.0, (NX, NY, NZ), jnp.float32) * ramp
    return values.astype(jnp.float32)


def place_ends(entries, key, least, top_value):
    longest = entries.shape.index(max(entries.shape))
    spots = []
    for shift in (0, 1):
        where = [jax.random.randint(jax.random.fold_in(key, axis), (), 0, length) for axis, length in enumerate(entries.shape)]
        where[longest] = (where[longest] + shift) % entries.shape[longest]
        spots.append(tuple(where))
    return entries.at[spots[0]].set(least).at[spots[1]].set(top_value)


def block_scale(stream_key, extent, cuts, least, high):
    def one(dim, blocks):
        draws = jax.random.uniform(jax.random.fold_in(jax.random.fold_in(stream_key, 6), dim), (blocks,), jnp.float32, least / len(cuts), high / len(cuts))
        return jnp.repeat(jnp.exp(draws), extent[dim] // blocks).reshape((-1,) + (1,) * (len(extent) - dim - 1))

    factor_of = one(*cuts[0])
    for cut in cuts[1:]:
        factor_of = factor_of * one(*cut)
    return factor_of


def normal_values(own_key, shape, scale, reach, cuts=(), held_as=jnp.bfloat16):
    loudness = block_scale(own_key, shape, cuts, -0.22, 0.18) if cuts else 1.0
    drawn = jax.random.normal(own_key, shape, jnp.float32) * scale * loudness
    return jnp.minimum(jnp.maximum(drawn, -reach), reach).astype(held_as)


def setup_inputs(seed: int = 0) -> dict:
    key_list = jax.random.split(jax.random.key(seed), 6)
    opening_warmth_field = draw_opening_warmth_field(jax.random.fold_in(key_list[5], 71), 0)
    cellwise_warming_source = normal_values(key_list[1], (NX, NY, NZ), 1.0, 6.0, ((0, 4), (1, 2), (2, 4)), jnp.float32)
    substance_category_per_voxel = place_ends(jax.random.randint(key_list[2], (NX, NY, NZ), 0, CLASSES), jax.random.fold_in(key_list[2], 1), 0, CLASSES - 1).astype(jnp.int32)
    thermal_coefficient_table = jnp.clip(jnp.exp(jax.random.uniform(key_list[3], (CLASSES,), jnp.float32, math.log(0.2), math.log(5.0))), 0.2, 5.0)
    boundary_cooling_flags = place_ends((jax.random.randint(key_list[4], (NX, NY, NZ), 0, 4) < 1).astype(jnp.int32), jax.random.fold_in(key_list[4], 1), 0, 1)
    return {"opening_warmth_field": opening_warmth_field, "cellwise_warming_source": cellwise_warming_source, "substance_category_per_voxel": substance_category_per_voxel, "thermal_coefficient_table": thermal_coefficient_table, "boundary_cooling_flags": boundary_cooling_flags}


interval_delta = 2.0
cooling = 3.0
kind_weights = (1.0, 0.5, 0.25)
kind_counts = (6.0, 12.0, 8.0)


def split_axis(values, axis):
    length = values.shape[axis] - 2
    center = lax.slice_in_dim(values, 1, length + 1, axis=axis)
    beside = lax.slice_in_dim(values, 0, length, axis=axis) + lax.slice_in_dim(values, 2, length + 2, axis=axis)
    return center, beside


def neighbor_sums(padded):
    leading_extent = padded.ndim - 3
    pieces = [(padded, 0)]
    for shift_vector in range(3):
        next_pieces = []
        for values, neighbors in pieces:
            center, beside = split_axis(values, leading_extent + shift_vector)
            next_pieces.append((center, neighbors))
            next_pieces.append((beside, neighbors + 1))
        pieces = next_pieces
    totals = [None, None, None]
    for values, neighbors in pieces:
        if neighbors > 0:
            if totals[neighbors - 1] is None:
                totals[neighbors - 1] = values
            else:
                totals[neighbors - 1] = totals[neighbors - 1] + values
    return totals


def coupling(padded, padded_flux, cond):
    field_sums = neighbor_sums(padded)
    accumulated_flux = neighbor_sums(padded_flux)
    computed_output = kind_weights[0] * (cond * field_sums[0] + accumulated_flux[0])
    computed_output = computed_output + kind_weights[1] * (cond * field_sums[1] + accumulated_flux[1])
    computed_output = computed_output + kind_weights[2] * (cond * field_sums[2] + accumulated_flux[2])
    return computed_output


def reference(opening_warmth_field, cellwise_warming_source, substance_category_per_voxel, thermal_coefficient_table, boundary_cooling_flags):
    cond = jnp.take(thermal_coefficient_table, substance_category_per_voxel)
    cond_sums = neighbor_sums(jnp.pad(cond, 1))
    spread = kind_weights[0] * (kind_counts[0] * cond + cond_sums[0])
    spread = spread + kind_weights[1] * (kind_counts[1] * cond + cond_sums[1])
    spread = spread + kind_weights[2] * (kind_counts[2] * cond + cond_sums[2])
    diagonal = 1.0 + interval_delta * cooling * boundary_cooling_flags.astype(jnp.float32) + 0.5 * interval_delta * spread

    def apply_stencil_matrix(field):
        padded = jnp.pad(field, 1)
        padded_flux = jnp.pad(cond * field, 1)
        return diagonal * field - 0.5 * interval_delta * coupling(padded, padded_flux, cond)

    closing_warmth_field = opening_warmth_field
    remaining_mismatch = opening_warmth_field
    for tstep in range(TSTEPS):
        forcing_term = closing_warmth_field + interval_delta * cellwise_warming_source
        remaining_mismatch = forcing_term - apply_stencil_matrix(closing_warmth_field)
        search_heading = remaining_mismatch
        norm_now = jnp.sum(remaining_mismatch * remaining_mismatch)
        for step in range(ITERS):
            image = apply_stencil_matrix(search_heading)
            descent_alpha = norm_now / jnp.sum(search_heading * image)
            closing_warmth_field = closing_warmth_field + descent_alpha * search_heading
            remaining_mismatch = remaining_mismatch - descent_alpha * image
            following_norm = jnp.sum(remaining_mismatch * remaining_mismatch)
            search_heading = remaining_mismatch + (following_norm / norm_now) * search_heading
            norm_now = following_norm
    return closing_warmth_field, remaining_mismatch
```

```python
import functools

import jax
import jax.numpy as jnp
from jax import lax
from jax.experimental import pallas as pl
from jax.experimental.pallas import tpu as pltpu
from jax.sharding import PartitionSpec as P

ITERS = 4
interval_delta = 2.0
cooling = 3.0

MESH = pl.DeviceIdType.MESH
AXES = ("gx", "gy", "gz")
SUB = 8
REACH = 4
LANES = 128
FIELDS = 4
DEPTH = ITERS + 1
SLOT = 2 * DEPTH
PER = LANES // (FIELDS * SLOT)
PAIRS = [(i, j) for i in range(ITERS + 1) for j in range(i, ITERS + 1) if i < ITERS]
WAYS = [(a, b, c) for a in (0, 1, -1) for b in (0, 1, -1) for c in (0, 1, -1) if a or b or c]


def smooth(values, axis):
    size = values.shape[axis]
    return (values + values) + (pltpu.roll(values, 1, axis) + pltpu.roll(values, size - 1, axis))


def smooth_all(before, center, after):
    return smooth(smooth(before + (center + center) + after, 0), 1)


def kernel(
    counts,
    warm_in,
    source_in,
    category_in,
    table_in,
    flags_in,
    both_out,
    pair,
    push_in,
    cool,
    basis,
    flux,
    warm_flux,
    diag,
    couple,
    table,
    table_row,
    source,
    ints,
    edges,
    beside,
    row_out,
    plane_rows,
    line_rows,
    all_rows,
    load_sems,
    halo_send,
    halo_recv,
    row_send,
    row_recv,
    near,
    far,
):
    plane, line = counts[0] * counts[1], counts[2]
    nx, ny, nz = both_out.shape[1:]
    depth = DEPTH
    wide, tall, long = pair.shape[1:]
    short = ny + SUB
    groups = edges.shape[0]
    ends = -(-depth // PER)
    last = (nx - depth) // PER
    direct = max(counts) <= REACH
    here = [lax.axis_index(a) for a in AXES]
    in_plane = here[0] * counts[1] + here[1]

    def exists(offset):
        good = None
        for k in range(3):
            if offset[k] > 0:
                one = here[k] < counts[k] - offset[k]
            elif offset[k] < 0:
                one = here[k] >= -offset[k]
            else:
                continue
            good = one if good is None else jnp.logical_and(good, one)
        return good

    def at(offset):
        return {a: here[k] + offset[k] for k, a in enumerate(AXES)}

    def back(offset):
        return tuple(-o for o in offset)

    def signal(semaphore, offset):
        @pl.when(exists(offset))
        def _():
            pl.semaphore_signal(semaphore, inc=1, device_id=at(offset), device_id_type=MESH)

    def present(offsets):
        return sum(jnp.where(exists(offset), 1, 0) for offset in offsets)

    plane_targets = [
        {"gx": other // counts[1], "gy": other % counts[1], "gz": here[2]}
        for other in [(in_plane + step) % plane for step in range(1, plane)]
    ]
    line_targets = [
        {"gx": here[0], "gy": here[1], "gz": (here[2] + step) % line} for step in range(1, line)
    ]
    moved_by = [[(here[k] + step) % counts[k] for step in range(counts[k])] for k in range(3)]
    all_targets = [
        {"gx": moved_by[0][a], "gy": moved_by[1][b], "gz": moved_by[2][c]}
        for c in reversed(range(counts[2]))
        for b in reversed(range(counts[1]))
        for a in reversed(range(counts[0]))
        if a or b or c
    ]

    barrier = pltpu.get_barrier_semaphore()
    ways = [w for w in WAYS if all(abs(w[k]) < counts[k] for k in range(3))]
    for way in reversed(ways):
        signal(barrier, way)
    if not direct:
        for target in plane_targets + line_targets:
            pl.semaphore_signal(barrier, inc=1, device_id=target, device_id_type=MESH)

    own = (pl.ds(depth, nx), pl.ds(0, ny), pl.ds(0, nz))
    loads = [
        pltpu.make_async_copy(table_in, table_row, load_sems.at[4]),
        pltpu.make_async_copy(category_in, ints.at[0], load_sems.at[0]),
        pltpu.make_async_copy(flags_in, ints.at[1], load_sems.at[1]),
        pltpu.make_async_copy(warm_in, pair.at[(0,) + own], load_sems.at[2]),
        pltpu.make_async_copy(source_in, source, load_sems.at[3]),
    ]
    for load in loads:
        load.start()

    def clear(ref, *index):
        shape = ref.at[index].shape
        ref[index] = jnp.zeros(shape, jnp.float32)

    table[...] = jnp.zeros(table.shape, jnp.float32)
    body = slice(0, nz)
    for way, planes, slots in (
        ((-1, 0, 0), slice(0, depth), slice(0, ends)),
        ((1, 0, 0), slice(depth + nx, wide), slice(ends + groups, None)),
    ):

        @pl.when(jnp.logical_not(exists(way)))
        def _():
            for f in range(2):
                clear(pair, f, planes, slice(None), body)
            clear(push_in, planes, slice(None), body)
            clear(cool, planes, slice(None), body)
            for side in range(2):
                clear(beside, side, slots, slice(None), slice(None))

    for way, rows, few in (
        ((0, 1, 0), slice(ny, ny + SUB), slice(ny, ny + SUB // 2)),
        ((0, -1, 0), slice(tall - SUB, tall), slice(short - SUB // 2, short)),
    ):

        @pl.when(jnp.logical_not(exists(way)))
        def _():
            for f in range(2):
                clear(pair, f, slice(None), rows, body)
            clear(push_in, slice(None), few, body)
            clear(cool, slice(None), few, body)
            for side in range(2):
                clear(beside, side, slice(None), rows, slice(None))

    for side, way in enumerate(((0, 0, -1), (0, 0, 1))):

        @pl.when(jnp.logical_not(exists(way)))
        def _():
            clear(beside, side, slice(None), slice(None), slice(None))

    for load in loads:
        load.wait()

    table[0:1, 0 : table_in.shape[1]] = table_row[...]
    lookup = jnp.broadcast_to(table[0:1, :], (ny, LANES))
    lane = lax.broadcasted_iota(jnp.int32, (ny, LANES), 1)
    for start in range(0, nx, PER):
        packed = None
        for i in range(start, min(start + PER, nx)):
            cond = jnp.take_along_axis(lookup, ints[0, i], axis=1)
            flag = ints[1, i].astype(jnp.float32)
            warm = pair[0, depth + i, 0:ny, 0:nz]
            push = interval_delta * source[i] - (interval_delta * cooling) * flag * warm
            pair[1, depth + i, 0:ny, 0:nz] = cond
            cool[depth + i, 0:ny, 0:nz] = flag
            push_in[depth + i, 0:ny, 0:nz] = push
            for f, piece in enumerate((warm, cond, push, flag)):
                q = (i - start) * FIELDS + f
                turned = pltpu.roll(piece, (q * SLOT + depth) % LANES, 1)
                packed = turned if packed is None else jnp.where(lane >= q * SLOT, turned, packed)
        edges[start // PER] = packed

    most = 7.0 + 24.0 * jnp.max(table[0:1, :], axis=1, keepdims=True)
    high, low = most, jnp.ones_like(most)
    middle = 0.5 * (high + low)
    half = 0.5 * (high - low)
    twice = 2.0 / half

    waits = present(back(w) for w in ways)
    if not direct:
        waits = waits + (plane + line - 2)
    pl.semaphore_wait(barrier, waits)

    def span(step, size, total, least, most):
        if step == 0:
            return pl.ds(least, size), pl.ds(least, size)
        if step > 0:
            return pl.ds(least + size - total, total), pl.ds(most - total, total)
        return pl.ds(least, total), pl.ds(least + size, total)

    def xspan(step, size, total):
        if step == 0:
            return pl.ds(depth, size), pl.ds(depth, size)
        if step > 0:
            return pl.ds(depth + size - total, total), pl.ds(depth - total, total)
        return pl.ds(depth, total), pl.ds(depth + size, total)

    halos = []

    def send(src, dst, way):
        k = len(halos)
        copy = pltpu.make_async_remote_copy(
            src_ref=src,
            dst_ref=dst,
            send_sem=halo_send.at[k],
            recv_sem=halo_recv.at[k],
            device_id=at(way),
            device_id_type=MESH,
        )
        pl.when(exists(way))(copy.start)
        halos.append((copy, way))

    def send_edges(way):
        dx, dy, dz = way
        if dx == 0:
            src_x, dst_x = pl.ds(0, groups), pl.ds(ends, groups)
        elif dx > 0:
            src_x, dst_x = pl.ds(last, groups - last), pl.ds(0, groups - last)
        else:
            src_x, dst_x = pl.ds(0, ends), pl.ds(ends + groups, ends)
        src_y, dst_y = span(dy, ny, depth, 0, tall)
        send(edges.at[src_x, src_y], beside.at[0 if dz > 0 else 1, dst_x, dst_y], way)

    def send_fields(way):
        dx, dy = way[:2]
        z = pl.ds(0, nz)
        src_x, dst_x = xspan(dx, nx, depth)
        src_y, dst_y = span(dy, ny, depth, 0, tall)
        both = pl.ds(0, 2)
        send(pair.at[both, src_x, src_y, z], pair.at[both, dst_x, dst_y, z], way)
        for ref, less in ((push_in, 1), (cool, 2)):
            src_x, dst_x = xspan(dx, nx, depth - less)
            src_y, dst_y = span(dy, ny, depth - less, 0, short)
            send(ref.at[src_x, src_y, z], ref.at[dst_x, dst_y, z], way)

    for way in sorted(ways, key=lambda w: -sum(map(abs, w))):
        if way[2]:
            send_edges(way)
    for way in sorted(ways, key=lambda w: -sum(map(abs, w))):
        if not way[2]:
            send_fields(way)
    if direct:
        for way in ways:
            signal(near, way)
        hops = [(a, 0, c) for a in (0, 2, -2) for c in (0, 2, -2) if a or c]
        hops = [h for h in hops if abs(h[0]) < counts[0] and abs(h[2]) < counts[2]]
        pl.semaphore_wait(near, present(back(w) for w in ways))
        for hop in hops:
            signal(far, hop)

    def share(stage, rows_ref, slot, targets):
        for target in targets:
            pltpu.make_async_remote_copy(
                src_ref=row_out.at[stage],
                dst_ref=rows_ref.at[slot],
                send_sem=row_send.at[stage],
                recv_sem=row_recv.at[stage],
                device_id=target,
                device_id_type=MESH,
            ).start()

    def share_wait(stage, rows_ref, targets):
        if targets:
            whole = pltpu.make_async_remote_copy(
                src_ref=rows_ref.at[pl.ds(0, len(targets))],
                dst_ref=rows_ref.at[pl.ds(0, len(targets))],
                send_sem=row_send.at[stage],
                recv_sem=row_recv.at[stage],
                device_id=targets[0],
                device_id_type=MESH,
            )
            whole.wait_send()
            whole.wait_recv()

    for copy, way in halos:
        pl.when(exists(back(way)))(copy.wait_recv)

    first_half = lax.broadcasted_iota(jnp.int32, (SUB, LANES), 0) < SUB // 2
    all_lanes = lax.broadcasted_iota(jnp.int32, (tall, LANES), 1)
    left_side = all_lanes % SLOT < depth

    def narrow(v):
        mask = jnp.concatenate([first_half] * (v.shape[1] // LANES), axis=1)
        join = jnp.where(mask, v[ny : ny + SUB], v[ny + SUB :])
        return jnp.concatenate([v[:ny], join], axis=0)

    regions = [(0, ends, 0, depth, nx - depth - last * PER)]
    regions += [(ends, groups, depth, nx, 0), (ends + groups, ends, depth + nx, depth, 0)]
    for first_group, some, first_plane, planes, skip in regions:
        for g in range(some):
            merged = jnp.where(left_side, beside[0, first_group + g], beside[1, first_group + g])
            thin = narrow(merged)
            for s in range(PER):
                j = g * PER + s - skip
                if not 0 <= j < planes:
                    continue
                i = first_plane + j
                shifts = [-((s * FIELDS + f) * SLOT + depth) % LANES for f in range(FIELDS)]
                for f in range(2):
                    pair[f, i, :, nz:] = pltpu.roll(merged, shifts[f], 1)
                if 1 <= i < wide - 1:
                    push_in[i, :, nz:] = pltpu.roll(thin, shifts[2], 1)
                if 2 <= i < wide - 2:
                    cool[i, :, nz:] = pltpu.roll(thin, shifts[3], 1)
                warm_flux[i] = pair[0, i] * pair[1, i]

    def valid(index, size, cut, k):
        inner = index < size
        right = jnp.logical_and(index < size + cut, here[k] < counts[k] - 1)
        left = jnp.logical_and(index >= size + cut, here[k] > 0)
        return jnp.logical_or(inner, jnp.logical_or(right, left))

    def inside_of(rows, cut):
        y_index = lax.broadcasted_iota(jnp.int32, (rows, long), 0)
        z_index = lax.broadcasted_iota(jnp.int32, (rows, long), 1)
        both = jnp.logical_and(valid(y_index, ny, cut, 1), valid(z_index, nz, LANES // 2, 2))
        return jnp.where(both, 1.0, 0.0)

    x_left = jnp.where(here[0] > 0, 1.0, 0.0)
    x_right = jnp.where(here[0] < counts[0] - 1, 1.0, 0.0)

    def x_inside(i):
        return jnp.where(i < depth, x_left, jnp.where(i >= depth + nx, x_right, 1.0))

    quarter = 0.125 * interval_delta
    within = inside_of(short, SUB // 2)
    inside = quarter * within
    several = next(u for u in (4, 2) if (wide - 2) % u == 0)

    @pl.loop(0, (wide - 2) // several)
    def _(group):
        for u in range(several):
            i = 1 + several * group + u
            cond = narrow(pair[1, i])
            warm = narrow(pair[0, i])
            ring = narrow(smooth_all(pair[1, i - 1], pair[1, i], pair[1, i + 1]))
            near_warm = narrow(smooth_all(pair[0, i - 1], pair[0, i], pair[0, i + 1]))
            push = narrow(smooth_all(warm_flux[i - 1], warm_flux[i], warm_flux[i + 1]))
            spread = 8.0 * interval_delta * cond + quarter * ring
            image = spread * warm - (quarter * cond * near_warm + x_inside(i) * inside * push)
            left = push_in[i] - image
            edge = (quarter * twice) * cond
            basis[0, i] = left
            diag[i] = twice * (spread + (1.0 - middle) + interval_delta * cooling * cool[i])
            couple[i] = edge
            flux[0, i] = edge * left
    for k in range(ITERS):

        half_planes = wide // 2 - 2 - k

        @pl.loop(0, 2)
        def _(group):
            for u in range(half_planes):
                i = 2 + k + half_planes * group + u
                edge = couple[i]
                mid = basis[k, i]
                own = smooth_all(basis[k, i - 1], mid, basis[k, i + 1])
                push = smooth_all(flux[k % 2, i - 1], flux[k % 2, i], flux[k % 2, i + 1])
                fresh = diag[i] * mid - (edge * own + x_inside(i) * within * push)
                if k > 0:
                    fresh = fresh - basis[k - 1, i]
                basis[k + 1, i] = fresh
                if k + 1 < ITERS:
                    flux[(k + 1) % 2, i] = edge * fresh

    sums = [None] * len(PAIRS)
    for i in range(depth, depth + nx):
        rows = [basis[k, i, 0:ny, 0:nz] for k in range(ITERS + 1)]
        for n, (a, b) in enumerate(PAIRS):
            term = rows[a] * rows[b]
            sums[n] = term if sums[n] is None else sums[n] + term
    diagonal = lax.broadcasted_iota(jnp.int32, (SUB, LANES), 0)
    across = lax.broadcasted_iota(jnp.int32, (SUB, LANES), 1)
    row = jnp.zeros((SUB, LANES), jnp.float32)
    for start in range(0, len(PAIRS), SUB):
        tile = jnp.zeros((SUB, LANES), jnp.float32)
        for n in range(start, min(start + SUB, len(PAIRS))):
            tile = jnp.where(diagonal == n - start, jnp.sum(sums[n], axis=0, keepdims=True), tile)
        column = jnp.sum(tile, axis=1, keepdims=True)
        row = row + jnp.where(across == diagonal + start, column, 0.0)
    row = jnp.sum(row, axis=0, keepdims=True)
    row_out[0] = row
    if direct:
        pl.semaphore_wait(far, present(back(h) for h in hops))
        mine = in_plane * line + here[2]
        all_rows[mine] = row
        share(0, all_rows, mine, all_targets)
        share_wait(0, all_rows, all_targets)
        row = jnp.sum(all_rows[...], axis=0)
    else:
        plane_rows[in_plane] = row
        share(0, plane_rows, in_plane, plane_targets)
        share_wait(0, plane_rows, plane_targets)
        row = jnp.sum(plane_rows[...], axis=0)
        row_out[1] = row
        line_rows[here[2]] = row
        share(1, line_rows, here[2], line_targets)
        share_wait(1, line_rows, line_targets)
        row = jnp.sum(line_rows[...], axis=0)
    row_lane = lax.broadcasted_iota(jnp.int32, (1, LANES), 1)
    pick = lambda v, i: jnp.sum(jnp.where(row_lane == i, v, 0.0), axis=1, keepdims=True)
    gram = {}
    for n, (a, b) in enumerate(PAIRS):
        gram[a, b] = gram[b, a] = pick(row, n)

    def apply(p):
        q = [middle * a for a in p] + [jnp.zeros_like(half)]
        for i, a in enumerate(p):
            q[i + 1] = q[i + 1] + (0.5 * half) * a
            if i > 0:
                q[i - 1] = q[i - 1] + (0.5 * half) * a
        return q

    def product(p, q):
        value = None
        for i, a in enumerate(p):
            inner = None
            for j, b in enumerate(q):
                term = gram[i, j] * b
                inner = term if inner is None else inner + term
            inner = a * inner
            value = inner if value is None else value + inner
        return value

    left = [jnp.ones_like(half)]
    heading = list(left)
    moved = []
    norm = product(left, left)
    for step in range(ITERS):
        image = apply(heading)
        alpha = norm / product(heading, image)
        moved = [a + alpha * b for a, b in zip(moved, heading)] + [
            alpha * b for b in heading[len(moved) :]
        ]
        left = [a - alpha * b for a, b in zip(left, image)] + [
            -alpha * b for b in image[len(left) :]
        ]
        if step + 1 < ITERS:
            following = product(left, left)
            ratio = following / norm
            heading = [a + ratio * b for a, b in zip(left, heading)] + left[len(heading) :]
            norm = following

    for i in range(nx):
        warm = pair[0, depth + i, 0:ny, 0:nz]
        end = jnp.zeros_like(warm)
        for k in range(ITERS + 1):
            value = basis[k, depth + i, 0:ny, 0:nz]
            if k < ITERS:
                warm = warm + moved[k] * value
            end = end + left[k] * value
        both_out[0, i] = warm
        both_out[1, i] = end

    for copy, way in halos:
        pl.when(exists(way))(copy.wait_send)


def body(counts, warm, source, category, table, flags):
    nx, ny, nz = warm.shape
    depth = DEPTH
    groups, ends = -(-nx // PER), -(-depth // PER)
    copies = 8 * 3 + 18
    plane, line = counts[0] * counts[1], counts[2]
    if nx < depth or nx % 2 or ny % SUB or nz != LANES or table.shape[0] > LANES:
        raise ValueError("block shape")
    if groups - (nx - depth) // PER != ends:
        raise ValueError("block shape")
    wide, tall, short, long = nx + 2 * depth, ny + 2 * SUB, ny + SUB, nz + LANES
    table = table[None]
    any_spec = pl.BlockSpec(memory_space=pl.ANY)
    vmem = pl.BlockSpec(memory_space=pltpu.VMEM)
    f32 = jnp.float32
    both = pl.pallas_call(
        functools.partial(kernel, counts),
        out_shape=pltpu.VMEM((2,) + warm.shape, jnp.float32),
        in_specs=[any_spec] * 5,
        out_specs=vmem,
        scratch_shapes=[
            pltpu.VMEM((2, wide, tall, long), f32),
            pltpu.VMEM((wide, short, long), f32),
            pltpu.VMEM((wide, short, long), f32),
            pltpu.VMEM((ITERS + 1, wide, short, long), f32),
            pltpu.VMEM((2, wide, short, long), f32),
            pltpu.VMEM((wide, tall, long), f32),
            pltpu.VMEM((wide, short, long), f32),
            pltpu.VMEM((wide, short, long), f32),
            pltpu.VMEM((SUB, LANES), f32),
            pltpu.VMEM(table.shape, f32),
            pltpu.VMEM((nx, ny, nz), f32),
            pltpu.VMEM((2, nx, ny, nz), jnp.int32),
            pltpu.VMEM((groups, ny, nz), f32),
            pltpu.VMEM((2, groups + 2 * ends, tall, nz), f32),
            pltpu.VMEM((2, 1, LANES), f32),
            pltpu.VMEM((plane, 1, LANES), f32),
            pltpu.VMEM((line, 1, LANES), f32),
            pltpu.VMEM((plane * line, 1, LANES), f32),
            pltpu.SemaphoreType.DMA((5,)),
            pltpu.SemaphoreType.DMA((copies,)),
            pltpu.SemaphoreType.DMA((copies,)),
            pltpu.SemaphoreType.DMA((2,)),
            pltpu.SemaphoreType.DMA((2,)),
            pltpu.SemaphoreType.REGULAR,
            pltpu.SemaphoreType.REGULAR,
        ],
        compiler_params=pltpu.CompilerParams(collective_id=0, has_side_effects=True),
    )(warm, source, category, table, flags)
    return both[0], both[1]


def solution(mesh):
    counts = tuple(mesh.shape[a] for a in AXES)
    spec = P("gx", "gy", "gz")
    return jax.shard_map(
        functools.partial(body, counts),
        mesh=mesh,
        in_specs=(spec, spec, spec, P(), spec),
        out_specs=(spec, spec),
        check_vma=False,
    )
```

```python
import functools

import jax
import jax.numpy as jnp
from jax import lax
from jax.experimental import pallas as pl
from jax.experimental.pallas import tpu as pltpu
from jax.sharding import PartitionSpec as P

ITERS = 4
interval_delta = 2.0
cooling = 3.0

MESH = pl.DeviceIdType.MESH
AXES = ("gx", "gy", "gz")
SUB = 8
REACH = 4
LANES = 128
FIELDS = 4
DEPTH = ITERS + 1
SLOT = 2 * DEPTH
PER = LANES // (FIELDS * SLOT)
MOMENTS = 2 * ITERS
REGIONS = [(a, c) for c in (0, 1, -1) for a in (0, 1, -1)]


def smooth_y(values):
    pairs = values + pltpu.roll(values, 1, 0)
    return pairs + pltpu.roll(pairs, values.shape[0] - 1, 0)


def smooth_z(values):
    size = values.shape[1]
    return (values + values) + (pltpu.roll(values, 1, 1) + pltpu.roll(values, size - 1, 1))


def smooth_z_own(values):
    size = values.shape[1] // 2
    main, side = values[:, :size], values[:, size:]
    lane = lax.broadcasted_iota(jnp.int32, main.shape, 1)
    before = pltpu.roll(jnp.where(lane == size - 1, side, main), 1, 1)
    after = pltpu.roll(jnp.where(lane == 0, side, main), size - 1, 1)
    return (main + main) + (before + after)


def kernel(
    counts,
    warm_in,
    source_in,
    category_in,
    table_in,
    flags_in,
    both_out,
    pair,
    push_in,
    cool,
    basis,
    flux,
    spread,
    diag,
    couple,
    masks,
    table,
    table_row,
    source,
    ints,
    edges,
    beside,
    ledger,
    row_out,
    plane_rows,
    line_rows,
    all_rows,
    load_sems,
    halo_send,
    halo_recv,
    row_send,
    row_recv,
    near,
    far,
):
    plane, line = counts[0] * counts[1], counts[2]
    nx, ny, nz = both_out.shape[1:]
    depth = DEPTH
    wide, tall, long = pair.shape[1:]
    short = ny + SUB
    groups = edges.shape[0]
    ends = -(-depth // PER)
    last = (nx - depth) // PER
    direct = max(counts) <= REACH
    here = [lax.axis_index(a) for a in AXES]
    in_plane = here[0] * counts[1] + here[1]

    def exists(offset):
        good = None
        for k in range(3):
            if offset[k] > 0:
                one = here[k] < counts[k] - offset[k]
            elif offset[k] < 0:
                one = here[k] >= -offset[k]
            else:
                continue
            good = one if good is None else jnp.logical_and(good, one)
        return good

    def at(offset):
        return {a: here[k] + offset[k] for k, a in enumerate(AXES)}

    def back(offset):
        return tuple(-o for o in offset)

    def signal(semaphore, offset):
        @pl.when(exists(offset))
        def _():
            pl.semaphore_signal(semaphore, inc=1, device_id=at(offset), device_id_type=MESH)

    def present(offsets):
        return sum(jnp.where(exists(offset), 1, 0) for offset in offsets)

    plane_targets = [
        {"gx": other // counts[1], "gy": other % counts[1], "gz": here[2]}
        for other in [(in_plane + step) % plane for step in range(1, plane)]
    ]
    line_targets = [
        {"gx": here[0], "gy": here[1], "gz": (here[2] + step) % line} for step in range(1, line)
    ]
    moved_by = [[(here[k] + step) % counts[k] for step in range(counts[k])] for k in range(3)]
    all_targets = [
        {"gx": moved_by[0][a], "gy": moved_by[1][b], "gz": moved_by[2][c]}
        for c in reversed(range(counts[2]))
        for b in reversed(range(counts[1]))
        for a in reversed(range(counts[0]))
        if a or b or c
    ]

    regions = [r for r in REGIONS if abs(r[0]) < counts[0] and abs(r[1]) < counts[2]]

    def by_class(act):
        if counts[1] == 1:
            act((0,))
            return
        pl.when(here[1] == 0)(lambda: act((0, 1)))
        pl.when(here[1] == counts[1] - 1)(lambda: act((0, -1)))
        if counts[1] > 2:
            inner = jnp.logical_and(here[1] > 0, here[1] < counts[1] - 1)
            pl.when(inner)(lambda: act((0, 1, -1)))

    def guard(region, act):
        if region == (0, 0):
            act()
        else:
            pl.when(exists((region[0], 0, region[1])))(act)

    def ways_of(region, steps):
        ways = [(region[0], step, region[1]) for step in sorted(steps, key=lambda v: -abs(v))]
        return [way for way in ways if any(way)]

    def neighbours():
        total = 0
        for region in regions:
            here_too = 1 if region == (0, 0) else jnp.where(exists((region[0], 0, region[1])), 1, 0)
            beside_y = present([(0, 1, 0), (0, -1, 0)]) if counts[1] > 1 else 0
            total = total + here_too * (beside_y + (0 if region == (0, 0) else 1))
        return total

    def signal_all(semaphore):
        def act(steps):
            for region in reversed(regions):

                def go(region=region):
                    for way in ways_of(region, steps):
                        pl.semaphore_signal(semaphore, inc=1, device_id=at(way), device_id_type=MESH)

                guard(region, go)

        by_class(act)

    own = (pl.ds(depth, nx), pl.ds(0, ny), pl.ds(0, nz))
    loads = [
        pltpu.make_async_copy(table_in, table_row, load_sems.at[0]),
        pltpu.make_async_copy(category_in, ints.at[0], load_sems.at[1]),
        pltpu.make_async_copy(flags_in, ints.at[1], load_sems.at[1]),
        pltpu.make_async_copy(warm_in, pair.at[(0,) + own], load_sems.at[1]),
        pltpu.make_async_copy(source_in, source, load_sems.at[1]),
    ]
    for load in loads:
        load.start()

    barrier = pltpu.get_barrier_semaphore()
    signal_all(barrier)
    if not direct:
        for target in plane_targets + line_targets:
            pl.semaphore_signal(barrier, inc=1, device_id=target, device_id_type=MESH)

    def clear(ref, *index):
        shape = ref.at[index].shape
        ref[index] = jnp.zeros(shape, jnp.float32)

    table[...] = jnp.zeros(table.shape, jnp.float32)
    body = slice(0, nz)
    for way, planes, slots in (
        ((-1, 0, 0), slice(0, depth), slice(0, ends)),
        ((1, 0, 0), slice(depth + nx, wide), slice(ends + groups, None)),
    ):

        @pl.when(jnp.logical_not(exists(way)))
        def _():
            for f in range(2):
                clear(pair, f, planes, slice(None), body)
            clear(push_in, planes, slice(None), body)
            clear(cool, planes, slice(None), body)
            for side in range(2):
                clear(beside, side, slots, slice(None), slice(None))

    for way, rows, few in (
        ((0, 1, 0), slice(ny, ny + SUB), slice(ny, ny + SUB // 2)),
        ((0, -1, 0), slice(tall - SUB, tall), slice(short - SUB // 2, short)),
    ):

        @pl.when(jnp.logical_not(exists(way)))
        def _():
            for f in range(2):
                clear(pair, f, slice(None), rows, body)
            clear(push_in, slice(None), few, body)
            clear(cool, slice(None), few, body)
            for side in range(2):
                clear(beside, side, slice(None), rows, slice(None))

    for side, way in enumerate(((0, 0, -1), (0, 0, 1))):

        @pl.when(jnp.logical_not(exists(way)))
        def _():
            clear(beside, side, slice(None), slice(None), slice(None))

    def valid(index, size, cut, k):
        inner = index < size
        right = jnp.logical_and(index < size + cut, here[k] < counts[k] - 1)
        left = jnp.logical_and(index >= size + cut, here[k] > 0)
        return jnp.logical_or(inner, jnp.logical_or(right, left))

    y_index = lax.broadcasted_iota(jnp.int32, (short, long), 0)
    z_index = lax.broadcasted_iota(jnp.int32, (short, long), 1)
    both_in = jnp.logical_and(valid(y_index, ny, SUB // 2, 1), valid(z_index, nz, LANES // 2, 2))
    within = jnp.where(both_in, 1.0, 0.0)
    masks[0] = jnp.where(here[0] > 0, 1.0, 0.0) * within
    masks[1] = within
    masks[2] = jnp.where(here[0] < counts[0] - 1, 1.0, 0.0) * within

    def inside(i):
        return masks[0 if i < depth else 2 if i >= depth + nx else 1]

    loads[0].wait()
    table[0:1, 0 : table_in.shape[1]] = table_row[...]
    most = 7.0 + 24.0 * jnp.max(table[0:1, :], axis=1, keepdims=True)
    high, low = most, jnp.ones_like(most)
    middle = 0.5 * (high + low)
    half = 0.5 * (high - low)
    twice = 2.0 / half
    quarter = 0.125 * interval_delta
    lookup = jnp.broadcast_to(table[0:1, :], (ny, LANES))
    lane = lax.broadcasted_iota(jnp.int32, (ny, LANES), 1)

    every = ledger.at[pl.ds(0, 4 * nx * ny)]
    pltpu.make_async_copy(every, every, load_sems.at[1]).wait()
    for start in range(0, nx, PER):
        packed = None
        for i in range(start, min(start + PER, nx)):
            cond = jnp.take_along_axis(lookup, ints[0, i], axis=1)
            flag = ints[1, i].astype(jnp.float32)
            warm = pair[0, depth + i, 0:ny, 0:nz]
            push = interval_delta * source[i] - (interval_delta * cooling) * flag * warm
            push = twice * push
            pair[1, depth + i, 0:ny, 0:nz] = cond
            cool[depth + i, 0:ny, 0:nz] = flag
            push_in[depth + i, 0:ny, 0:nz] = push
            for f, piece in enumerate((warm, cond, push, flag)):
                q = (i - start) * FIELDS + f
                turned = pltpu.roll(piece, (q * SLOT + depth) % LANES, 1)
                packed = turned if packed is None else jnp.where(lane >= q * SLOT, turned, packed)
        edges[start // PER] = packed

    waits = neighbours()
    if not direct:
        waits = waits + (plane + line - 2)
    pl.semaphore_wait(barrier, waits)

    def y_span(step, reach, full):
        if step == 0:
            return pl.ds(0, ny), pl.ds(0, ny)
        if step > 0:
            return pl.ds(ny - reach, reach), pl.ds(full - reach, reach)
        return pl.ds(0, reach), pl.ds(ny, reach)

    def x_span(step, reach):
        if step == 0:
            return pl.ds(depth, nx), pl.ds(depth, nx)
        if step > 0:
            return pl.ds(depth + nx - reach, reach), pl.ds(depth - reach, reach)
        return pl.ds(depth, reach), pl.ds(depth + nx, reach)

    def send(src, dst, way, stage):
        region = (way[0], way[2])
        pltpu.make_async_remote_copy(
            src_ref=src,
            dst_ref=dst,
            send_sem=halo_send.at[REGIONS.index(region)],
            recv_sem=halo_recv.at[stage + REGIONS.index((-way[0], -way[2]))],
            device_id=at(way),
            device_id_type=MESH,
        ).start()

    def send_field(view, way, reach, full, stage):
        src_x, dst_x = x_span(way[0], reach)
        src_y, dst_y = y_span(way[1], reach, full)
        z = pl.ds(0, nz)
        send(view(src_x, src_y, z), view(dst_x, dst_y, z), way, stage)

    def send_first(way):
        send_field(lambda *v: pair.at[(1,) + v], way, depth, tall, 0)
        send_field(lambda *v: cool.at[v], way, depth - 2, short, 0)

    def send_second(way):
        send_field(lambda *v: pair.at[(0,) + v], way, depth, tall, 9)
        send_field(lambda *v: push_in.at[v], way, depth - 1, short, 9)

    def send_edges(way):
        if way[0] == 0:
            src_x, dst_x = pl.ds(0, groups), pl.ds(ends, groups)
        elif way[0] > 0:
            src_x, dst_x = pl.ds(last, groups - last), pl.ds(0, groups - last)
        else:
            src_x, dst_x = pl.ds(0, ends), pl.ds(ends + groups, ends)
        src_y, dst_y = y_span(way[1], depth, tall)
        send(edges.at[src_x, src_y], beside.at[0 if way[2] > 0 else 1, dst_x, dst_y], way, 0)

    def send_all(steps):
        for z_side, action in ((False, send_first), (True, send_edges), (False, send_second)):
            for region in regions:
                if z_side == (region[1] != 0):

                    def go(region=region, action=action):
                        for way in ways_of(region, steps):
                            action(way)

                    guard(region, go)

    by_class(send_all)

    def x_rows(step, reach):
        return reach if step else nx

    def y_rows(step, reach):
        return reach if step else ny

    def moved_rows(way, kind):
        if kind == 2:
            return (ends if way[0] else groups) * y_rows(way[1], depth)
        reaches = ((depth, depth - 2), (depth, depth - 1))[kind]
        return sum(x_rows(way[0], r) * y_rows(way[1], r) for r in reaches)

    def region_wait(region, kinds, semaphore, receive):
        def wait(ways):
            rows = sum(moved_rows(way, kind) for way in ways for kind in kinds)
            if rows == 0:
                return
            whole = pltpu.make_async_remote_copy(
                src_ref=ledger.at[pl.ds(0, rows)],
                dst_ref=ledger.at[pl.ds(0, rows)],
                send_sem=semaphore,
                recv_sem=semaphore,
                device_id=all_targets[0],
                device_id_type=MESH,
            )
            if receive:
                whole.wait_recv()
            else:
                whole.wait_send()

        def go():
            wait(ways_of(region, (0,) if counts[1] == 1 else (0, 1)))
            if counts[1] > 2:
                inner = jnp.logical_and(here[1] > 0, here[1] < counts[1] - 1)
                pl.when(inner)(lambda: wait(ways_of((region[0], region[1]), (1,))))

        guard(region, go)

    def wait_halo(kind):
        for region in regions:
            if (kind == 2) == (region[1] != 0):
                stage = 9 if kind == 1 else 0
                region_wait(region, (kind,), halo_recv.at[stage + REGIONS.index(region)], True)

    if direct:
        signal_all(near)
        hops = [(a, 0, c) for a in (0, 2, -2) for c in (0, 2, -2) if a or c]
        hops = [h for h in hops if abs(h[0]) < counts[0] and abs(h[2]) < counts[2]]
        pl.semaphore_wait(near, neighbours())
        for hop in hops:
            signal(far, hop)

    def share(stage, rows_ref, slot, targets):
        for target in targets:
            pltpu.make_async_remote_copy(
                src_ref=row_out.at[stage],
                dst_ref=rows_ref.at[slot],
                send_sem=row_send.at[stage],
                recv_sem=row_recv.at[stage],
                device_id=target,
                device_id_type=MESH,
            ).start()

    def share_wait(stage, rows_ref, targets):
        if targets:
            whole = pltpu.make_async_remote_copy(
                src_ref=rows_ref.at[pl.ds(0, len(targets))],
                dst_ref=rows_ref.at[pl.ds(0, len(targets))],
                send_sem=row_send.at[stage],
                recv_sem=row_recv.at[stage],
                device_id=targets[0],
                device_id_type=MESH,
            )
            whole.wait_send()
            whole.wait_recv()

    wait_halo(0)
    wait_halo(2)

    first_half = lax.broadcasted_iota(jnp.int32, (SUB, LANES), 0) < SUB // 2
    left_side = lax.broadcasted_iota(jnp.int32, (tall, LANES), 1) % SLOT < depth

    def narrow(v):
        mask = jnp.concatenate([first_half] * (v.shape[1] // LANES), axis=1)
        join = jnp.where(mask, v[ny : ny + SUB], v[ny + SUB :])
        return jnp.concatenate([v[:ny], join], axis=0)

    spans = [(0, ends, 0, depth, nx - depth - last * PER)]
    spans += [(ends, groups, depth, nx, 0), (ends + groups, ends, depth + nx, depth, 0)]
    for first_group, some, first_plane, planes, skip in spans:
        for g in range(some):
            merged = jnp.where(left_side, beside[0, first_group + g], beside[1, first_group + g])
            thin = narrow(merged)
            for s in range(PER):
                j = g * PER + s - skip
                if not 0 <= j < planes:
                    continue
                i = first_plane + j
                shifts = [-((s * FIELDS + f) * SLOT + depth) % LANES for f in range(FIELDS)]
                for f in range(2):
                    pair[f, i, :, nz:] = pltpu.roll(merged, shifts[f], 1)
                if 1 <= i < wide - 1:
                    push_in[i, :, nz:] = pltpu.roll(thin, shifts[2], 1)
                if 2 <= i < wide - 2:
                    cool[i, :, nz:] = pltpu.roll(thin, shifts[3], 1)

    def along_x(least, most, planes_of, use):
        before = sums = None
        for i in range(least, most):
            now = planes_of(i)
            if i > least:
                joined = [a + b for a, b in zip(before, now)]
                if sums is not None:
                    use(i - 1, *[a + b for a, b in zip(sums, joined)])
                sums = joined
            before = now

    def ring_of(i):
        return (smooth_z(narrow(smooth_y(pair[1, i]))),)

    def use_ring(i, ring):
        cond = narrow(pair[1, i])
        base = twice * (8.0 * interval_delta * cond + quarter * ring)
        spread[i] = base
        couple[i] = (quarter * twice) * cond
        if 2 <= i < wide - 2:
            diag[i] = base + twice * ((1.0 - middle) + interval_delta * cooling * cool[i])

    along_x(0, wide, ring_of, use_ring)

    wait_halo(1)

    totals = [None] * MOMENTS

    def gather(n, a, b):
        part = a * b
        part = part[:SUB] + part[SUB:] if ny == 2 * SUB else sum(
            part[r : r + SUB] for r in range(0, ny, SUB)
        )
        totals[n] = part if totals[n] is None else totals[n] + part

    def core(v):
        return v[:ny, :nz]

    def warm_of(i):
        warm = pair[0, i]
        warm_flux = (quarter * twice) * (pair[1, i] * warm)
        return smooth_z(narrow(smooth_y(warm))), smooth_z(narrow(smooth_y(warm_flux)))

    def use_warm(i, ring, push):
        edge = couple[i]
        image = spread[i] * narrow(pair[0, i]) - (edge * ring + inside(i) * push)
        fresh = push_in[i] - image
        basis[0, i] = fresh
        flux[0, i] = edge * fresh
        if depth <= i < depth + nx:
            gather(0, core(fresh), core(fresh))

    along_x(0, wide, warm_of, use_warm)

    for k in range(ITERS - 1):

        def level_of(i, k=k):
            return smooth_z(smooth_y(basis[k, i])), smooth_z(smooth_y(flux[k % 2, i]))

        def use_level(i, ring, push, k=k):
            edge = couple[i]
            mid = basis[k, i]
            fresh = diag[i] * mid - (edge * ring + inside(i) * push)
            if k > 0:
                fresh = fresh - basis[k - 1, i]
            basis[k + 1, i] = fresh
            flux[(k + 1) % 2, i] = edge * fresh
            if depth <= i < depth + nx:
                gather(2 * k + 1, core(mid), core(fresh))
                gather(2 * k + 2, core(fresh), core(fresh))

        along_x(k + 1, wide - k - 1, level_of, use_level)

    k = ITERS - 1

    def last_of(i):
        return (
            smooth_z_own(smooth_y(basis[k, i])[:ny]),
            smooth_z_own(smooth_y(flux[k % 2, i])[:ny]),
        )

    def use_last(i, ring, push):
        mid = basis[k, i, 0:ny, 0:nz]
        fresh = diag[i, 0:ny, 0:nz] * mid - (couple[i, 0:ny, 0:nz] * ring + push)
        fresh = fresh - basis[k - 1, i, 0:ny, 0:nz]
        basis[k + 1, i, 0:ny, 0:nz] = fresh
        gather(2 * k + 1, mid, fresh)

    along_x(depth - 1, depth + nx + 1, last_of, use_last)

    diagonal = lax.broadcasted_iota(jnp.int32, (SUB, LANES), 0)
    across = lax.broadcasted_iota(jnp.int32, (SUB, LANES), 1)
    tile = jnp.zeros((SUB, LANES), jnp.float32)
    for n in range(MOMENTS):
        tile = jnp.where(diagonal == n, jnp.sum(totals[n], axis=0, keepdims=True), tile)
    column = jnp.sum(tile, axis=1, keepdims=True)
    row = jnp.sum(jnp.where(across == diagonal, column, 0.0), axis=0, keepdims=True)
    if direct:
        pl.semaphore_wait(far, present(back(h) for h in hops))
    row_out[0] = row

    def settle():
        for region in regions:
            kinds = (2,) if region[1] else (0, 1)
            region_wait(region, kinds, halo_send.at[REGIONS.index(region)], False)

    if direct:
        mine = in_plane * line + here[2]
        all_rows[mine] = row
        share(0, all_rows, mine, all_targets)
        settle()
        share_wait(0, all_rows, all_targets)
        row = jnp.sum(all_rows[...], axis=0)
    else:
        plane_rows[in_plane] = row
        share(0, plane_rows, in_plane, plane_targets)
        settle()
        share_wait(0, plane_rows, plane_targets)
        row = jnp.sum(plane_rows[...], axis=0)
        row_out[1] = row
        line_rows[here[2]] = row
        share(1, line_rows, here[2], line_targets)
        share_wait(1, line_rows, line_targets)
        row = jnp.sum(line_rows[...], axis=0)
    row_lane = lax.broadcasted_iota(jnp.int32, (1, LANES), 1)
    gram = {}
    for n in range(MOMENTS):
        value = jnp.sum(jnp.where(row_lane == n, row, 0.0), axis=1, keepdims=True)
        gram[n // 2, (n + 1) // 2] = value
    for gap in range(2, ITERS + 1):
        for i in range(ITERS + 1 - gap):
            j = i + gap
            value = gram[i + 1, j - 1] - gram[i, j - 2]
            if i > 0:
                value = value + gram[i - 1, j - 1]
            gram[i, j] = value
    for i, j in list(gram):
        gram[j, i] = gram[i, j]

    def apply(p):
        q = [middle * a for a in p] + [jnp.zeros_like(half)]
        for i, a in enumerate(p):
            q[i + 1] = q[i + 1] + (0.5 * half) * a
            if i > 0:
                q[i - 1] = q[i - 1] + (0.5 * half) * a
        return q

    def product(p, q):
        value = None
        for i, a in enumerate(p):
            inner = None
            for j, b in enumerate(q):
                term = gram[i, j] * b
                inner = term if inner is None else inner + term
            inner = a * inner
            value = inner if value is None else value + inner
        return value

    left = [0.5 * half]
    heading = list(left)
    moved = []
    norm = product(left, left)
    for step in range(ITERS):
        image = apply(heading)
        alpha = norm / product(heading, image)
        moved = [a + alpha * b for a, b in zip(moved, heading)] + [
            alpha * b for b in heading[len(moved) :]
        ]
        left = [a - alpha * b for a, b in zip(left, image)] + [
            -alpha * b for b in image[len(left) :]
        ]
        if step + 1 < ITERS:
            following = product(left, left)
            ratio = following / norm
            heading = [a + ratio * b for a, b in zip(left, heading)] + left[len(heading) :]
            norm = following

    for i in range(nx):
        warm = pair[0, depth + i, 0:ny, 0:nz]
        end = jnp.zeros_like(warm)
        for k in range(ITERS + 1):
            value = basis[k, depth + i, 0:ny, 0:nz]
            if k < ITERS:
                warm = warm + moved[k] * value
            end = end + left[k] * value
        both_out[0, i] = warm
        both_out[1, i] = end


def body(counts, warm, source, category, table, flags):
    nx, ny, nz = warm.shape
    depth = DEPTH
    groups, ends = -(-nx // PER), -(-depth // PER)
    plane, line = counts[0] * counts[1], counts[2]
    if nx < depth or nx % 2 or ny % SUB or nz != LANES or table.shape[0] > LANES:
        raise ValueError("block shape")
    if groups - (nx - depth) // PER != ends:
        raise ValueError("block shape")
    wide, tall, short, long = nx + 2 * depth, ny + 2 * SUB, ny + SUB, nz + LANES
    table = table[None]
    any_spec = pl.BlockSpec(memory_space=pl.ANY)
    vmem = pl.BlockSpec(memory_space=pltpu.VMEM)
    f32 = jnp.float32
    both = pl.pallas_call(
        functools.partial(kernel, counts),
        out_shape=pltpu.VMEM((2,) + warm.shape, jnp.float32),
        in_specs=[any_spec] * 5,
        out_specs=vmem,
        scratch_shapes=[
            pltpu.VMEM((2, wide, tall, long), f32),
            pltpu.VMEM((wide, short, long), f32),
            pltpu.VMEM((wide, short, long), f32),
            pltpu.VMEM((ITERS + 1, wide, short, long), f32),
            pltpu.VMEM((2, wide, short, long), f32),
            pltpu.VMEM((wide, short, long), f32),
            pltpu.VMEM((wide, short, long), f32),
            pltpu.VMEM((wide, short, long), f32),
            pltpu.VMEM((3, short, long), f32),
            pltpu.VMEM((SUB, LANES), f32),
            pltpu.VMEM(table.shape, f32),
            pltpu.VMEM((nx, ny, nz), f32),
            pltpu.VMEM((2, nx, ny, nz), jnp.int32),
            pltpu.VMEM((groups, ny, nz), f32),
            pltpu.VMEM((2, groups + 2 * ends, tall, nz), f32),
            pltpu.VMEM((4 * nx * ny, LANES), f32),
            pltpu.VMEM((2, 1, LANES), f32),
            pltpu.VMEM((plane, 1, LANES), f32),
            pltpu.VMEM((line, 1, LANES), f32),
            pltpu.VMEM((plane * line, 1, LANES), f32),
            pltpu.SemaphoreType.DMA((2,)),
            pltpu.SemaphoreType.DMA((9,)),
            pltpu.SemaphoreType.DMA((12,)),
            pltpu.SemaphoreType.DMA((2,)),
            pltpu.SemaphoreType.DMA((2,)),
            pltpu.SemaphoreType.REGULAR,
            pltpu.SemaphoreType.REGULAR,
        ],
        compiler_params=pltpu.CompilerParams(collective_id=0, has_side_effects=True),
    )(warm, source, category, table, flags)
    return both[0], both[1]


def solution(mesh):
    counts = tuple(mesh.shape[a] for a in AXES)
    spec = P("gx", "gy", "gz")
    return jax.shard_map(
        functools.partial(body, counts),
        mesh=mesh,
        in_specs=(spec, spec, spec, P(), spec),
        out_specs=(spec, spec),
        check_vma=False,
    )
```

```python
import functools

import jax
import jax.numpy as jnp
from jax import lax
from jax.experimental import pallas as pl
from jax.experimental.pallas import tpu as pltpu
from jax.sharding import PartitionSpec as P

ITERS = 4
interval_delta = 2.0
cooling = 3.0

MESH = pl.DeviceIdType.MESH
AXES = ("gx", "gy", "gz")
SUB = 8
REACH = 4
LANES = 128
FIELDS = 4
DEPTH = ITERS + 1
BOTH = 2
MOMENTS = 2 * ITERS
REGIONS = [(a, c) for c in (0, 1, -1) for a in (0, 1, -1)]


def smooth_y(values):
    pairs = values + pltpu.roll(values, 1, 0)
    return pairs + pltpu.roll(pairs, values.shape[0] - 1, 0)


def smooth_z(values):
    size = values.shape[1]
    return (values + values) + (pltpu.roll(values, 1, 1) + pltpu.roll(values, size - 1, 1))


def smooth_z_own(values):
    size = values.shape[1] // 2
    main, side = values[:, :size], values[:, size:]
    lane = lax.broadcasted_iota(jnp.int32, main.shape, 1)
    before = pltpu.roll(jnp.where(lane == size - 1, side, main), 1, 1)
    after = pltpu.roll(jnp.where(lane == 0, side, main), size - 1, 1)
    return (main + main) + (before + after)


def kernel(
    counts,
    warm_in,
    source_in,
    category_in,
    table_in,
    flags_in,
    both_out,
    pair,
    push_in,
    cool,
    basis,
    flux,
    spread,
    diag,
    couple,
    masks,
    table,
    table_row,
    source,
    ints,
    edges,
    beside,
    ledger,
    row_out,
    plane_rows,
    line_rows,
    all_rows,
    load_sems,
    halo_send,
    halo_recv,
    row_send,
    row_recv,
    near,
    far,
):
    plane, line = counts[0] * counts[1], counts[2]
    nx, ny, nz = both_out.shape[1:]
    depth = DEPTH
    wide, tall, long = pair.shape[1:]
    short = ny + SUB
    tail = nx - depth
    direct = max(counts) <= REACH
    here = [lax.axis_index(a) for a in AXES]
    in_plane = here[0] * counts[1] + here[1]

    def exists(offset):
        good = None
        for k in range(3):
            if offset[k] > 0:
                one = here[k] < counts[k] - offset[k]
            elif offset[k] < 0:
                one = here[k] >= -offset[k]
            else:
                continue
            good = one if good is None else jnp.logical_and(good, one)
        return good

    def at(offset):
        return {a: here[k] + offset[k] for k, a in enumerate(AXES)}

    def back(offset):
        return tuple(-o for o in offset)

    def signal(semaphore, offset):
        @pl.when(exists(offset))
        def _():
            pl.semaphore_signal(semaphore, inc=1, device_id=at(offset), device_id_type=MESH)

    def present(offsets):
        return sum(jnp.where(exists(offset), 1, 0) for offset in offsets)

    plane_targets = [
        {"gx": other // counts[1], "gy": other % counts[1], "gz": here[2]}
        for other in [(in_plane + step) % plane for step in range(1, plane)]
    ]
    line_targets = [
        {"gx": here[0], "gy": here[1], "gz": (here[2] + step) % line} for step in range(1, line)
    ]
    moved_by = [[(here[k] + step) % counts[k] for step in range(counts[k])] for k in range(3)]
    all_targets = [
        {"gx": moved_by[0][a], "gy": moved_by[1][b], "gz": moved_by[2][c]}
        for c in reversed(range(counts[2]))
        for b in reversed(range(counts[1]))
        for a in reversed(range(counts[0]))
        if a or b or c
    ]

    regions = [r for r in REGIONS if abs(r[0]) < counts[0] and abs(r[1]) < counts[2]]

    def by_class(act):
        if counts[1] == 1:
            act((0,))
            return
        pl.when(here[1] == 0)(lambda: act((0, 1)))
        pl.when(here[1] == counts[1] - 1)(lambda: act((0, -1)))
        if counts[1] > 2:
            inner = jnp.logical_and(here[1] > 0, here[1] < counts[1] - 1)
            pl.when(inner)(lambda: act((0, 1, -1)))

    def guard(region, act):
        if region == (0, 0):
            act()
        else:
            pl.when(exists((region[0], 0, region[1])))(act)

    def ways_of(region, steps):
        ways = [(region[0], step, region[1]) for step in sorted(steps, key=lambda v: -abs(v))]
        return [way for way in ways if any(way)]

    def neighbours():
        total = 0
        for region in regions:
            here_too = 1 if region == (0, 0) else jnp.where(exists((region[0], 0, region[1])), 1, 0)
            beside_y = present([(0, 1, 0), (0, -1, 0)]) if counts[1] > 1 else 0
            total = total + here_too * (beside_y + (0 if region == (0, 0) else 1))
        return total

    def signal_all(semaphore):
        def act(steps):
            for region in reversed(regions):

                def go(region=region):
                    for way in ways_of(region, steps):
                        pl.semaphore_signal(semaphore, inc=1, device_id=at(way), device_id_type=MESH)

                guard(region, go)

        by_class(act)

    own = (pl.ds(depth, nx), pl.ds(0, ny), pl.ds(0, nz))
    loads = [
        pltpu.make_async_copy(table_in, table_row, load_sems.at[0]),
        pltpu.make_async_copy(category_in, ints.at[0], load_sems.at[1]),
        pltpu.make_async_copy(flags_in, ints.at[1], load_sems.at[1]),
        pltpu.make_async_copy(warm_in, pair.at[(0,) + own], load_sems.at[1]),
        pltpu.make_async_copy(source_in, source, load_sems.at[1]),
    ]
    for load in loads:
        load.start()

    barrier = pltpu.get_barrier_semaphore()
    signal_all(barrier)
    if not direct:
        for target in plane_targets + line_targets:
            pl.semaphore_signal(barrier, inc=1, device_id=target, device_id_type=MESH)

    def clear(ref, *index):
        shape = ref.at[index].shape
        ref[index] = jnp.zeros(shape, jnp.float32)

    table[...] = jnp.zeros(table.shape, jnp.float32)
    body = slice(0, nz)
    for way, planes, slots in (
        ((-1, 0, 0), slice(0, depth), 0),
        ((1, 0, 0), slice(depth + nx, wide), 1 + BOTH),
    ):

        @pl.when(jnp.logical_not(exists(way)))
        def _():
            for f in range(2):
                clear(pair, f, planes, slice(None), body)
            clear(push_in, planes, slice(None), body)
            clear(cool, planes, slice(None), body)
            for side in range(2):
                clear(beside, side, slots, slice(None), slice(None))

    for way, rows, few in (
        ((0, 1, 0), slice(ny, ny + SUB), slice(ny, ny + SUB // 2)),
        ((0, -1, 0), slice(tall - SUB, tall), slice(short - SUB // 2, short)),
    ):

        @pl.when(jnp.logical_not(exists(way)))
        def _():
            for f in range(2):
                clear(pair, f, slice(None), rows, body)
            clear(push_in, slice(None), few, body)
            clear(cool, slice(None), few, body)
            for side in range(2):
                clear(beside, side, slice(None), rows, slice(None))

    for side, way in enumerate(((0, 0, -1), (0, 0, 1))):

        @pl.when(jnp.logical_not(exists(way)))
        def _():
            clear(beside, side, slice(None), slice(None), slice(None))

    def valid(index, size, cut, k):
        inner = index < size
        right = jnp.logical_and(index < size + cut, here[k] < counts[k] - 1)
        left = jnp.logical_and(index >= size + cut, here[k] > 0)
        return jnp.logical_or(inner, jnp.logical_or(right, left))

    y_index = lax.broadcasted_iota(jnp.int32, (short, long), 0)
    z_index = lax.broadcasted_iota(jnp.int32, (short, long), 1)
    both_in = jnp.logical_and(valid(y_index, ny, SUB // 2, 1), valid(z_index, nz, LANES // 2, 2))
    within = jnp.where(both_in, 1.0, 0.0)
    masks[0] = jnp.where(here[0] > 0, 1.0, 0.0) * within
    masks[1] = within
    masks[2] = jnp.where(here[0] < counts[0] - 1, 1.0, 0.0) * within

    def inside(i):
        return masks[0 if i < depth else 2 if i >= depth + nx else 1]

    loads[0].wait()
    table[0:1, 0 : table_in.shape[1]] = table_row[...]
    most = 7.0 + 24.0 * jnp.max(table[0:1, :], axis=1, keepdims=True)
    high, low = most, jnp.ones_like(most)
    middle = 0.5 * (high + low)
    half = 0.5 * (high - low)
    twice = 2.0 / half
    quarter = 0.125 * interval_delta
    lookup = jnp.broadcast_to(table[0:1, :], (ny, LANES))
    lane = lax.broadcasted_iota(jnp.int32, (ny, LANES), 1)

    every = ledger.at[pl.ds(0, 4 * nx * ny)]
    pltpu.make_async_copy(every, every, load_sems.at[1]).wait()
    packed = [[None, None], [None, None]]
    for i in range(nx):
        cond = jnp.take_along_axis(lookup, ints[0, i], axis=1)
        flag = ints[1, i].astype(jnp.float32)
        warm = pair[0, depth + i, 0:ny, 0:nz]
        push = interval_delta * source[i] - (interval_delta * cooling) * flag * warm
        push = twice * push
        pair[1, depth + i, 0:ny, 0:nz] = cond
        cool[depth + i, 0:ny, 0:nz] = flag
        push_in[depth + i, 0:ny, 0:nz] = push
        for g, start in enumerate((0, tail)):
            if not 0 <= i - start < depth:
                continue
            for f, piece in enumerate((warm, cond, push, flag)):
                at_lane = ((i - start) * FIELDS + f) * depth
                turned = pltpu.roll(piece, at_lane + depth, 1)
                for side in range(2):
                    old = packed[side][g]
                    if old is not None:
                        turned_in = jnp.where(lane >= at_lane + side * depth, turned, old)
                    else:
                        turned_in = turned
                    packed[side][g] = turned_in
    for side in range(2):
        for g in range(BOTH):
            edges[side, g] = packed[side][g]

    waits = neighbours()
    if not direct:
        waits = waits + (plane + line - 2)
    pl.semaphore_wait(barrier, waits)

    def y_span(step, reach, full):
        if step == 0:
            return pl.ds(0, ny), pl.ds(0, ny)
        if step > 0:
            return pl.ds(ny - reach, reach), pl.ds(full - reach, reach)
        return pl.ds(0, reach), pl.ds(ny, reach)

    def x_span(step, reach):
        if step == 0:
            return pl.ds(depth, nx), pl.ds(depth, nx)
        if step > 0:
            return pl.ds(depth + nx - reach, reach), pl.ds(depth - reach, reach)
        return pl.ds(depth, reach), pl.ds(depth + nx, reach)

    def send(src, dst, way, stage):
        pltpu.make_async_remote_copy(
            src_ref=src,
            dst_ref=dst,
            send_sem=halo_send.at[0],
            recv_sem=halo_recv.at[stage],
            device_id=at(way),
            device_id_type=MESH,
        ).start()

    def send_field(view, way, reach, full, stage):
        src_x, dst_x = x_span(way[0], reach)
        src_y, dst_y = y_span(way[1], reach, full)
        z = pl.ds(0, nz)
        send(view(src_x, src_y, z), view(dst_x, dst_y, z), way, stage)

    def send_first(way):
        send_field(lambda *v: pair.at[(1,) + v], way, depth, tall, 0)
        send_field(lambda *v: cool.at[v], way, depth - 2, short, 0)

    def send_second(way):
        send_field(lambda *v: pair.at[(0,) + v], way, depth, tall, 1)
        send_field(lambda *v: push_in.at[v], way, depth - 1, short, 1)

    def send_edges(way):
        if way[0] == 0:
            src_x, dst_x = pl.ds(0, BOTH), pl.ds(1, BOTH)
        elif way[0] > 0:
            src_x, dst_x = pl.ds(1, 1), pl.ds(0, 1)
        else:
            src_x, dst_x = pl.ds(0, 1), pl.ds(1 + BOTH, 1)
        src_y, dst_y = y_span(way[1], depth, tall)
        side = 0 if way[2] > 0 else 1
        send(edges.at[side, src_x, src_y], beside.at[side, dst_x, dst_y], way, 0)

    def send_all(steps):
        steps_on = tuple(v for v in steps if v)
        sides = [r for r in regions if r[0] and not r[1]]
        depths = sorted([r for r in regions if r[1]], key=lambda r: -abs(r[0]))
        plan = [(r, steps, (send_edges,)) for r in depths]
        plan += [(r, steps_on, (send_first,)) for r in sides]
        for action in (send_first, send_second):
            if action is send_second:
                plan += [(r, steps_on, (action,)) for r in sides]
            plan += [((0, 0), steps_on, (action,))] + [(r, (0,), (action,)) for r in sides]
        for region, some, actions in plan:

            def go(region=region, some=some, actions=actions):
                for action in actions:
                    for way in ways_of(region, some):
                        action(way)

            if ways_of(region, some):
                guard(region, go)

    by_class(send_all)

    def x_rows(step, reach):
        return reach if step else nx

    def y_rows(step, reach):
        return reach if step else ny

    def moved_rows(way, kind):
        if kind == 2:
            return (1 if way[0] else BOTH) * y_rows(way[1], depth)
        reaches = ((depth, depth - 2), (depth, depth - 1))[kind]
        return sum(x_rows(way[0], r) * y_rows(way[1], r) for r in reaches)

    def sides_of(k):
        if counts[k] == 1:
            return [(None, 0)]
        edge = jnp.logical_or(here[k] == 0, here[k] == counts[k] - 1)
        if counts[k] == 2:
            return [(None, 1)]
        return [(edge, 1), (jnp.logical_not(edge), 2)]

    def wait_all(kinds, semaphore, receive):
        def wait(sides):
            rows = 0
            for way in [(a, b, c) for a in (0, 1) for b in (0, 1) for c in (0, 1)]:
                times = 1
                for step, some in zip(way, sides):
                    times = times * (some if step else 1)
                for kind in kinds:
                    if any(way) and (kind == 2) == bool(way[2]):
                        rows = rows + times * moved_rows(way, kind)
            if rows == 0:
                return
            whole = pltpu.make_async_remote_copy(
                src_ref=ledger.at[pl.ds(0, rows)],
                dst_ref=ledger.at[pl.ds(0, rows)],
                send_sem=semaphore,
                recv_sem=semaphore,
                device_id=all_targets[0],
                device_id_type=MESH,
            )
            if receive:
                whole.wait_recv()
            else:
                whole.wait_send()

        for x_good, x_some in sides_of(0):
            for y_good, y_some in sides_of(1):
                for z_good, z_some in sides_of(2):
                    good = None
                    for one in (x_good, y_good, z_good):
                        if one is not None:
                            good = one if good is None else jnp.logical_and(good, one)
                    act = functools.partial(wait, (x_some, y_some, z_some))
                    if good is None:
                        act()
                    else:
                        pl.when(good)(act)

    if direct:
        signal_all(near)
        hops = [(a, 0, c) for a in (0, 2, -2) for c in (0, 2, -2) if a or c]
        hops = [h for h in hops if abs(h[0]) < counts[0] and abs(h[2]) < counts[2]]
        pl.semaphore_wait(near, neighbours())
        for hop in hops:
            signal(far, hop)

    def share(stage, rows_ref, slot, targets):
        for target in targets:
            pltpu.make_async_remote_copy(
                src_ref=row_out.at[stage],
                dst_ref=rows_ref.at[slot],
                send_sem=row_send.at[stage],
                recv_sem=row_recv.at[stage],
                device_id=target,
                device_id_type=MESH,
            ).start()

    def share_wait(stage, rows_ref, targets):
        if targets:
            whole = pltpu.make_async_remote_copy(
                src_ref=rows_ref.at[pl.ds(0, len(targets))],
                dst_ref=rows_ref.at[pl.ds(0, len(targets))],
                send_sem=row_send.at[stage],
                recv_sem=row_recv.at[stage],
                device_id=targets[0],
                device_id_type=MESH,
            )
            whole.wait_send()
            whole.wait_recv()

    wait_all((0, 2), halo_recv.at[0], True)

    first_half = lax.broadcasted_iota(jnp.int32, (SUB, LANES), 0) < SUB // 2
    tall_lane = lax.broadcasted_iota(jnp.int32, (tall, LANES), 1)

    def narrow(v):
        mask = jnp.concatenate([first_half] * (v.shape[1] // LANES), axis=1)
        join = jnp.where(mask, v[ny : ny + SUB], v[ny + SUB :])
        return jnp.concatenate([v[:ny], join], axis=0)

    places = [(0, j) for j in range(depth)]
    places += [(1, p) if p < depth else (2, p - tail) for p in range(nx)]
    places += [(1 + BOTH, j) for j in range(depth)]
    for i, (g, slot) in enumerate(places):
        full = [beside[side, g] for side in range(2)]
        thin = [narrow(v) for v in full]
        for f, ref in enumerate((pair, pair, push_in, cool)):
            spare = (0, 0, 1, 2)[f]
            if not spare <= i < wide - spare:
                continue
            cut = (slot * FIELDS + f + 1) * depth
            both = full if f < 2 else thin
            kept = jnp.where(tall_lane[: both[0].shape[0]] < cut, both[0], both[1])
            kept = pltpu.roll(kept, LANES - cut, 1)
            if f < 2:
                ref[f, i, :, nz:] = kept
            else:
                ref[i, :, nz:] = kept

    def along_x(least, most, planes_of, use):
        before = sums = None
        for i in range(least, most):
            now = planes_of(i)
            if i > least:
                joined = [a + b for a, b in zip(before, now)]
                if sums is not None:
                    use(i - 1, *[a + b for a, b in zip(sums, joined)])
                sums = joined
            before = now

    def ring_of(i):
        return (smooth_z(narrow(smooth_y(pair[1, i]))),)

    def use_ring(i, ring):
        cond = narrow(pair[1, i])
        base = twice * (8.0 * interval_delta * cond + quarter * ring)
        spread[i] = base
        couple[i] = (quarter * twice) * cond
        if 2 <= i < wide - 2:
            diag[i] = base + twice * ((1.0 - middle) + interval_delta * cooling * cool[i])

    along_x(0, wide, ring_of, use_ring)

    wait_all((1,), halo_recv.at[1], True)

    totals = [None] * MOMENTS

    def gather(n, a, b):
        part = a * b
        part = part[:SUB] + part[SUB:] if ny == 2 * SUB else sum(
            part[r : r + SUB] for r in range(0, ny, SUB)
        )
        totals[n] = part if totals[n] is None else totals[n] + part

    def core(v):
        return v[:ny, :nz]

    def warm_of(i):
        warm = pair[0, i]
        warm_flux = (quarter * twice) * (pair[1, i] * warm)
        return smooth_z(narrow(smooth_y(warm))), smooth_z(narrow(smooth_y(warm_flux)))

    def use_warm(i, ring, push):
        edge = couple[i]
        image = spread[i] * narrow(pair[0, i]) - (edge * ring + inside(i) * push)
        fresh = push_in[i] - image
        basis[0, i] = fresh
        flux[0, i] = edge * fresh
        if depth <= i < depth + nx:
            gather(0, core(fresh), core(fresh))

    along_x(0, wide, warm_of, use_warm)

    for k in range(ITERS - 1):

        def level_of(i, k=k):
            return smooth_z(smooth_y(basis[k, i])), smooth_z(smooth_y(flux[k % 2, i]))

        def use_level(i, ring, push, k=k):
            edge = couple[i]
            mid = basis[k, i]
            fresh = diag[i] * mid - (edge * ring + inside(i) * push)
            if k > 0:
                fresh = fresh - basis[k - 1, i]
            basis[k + 1, i] = fresh
            flux[(k + 1) % 2, i] = edge * fresh
            if depth <= i < depth + nx:
                gather(2 * k + 1, core(mid), core(fresh))
                gather(2 * k + 2, core(fresh), core(fresh))

        along_x(k + 1, wide - k - 1, level_of, use_level)

    k = ITERS - 1

    def last_of(i):
        return (
            smooth_z_own(smooth_y(basis[k, i])[:ny]),
            smooth_z_own(smooth_y(flux[k % 2, i])[:ny]),
        )

    def use_last(i, ring, push):
        mid = basis[k, i, 0:ny, 0:nz]
        fresh = diag[i, 0:ny, 0:nz] * mid - (couple[i, 0:ny, 0:nz] * ring + push)
        fresh = fresh - basis[k - 1, i, 0:ny, 0:nz]
        basis[k + 1, i, 0:ny, 0:nz] = fresh
        gather(2 * k + 1, mid, fresh)

    along_x(depth - 1, depth + nx + 1, last_of, use_last)

    diagonal = lax.broadcasted_iota(jnp.int32, (SUB, LANES), 0)
    across = lax.broadcasted_iota(jnp.int32, (SUB, LANES), 1)
    tile = jnp.zeros((SUB, LANES), jnp.float32)
    for n in range(MOMENTS):
        tile = jnp.where(diagonal == n, jnp.sum(totals[n], axis=0, keepdims=True), tile)
    column = jnp.sum(tile, axis=1, keepdims=True)
    row = jnp.sum(jnp.where(across == diagonal, column, 0.0), axis=0, keepdims=True)
    if direct:
        pl.semaphore_wait(far, present(back(h) for h in hops))
    row_out[0] = row

    def settle():
        wait_all((0, 1, 2), halo_send.at[0], False)

    if direct:
        mine = in_plane * line + here[2]
        all_rows[mine] = row
        share(0, all_rows, mine, all_targets)
        settle()
        share_wait(0, all_rows, all_targets)
        row = jnp.sum(all_rows[...], axis=0)
    else:
        plane_rows[in_plane] = row
        share(0, plane_rows, in_plane, plane_targets)
        settle()
        share_wait(0, plane_rows, plane_targets)
        row = jnp.sum(plane_rows[...], axis=0)
        row_out[1] = row
        line_rows[here[2]] = row
        share(1, line_rows, here[2], line_targets)
        share_wait(1, line_rows, line_targets)
        row = jnp.sum(line_rows[...], axis=0)
    row_lane = lax.broadcasted_iota(jnp.int32, (1, LANES), 1)
    gram = {}
    for n in range(MOMENTS):
        value = jnp.sum(jnp.where(row_lane == n, row, 0.0), axis=1, keepdims=True)
        gram[n // 2, (n + 1) // 2] = value
    for gap in range(2, ITERS + 1):
        for i in range(ITERS + 1 - gap):
            j = i + gap
            value = gram[i + 1, j - 1] - gram[i, j - 2]
            if i > 0:
                value = value + gram[i - 1, j - 1]
            gram[i, j] = value
    for i, j in list(gram):
        gram[j, i] = gram[i, j]

    def apply(p):
        q = [middle * a for a in p] + [jnp.zeros_like(half)]
        for i, a in enumerate(p):
            q[i + 1] = q[i + 1] + (0.5 * half) * a
            if i > 0:
                q[i - 1] = q[i - 1] + (0.5 * half) * a
        return q

    def product(p, q):
        value = None
        for i, a in enumerate(p):
            inner = None
            for j, b in enumerate(q):
                term = gram[i, j] * b
                inner = term if inner is None else inner + term
            inner = a * inner
            value = inner if value is None else value + inner
        return value

    left = [0.5 * half]
    heading = list(left)
    moved = []
    norm = product(left, left)
    for step in range(ITERS):
        image = apply(heading)
        alpha = norm / product(heading, image)
        moved = [a + alpha * b for a, b in zip(moved, heading)] + [
            alpha * b for b in heading[len(moved) :]
        ]
        left = [a - alpha * b for a, b in zip(left, image)] + [
            -alpha * b for b in image[len(left) :]
        ]
        if step + 1 < ITERS:
            following = product(left, left)
            ratio = following / norm
            heading = [a + ratio * b for a, b in zip(left, heading)] + left[len(heading) :]
            norm = following

    for i in range(nx):
        warm = pair[0, depth + i, 0:ny, 0:nz]
        end = jnp.zeros_like(warm)
        for k in range(ITERS + 1):
            value = basis[k, depth + i, 0:ny, 0:nz]
            if k < ITERS:
                warm = warm + moved[k] * value
            end = end + left[k] * value
        both_out[0, i] = warm
        both_out[1, i] = end


def body(counts, warm, source, category, table, flags):
    nx, ny, nz = warm.shape
    depth = DEPTH
    plane, line = counts[0] * counts[1], counts[2]
    if nx < depth or nx % 2 or ny % SUB or nz != LANES or table.shape[0] > LANES:
        raise ValueError("block shape")
    if nx > 2 * depth or (FIELDS * depth + 1) * depth > LANES:
        raise ValueError("block shape")
    wide, tall, short, long = nx + 2 * depth, ny + 2 * SUB, ny + SUB, nz + LANES
    table = table[None]
    any_spec = pl.BlockSpec(memory_space=pl.ANY)
    vmem = pl.BlockSpec(memory_space=pltpu.VMEM)
    f32 = jnp.float32
    both = pl.pallas_call(
        functools.partial(kernel, counts),
        out_shape=pltpu.VMEM((2,) + warm.shape, jnp.float32),
        in_specs=[any_spec] * 5,
        out_specs=vmem,
        scratch_shapes=[
            pltpu.VMEM((2, wide, tall, long), f32),
            pltpu.VMEM((wide, short, long), f32),
            pltpu.VMEM((wide, short, long), f32),
            pltpu.VMEM((ITERS + 1, wide, short, long), f32),
            pltpu.VMEM((2, wide, short, long), f32),
            pltpu.VMEM((wide, short, long), f32),
            pltpu.VMEM((wide, short, long), f32),
            pltpu.VMEM((wide, short, long), f32),
            pltpu.VMEM((3, short, long), f32),
            pltpu.VMEM((SUB, LANES), f32),
            pltpu.VMEM(table.shape, f32),
            pltpu.VMEM((nx, ny, nz), f32),
            pltpu.VMEM((2, nx, ny, nz), jnp.int32),
            pltpu.VMEM((2, BOTH, ny, nz), f32),
            pltpu.VMEM((2, BOTH + 2, tall, nz), f32),
            pltpu.VMEM((16 * nx * ny, LANES), f32),
            pltpu.VMEM((2, 1, LANES), f32),
            pltpu.VMEM((plane, 1, LANES), f32),
            pltpu.VMEM((line, 1, LANES), f32),
            pltpu.VMEM((plane * line, 1, LANES), f32),
            pltpu.SemaphoreType.DMA((2,)),
            pltpu.SemaphoreType.DMA((1,)),
            pltpu.SemaphoreType.DMA((2,)),
            pltpu.SemaphoreType.DMA((2,)),
            pltpu.SemaphoreType.DMA((2,)),
            pltpu.SemaphoreType.REGULAR,
            pltpu.SemaphoreType.REGULAR,
        ],
        compiler_params=pltpu.CompilerParams(collective_id=0, has_side_effects=True),
    )(warm, source, category, table, flags)
    return both[0], both[1]


def solution(mesh):
    counts = tuple(mesh.shape[a] for a in AXES)
    spec = P("gx", "gy", "gz")
    return jax.shard_map(
        functools.partial(body, counts),
        mesh=mesh,
        in_specs=(spec, spec, spec, P(), spec),
        out_specs=(spec, spec),
        check_vma=False,
    )
```

```python
import functools

import jax
import jax.numpy as jnp
from jax import lax
from jax.experimental import pallas as pl
from jax.experimental.pallas import tpu as pltpu
from jax.sharding import PartitionSpec as P

ITERS = 4
interval_delta = 2.0
cooling = 3.0

MESH = pl.DeviceIdType.MESH
AXES = ("gx", "gy", "gz")
SUB = 8
REACH = 4
LANES = 128
FIELDS = 4
DEPTH = ITERS + 1
BOTH = 2
MOMENTS = 2 * ITERS
REGIONS = [(a, c) for c in (0, 1, -1) for a in (0, 1, -1)]


def smooth_y(values):
    pairs = values + pltpu.roll(values, 1, 0)
    return pairs + pltpu.roll(pairs, values.shape[0] - 1, 0)


def smooth_z(values):
    size = values.shape[1]
    return (values + values) + (pltpu.roll(values, 1, 1) + pltpu.roll(values, size - 1, 1))


def smooth_z_own(values):
    size = values.shape[1] // 2
    main, side = values[:, :size], values[:, size:]
    lane = lax.broadcasted_iota(jnp.int32, main.shape, 1)
    before = pltpu.roll(jnp.where(lane == size - 1, side, main), 1, 1)
    after = pltpu.roll(jnp.where(lane == 0, side, main), size - 1, 1)
    return (main + main) + (before + after)


def kernel(
    counts,
    warm_in,
    source_in,
    category_in,
    table_in,
    flags_in,
    both_out,
    pair,
    push_in,
    cool,
    basis,
    spread,
    diag,
    couple,
    masks,
    table,
    table_row,
    source,
    ints,
    edges,
    beside,
    ledger,
    row_out,
    plane_rows,
    line_rows,
    all_rows,
    load_sems,
    halo_send,
    halo_recv,
    row_send,
    row_recv,
    near,
    far,
):
    plane, line = counts[0] * counts[1], counts[2]
    nx, ny, nz = both_out.shape[1:]
    depth = DEPTH
    wide, tall, long = pair.shape[1:]
    short = ny + SUB
    tail = nx - depth
    direct = max(counts) <= REACH
    here = [lax.axis_index(a) for a in AXES]
    in_plane = here[0] * counts[1] + here[1]

    def exists(offset):
        good = None
        for k in range(3):
            if offset[k] > 0:
                one = here[k] < counts[k] - offset[k]
            elif offset[k] < 0:
                one = here[k] >= -offset[k]
            else:
                continue
            good = one if good is None else jnp.logical_and(good, one)
        return good

    def at(offset):
        return {a: here[k] + offset[k] for k, a in enumerate(AXES)}

    def back(offset):
        return tuple(-o for o in offset)

    def signal(semaphore, offset):
        @pl.when(exists(offset))
        def _():
            pl.semaphore_signal(semaphore, inc=1, device_id=at(offset), device_id_type=MESH)

    def present(offsets):
        return sum(jnp.where(exists(offset), 1, 0) for offset in offsets)

    plane_targets = [
        {"gx": other // counts[1], "gy": other % counts[1], "gz": here[2]}
        for other in [(in_plane + step) % plane for step in range(1, plane)]
    ]
    line_targets = [
        {"gx": here[0], "gy": here[1], "gz": (here[2] + step) % line} for step in range(1, line)
    ]
    moved_by = [[(here[k] + step) % counts[k] for step in range(counts[k])] for k in range(3)]
    all_targets = [
        {"gx": moved_by[0][a], "gy": moved_by[1][b], "gz": moved_by[2][c]}
        for c in reversed(range(counts[2]))
        for b in reversed(range(counts[1]))
        for a in reversed(range(counts[0]))
        if a or b or c
    ]

    regions = [r for r in REGIONS if abs(r[0]) < counts[0] and abs(r[1]) < counts[2]]

    def by_class(act):
        if counts[1] == 1:
            act((0,))
            return
        pl.when(here[1] == 0)(lambda: act((0, 1)))
        pl.when(here[1] == counts[1] - 1)(lambda: act((0, -1)))
        if counts[1] > 2:
            inner = jnp.logical_and(here[1] > 0, here[1] < counts[1] - 1)
            pl.when(inner)(lambda: act((0, 1, -1)))

    def guard(region, act):
        if region == (0, 0):
            act()
        else:
            pl.when(exists((region[0], 0, region[1])))(act)

    def ways_of(region, steps):
        ways = [(region[0], step, region[1]) for step in sorted(steps, key=lambda v: -abs(v))]
        return [way for way in ways if any(way)]

    def neighbours():
        total = 0
        for region in regions:
            here_too = 1 if region == (0, 0) else jnp.where(exists((region[0], 0, region[1])), 1, 0)
            beside_y = present([(0, 1, 0), (0, -1, 0)]) if counts[1] > 1 else 0
            total = total + here_too * (beside_y + (0 if region == (0, 0) else 1))
        return total

    def signal_all(semaphore):
        def act(steps):
            for region in reversed(regions):

                def go(region=region):
                    for way in ways_of(region, steps):
                        pl.semaphore_signal(semaphore, inc=1, device_id=at(way), device_id_type=MESH)

                guard(region, go)

        by_class(act)

    own = (pl.ds(depth, nx), pl.ds(0, ny), pl.ds(0, nz))
    loads = [
        pltpu.make_async_copy(table_in, table_row, load_sems.at[0]),
        pltpu.make_async_copy(category_in, ints.at[0], load_sems.at[1]),
        pltpu.make_async_copy(flags_in, ints.at[1], load_sems.at[1]),
        pltpu.make_async_copy(warm_in, pair.at[(0,) + own], load_sems.at[1]),
        pltpu.make_async_copy(source_in, source, load_sems.at[1]),
    ]
    for load in loads:
        load.start()

    barrier = pltpu.get_barrier_semaphore()
    signal_all(barrier)
    if not direct:
        for target in plane_targets + line_targets:
            pl.semaphore_signal(barrier, inc=1, device_id=target, device_id_type=MESH)

    def clear(ref, *index):
        shape = ref.at[index].shape
        ref[index] = jnp.zeros(shape, jnp.float32)

    table[...] = jnp.zeros(table.shape, jnp.float32)
    body = slice(0, nz)
    for way, planes, slots in (
        ((-1, 0, 0), slice(0, depth), 0),
        ((1, 0, 0), slice(depth + nx, wide), 1 + BOTH),
    ):

        @pl.when(jnp.logical_not(exists(way)))
        def _():
            for f in range(2):
                clear(pair, f, planes, slice(None), body)
            clear(push_in, planes, slice(None), body)
            clear(cool, planes, slice(None), body)
            for side in range(2):
                clear(beside, side, slots, slice(None), slice(None))

    for way, rows, few in (
        ((0, 1, 0), slice(ny, ny + SUB), slice(ny, ny + SUB // 2)),
        ((0, -1, 0), slice(tall - SUB, tall), slice(short - SUB // 2, short)),
    ):

        @pl.when(jnp.logical_not(exists(way)))
        def _():
            for f in range(2):
                clear(pair, f, slice(None), rows, body)
            clear(push_in, slice(None), few, body)
            clear(cool, slice(None), few, body)
            for side in range(2):
                clear(beside, side, slice(None), rows, slice(None))

    for side, way in enumerate(((0, 0, -1), (0, 0, 1))):

        @pl.when(jnp.logical_not(exists(way)))
        def _():
            clear(beside, side, slice(None), slice(None), slice(None))

    def valid(index, size, cut, k):
        inner = index < size
        right = jnp.logical_and(index < size + cut, here[k] < counts[k] - 1)
        left = jnp.logical_and(index >= size + cut, here[k] > 0)
        return jnp.logical_or(inner, jnp.logical_or(right, left))

    y_index = lax.broadcasted_iota(jnp.int32, (short, long), 0)
    z_index = lax.broadcasted_iota(jnp.int32, (short, long), 1)
    both_in = jnp.logical_and(valid(y_index, ny, SUB // 2, 1), valid(z_index, nz, LANES // 2, 2))
    within = jnp.where(both_in, 1.0, 0.0)
    masks[0] = jnp.where(here[0] > 0, 1.0, 0.0) * within
    masks[1] = within
    masks[2] = jnp.where(here[0] < counts[0] - 1, 1.0, 0.0) * within

    def inside(i):
        return masks[0 if i < depth else 2 if i >= depth + nx else 1]

    loads[0].wait()
    table[0:1, 0 : table_in.shape[1]] = table_row[...]
    most = 7.0 + 24.0 * jnp.max(table[0:1, :], axis=1, keepdims=True)
    high, low = most, jnp.ones_like(most)
    middle = 0.5 * (high + low)
    half = 0.5 * (high - low)
    twice = 2.0 / half
    quarter = 0.125 * interval_delta
    lookup = jnp.broadcast_to(table[0:1, :], (ny, LANES))
    lane = lax.broadcasted_iota(jnp.int32, (ny, LANES), 1)

    every = ledger.at[pl.ds(0, 4 * nx * ny)]
    pltpu.make_async_copy(every, every, load_sems.at[1]).wait()
    packed = [[None, None], [None, None]]
    for i in range(nx):
        cond = jnp.take_along_axis(lookup, ints[0, i], axis=1)
        flag = ints[1, i].astype(jnp.float32)
        warm = pair[0, depth + i, 0:ny, 0:nz]
        push = interval_delta * source[i] - (interval_delta * cooling) * flag * warm
        push = twice * push
        pair[1, depth + i, 0:ny, 0:nz] = cond
        cool[depth + i, 0:ny, 0:nz] = flag
        push_in[depth + i, 0:ny, 0:nz] = push
        for g, start in enumerate((0, tail)):
            if not 0 <= i - start < depth:
                continue
            for f, piece in enumerate((warm, cond, push, flag)):
                at_lane = ((i - start) * FIELDS + f) * depth
                turned = pltpu.roll(piece, at_lane + depth, 1)
                for side in range(2):
                    old = packed[side][g]
                    if old is not None:
                        turned_in = jnp.where(lane >= at_lane + side * depth, turned, old)
                    else:
                        turned_in = turned
                    packed[side][g] = turned_in
    for side in range(2):
        for g in range(BOTH):
            edges[side, g] = packed[side][g]

    waits = neighbours()
    if not direct:
        waits = waits + (plane + line - 2)
    pl.semaphore_wait(barrier, waits)

    def y_span(step, reach, full):
        if step == 0:
            return pl.ds(0, ny), pl.ds(0, ny)
        if step > 0:
            return pl.ds(ny - reach, reach), pl.ds(full - reach, reach)
        return pl.ds(0, reach), pl.ds(ny, reach)

    def x_span(step, reach):
        if step == 0:
            return pl.ds(depth, nx), pl.ds(depth, nx)
        if step > 0:
            return pl.ds(depth + nx - reach, reach), pl.ds(depth - reach, reach)
        return pl.ds(depth, reach), pl.ds(depth + nx, reach)

    def send(src, dst, way, stage):
        pltpu.make_async_remote_copy(
            src_ref=src,
            dst_ref=dst,
            send_sem=halo_send.at[0],
            recv_sem=halo_recv.at[stage],
            device_id=at(way),
            device_id_type=MESH,
        ).start()

    def send_field(view, way, reach, full, stage):
        src_x, dst_x = x_span(way[0], reach)
        src_y, dst_y = y_span(way[1], reach, full)
        z = pl.ds(0, nz)
        send(view(src_x, src_y, z), view(dst_x, dst_y, z), way, stage)

    def send_cond(way):
        send_field(lambda *v: pair.at[(1,) + v], way, depth, tall, 0)

    def send_warm(way):
        send_field(lambda *v: pair.at[(0,) + v], way, depth, tall, 1)

    def send_rest(way):
        send_field(lambda *v: push_in.at[v], way, depth - 1, short, 2)
        send_field(lambda *v: cool.at[v], way, depth - 2, short, 2)

    def send_edges(way):
        if way[0] == 0:
            src_x, dst_x = pl.ds(0, BOTH), pl.ds(1, BOTH)
        elif way[0] > 0:
            src_x, dst_x = pl.ds(1, 1), pl.ds(0, 1)
        else:
            src_x, dst_x = pl.ds(0, 1), pl.ds(1 + BOTH, 1)
        src_y, dst_y = y_span(way[1], depth, tall)
        side = 0 if way[2] > 0 else 1
        send(edges.at[side, src_x, src_y], beside.at[side, dst_x, dst_y], way, 0)

    def send_all(steps):
        steps_on = tuple(v for v in steps if v)
        sides = [r for r in regions if r[0] and not r[1]]
        depths = sorted([r for r in regions if r[1]], key=lambda r: -abs(r[0]))
        plan = [(r, steps, (send_edges,)) for r in depths]
        for action in (send_cond, send_warm, send_rest):
            plan += [((0, 0), steps_on, (action,))] + [(r, steps, (action,)) for r in sides]
        for region, some, actions in plan:

            def go(region=region, some=some, actions=actions):
                for action in actions:
                    for way in ways_of(region, some):
                        action(way)

            if ways_of(region, some):
                guard(region, go)

    by_class(send_all)

    def x_rows(step, reach):
        return reach if step else nx

    def y_rows(step, reach):
        return reach if step else ny

    def moved_rows(way, kind):
        if kind == 3:
            return (1 if way[0] else BOTH) * y_rows(way[1], depth)
        reaches = ((depth,), (depth,), (depth - 1, depth - 2))[kind]
        return sum(x_rows(way[0], r) * y_rows(way[1], r) for r in reaches)

    def sides_of(k):
        if counts[k] == 1:
            return [(None, 0)]
        edge = jnp.logical_or(here[k] == 0, here[k] == counts[k] - 1)
        if counts[k] == 2:
            return [(None, 1)]
        return [(edge, 1), (jnp.logical_not(edge), 2)]

    def wait_all(kinds, semaphore, receive):
        def wait(sides):
            rows = 0
            for way in [(a, b, c) for a in (0, 1) for b in (0, 1) for c in (0, 1)]:
                times = 1
                for step, some in zip(way, sides):
                    times = times * (some if step else 1)
                for kind in kinds:
                    if any(way) and (kind == 3) == bool(way[2]):
                        rows = rows + times * moved_rows(way, kind)
            if rows == 0:
                return
            whole = pltpu.make_async_remote_copy(
                src_ref=ledger.at[pl.ds(0, rows)],
                dst_ref=ledger.at[pl.ds(0, rows)],
                send_sem=semaphore,
                recv_sem=semaphore,
                device_id=all_targets[0],
                device_id_type=MESH,
            )
            if receive:
                whole.wait_recv()
            else:
                whole.wait_send()

        for x_good, x_some in sides_of(0):
            for y_good, y_some in sides_of(1):
                for z_good, z_some in sides_of(2):
                    good = None
                    for one in (x_good, y_good, z_good):
                        if one is not None:
                            good = one if good is None else jnp.logical_and(good, one)
                    act = functools.partial(wait, (x_some, y_some, z_some))
                    if good is None:
                        act()
                    else:
                        pl.when(good)(act)

    if direct:
        signal_all(near)
        hops = [(a, 0, c) for a in (0, 2, -2) for c in (0, 2, -2) if a or c]
        hops = [h for h in hops if abs(h[0]) < counts[0] and abs(h[2]) < counts[2]]
        pl.semaphore_wait(near, neighbours())
        for hop in hops:
            signal(far, hop)

    def share(stage, rows_ref, slot, targets):
        for target in targets:
            pltpu.make_async_remote_copy(
                src_ref=row_out.at[stage],
                dst_ref=rows_ref.at[slot],
                send_sem=row_send.at[stage],
                recv_sem=row_recv.at[stage],
                device_id=target,
                device_id_type=MESH,
            ).start()

    def share_wait(stage, rows_ref, targets):
        if targets:
            whole = pltpu.make_async_remote_copy(
                src_ref=rows_ref.at[pl.ds(0, len(targets))],
                dst_ref=rows_ref.at[pl.ds(0, len(targets))],
                send_sem=row_send.at[stage],
                recv_sem=row_recv.at[stage],
                device_id=targets[0],
                device_id_type=MESH,
            )
            whole.wait_send()
            whole.wait_recv()

    wait_all((0, 3), halo_recv.at[0], True)

    first_half = lax.broadcasted_iota(jnp.int32, (SUB, LANES), 0) < SUB // 2
    tall_lane = lax.broadcasted_iota(jnp.int32, (tall, LANES), 1)

    def narrow(v):
        mask = jnp.concatenate([first_half] * (v.shape[1] // LANES), axis=1)
        join = jnp.where(mask, v[ny : ny + SUB], v[ny + SUB :])
        return jnp.concatenate([v[:ny], join], axis=0)

    places = [(0, j) for j in range(depth)]
    places += [(1, p) if p < depth else (2, p - tail) for p in range(nx)]
    places += [(1 + BOTH, j) for j in range(depth)]

    def unpack(fields):
        for i, (g, slot) in enumerate(places):
            both = [beside[side, g] for side in range(2)]
            if fields[0] >= 2:
                both = [narrow(v) for v in both]
            for f in fields:
                ref, spare = ((pair, 0), (pair, 0), (push_in, 1), (cool, 2))[f]
                if not spare <= i < wide - spare:
                    continue
                cut = (slot * FIELDS + f + 1) * depth
                kept = jnp.where(tall_lane[: both[0].shape[0]] < cut, both[0], both[1])
                kept = pltpu.roll(kept, LANES - cut, 1)
                if f < 2:
                    ref[f, i, :, nz:] = kept
                else:
                    ref[i, :, nz:] = kept

    unpack((1, 0))

    def along_x(least, most, planes_of, use):
        before = sums = None
        for i in range(least, most):
            now = planes_of(i)
            if i > least:
                joined = [a + b for a, b in zip(before, now)]
                if sums is not None:
                    use(i - 1, *[a + b for a, b in zip(sums, joined)])
                sums = joined
            before = now

    def ring_of(i):
        return (smooth_z(narrow(smooth_y(pair[1, i]))),)

    def use_ring(i, ring):
        cond = narrow(pair[1, i])
        base = twice * (8.0 * interval_delta * cond + quarter * ring)
        spread[i] = base
        couple[i] = (quarter * twice) * cond

    along_x(0, wide, ring_of, use_ring)

    wait_all((1,), halo_recv.at[1], True)

    totals = [None] * MOMENTS

    def gather(n, a, b):
        part = a * b
        part = part[:SUB] + part[SUB:] if ny == 2 * SUB else sum(
            part[r : r + SUB] for r in range(0, ny, SUB)
        )
        totals[n] = part if totals[n] is None else totals[n] + part

    def core(v):
        return v[:ny, :nz]

    def warm_of(i):
        warm = pair[0, i]
        warm_flux = (quarter * twice) * (pair[1, i] * warm)
        return smooth_z(narrow(smooth_y(warm))), smooth_z(narrow(smooth_y(warm_flux)))

    def use_warm(i, ring, push):
        edge = couple[i]
        image = spread[i] * narrow(pair[0, i]) - (edge * ring + inside(i) * push)
        basis[0, i] = image

    along_x(0, wide, warm_of, use_warm)
    unpack((2, 3))

    wait_all((2,), halo_recv.at[2], True)

    for k in range(ITERS - 1):

        def level_of(i, k=k):
            mid = basis[k, i]
            if k == 0:
                mid = push_in[i] - mid
                basis[0, i] = mid
                if depth <= i < depth + nx:
                    gather(0, core(mid), core(mid))
            return smooth_z(smooth_y(mid)), smooth_z(smooth_y(couple[i] * mid))

        def use_level(i, ring, push, k=k):
            edge = couple[i]
            mid = basis[k, i]
            if k == 0:
                main = spread[i] + twice * ((1.0 - middle) + interval_delta * cooling * cool[i])
                diag[i] = main
            else:
                main = diag[i]
            fresh = main * mid - (edge * ring + inside(i) * push)
            if k > 0:
                fresh = fresh - basis[k - 1, i]
            basis[k + 1, i] = fresh
            if depth <= i < depth + nx:
                gather(2 * k + 1, core(mid), core(fresh))
                gather(2 * k + 2, core(fresh), core(fresh))

        along_x(k + 1, wide - k - 1, level_of, use_level)

    k = ITERS - 1

    def last_of(i):
        return (
            smooth_z_own(smooth_y(basis[k, i])[:ny]),
            smooth_z_own(smooth_y(couple[i] * basis[k, i])[:ny]),
        )

    def use_last(i, ring, push):
        mid = basis[k, i, 0:ny, 0:nz]
        fresh = diag[i, 0:ny, 0:nz] * mid - (couple[i, 0:ny, 0:nz] * ring + push)
        fresh = fresh - basis[k - 1, i, 0:ny, 0:nz]
        basis[k + 1, i, 0:ny, 0:nz] = fresh
        gather(2 * k + 1, mid, fresh)

    along_x(depth - 1, depth + nx + 1, last_of, use_last)

    diagonal = lax.broadcasted_iota(jnp.int32, (SUB, LANES), 0)
    across = lax.broadcasted_iota(jnp.int32, (SUB, LANES), 1)
    tile = jnp.zeros((SUB, LANES), jnp.float32)
    for n in range(MOMENTS):
        tile = jnp.where(diagonal == n, jnp.sum(totals[n], axis=0, keepdims=True), tile)
    column = jnp.sum(tile, axis=1, keepdims=True)
    row = jnp.sum(jnp.where(across == diagonal, column, 0.0), axis=0, keepdims=True)
    if direct:
        pl.semaphore_wait(far, present(back(h) for h in hops))
    row_out[0] = row

    def settle():
        wait_all((0, 1, 2, 3), halo_send.at[0], False)

    if direct:
        mine = in_plane * line + here[2]
        all_rows[mine] = row
        share(0, all_rows, mine, all_targets)
        settle()
        share_wait(0, all_rows, all_targets)
        row = jnp.sum(all_rows[...], axis=0)
    else:
        plane_rows[in_plane] = row
        share(0, plane_rows, in_plane, plane_targets)
        settle()
        share_wait(0, plane_rows, plane_targets)
        row = jnp.sum(plane_rows[...], axis=0)
        row_out[1] = row
        line_rows[here[2]] = row
        share(1, line_rows, here[2], line_targets)
        share_wait(1, line_rows, line_targets)
        row = jnp.sum(line_rows[...], axis=0)
    row_lane = lax.broadcasted_iota(jnp.int32, (1, LANES), 1)
    gram = {}
    for n in range(MOMENTS):
        value = jnp.sum(jnp.where(row_lane == n, row, 0.0), axis=1, keepdims=True)
        gram[n // 2, (n + 1) // 2] = value
    for gap in range(2, ITERS + 1):
        for i in range(ITERS + 1 - gap):
            j = i + gap
            value = gram[i + 1, j - 1] - gram[i, j - 2]
            if i > 0:
                value = value + gram[i - 1, j - 1]
            gram[i, j] = value
    for i, j in list(gram):
        gram[j, i] = gram[i, j]

    def apply(p):
        q = [middle * a for a in p] + [jnp.zeros_like(half)]
        for i, a in enumerate(p):
            q[i + 1] = q[i + 1] + (0.5 * half) * a
            if i > 0:
                q[i - 1] = q[i - 1] + (0.5 * half) * a
        return q

    def product(p, q):
        value = None
        for i, a in enumerate(p):
            inner = None
            for j, b in enumerate(q):
                term = gram[i, j] * b
                inner = term if inner is None else inner + term
            inner = a * inner
            value = inner if value is None else value + inner
        return value

    left = [0.5 * half]
    heading = list(left)
    moved = []
    norm = product(left, left)
    for step in range(ITERS):
        image = apply(heading)
        alpha = norm / product(heading, image)
        moved = [a + alpha * b for a, b in zip(moved, heading)] + [
            alpha * b for b in heading[len(moved) :]
        ]
        left = [a - alpha * b for a, b in zip(left, image)] + [
            -alpha * b for b in image[len(left) :]
        ]
        if step + 1 < ITERS:
            following = product(left, left)
            ratio = following / norm
            heading = [a + ratio * b for a, b in zip(left, heading)] + left[len(heading) :]
            norm = following

    for i in range(nx):
        warm = pair[0, depth + i, 0:ny, 0:nz]
        end = jnp.zeros_like(warm)
        for k in range(ITERS + 1):
            value = basis[k, depth + i, 0:ny, 0:nz]
            if k < ITERS:
                warm = warm + moved[k] * value
            end = end + left[k] * value
        both_out[0, i] = warm
        both_out[1, i] = end


def body(counts, warm, source, category, table, flags):
    nx, ny, nz = warm.shape
    depth = DEPTH
    plane, line = counts[0] * counts[1], counts[2]
    if nx < depth or nx % 2 or ny % SUB or nz != LANES or table.shape[0] > LANES:
        raise ValueError("block shape")
    if nx > 2 * depth or (FIELDS * depth + 1) * depth > LANES:
        raise ValueError("block shape")
    wide, tall, short, long = nx + 2 * depth, ny + 2 * SUB, ny + SUB, nz + LANES
    table = table[None]
    any_spec = pl.BlockSpec(memory_space=pl.ANY)
    vmem = pl.BlockSpec(memory_space=pltpu.VMEM)
    f32 = jnp.float32
    both = pl.pallas_call(
        functools.partial(kernel, counts),
        out_shape=pltpu.VMEM((2,) + warm.shape, jnp.float32),
        in_specs=[any_spec] * 5,
        out_specs=vmem,
        scratch_shapes=[
            pltpu.VMEM((2, wide, tall, long), f32),
            pltpu.VMEM((wide, short, long), f32),
            pltpu.VMEM((wide, short, long), f32),
            pltpu.VMEM((ITERS + 1, wide, short, long), f32),
            pltpu.VMEM((wide, short, long), f32),
            pltpu.VMEM((wide, short, long), f32),
            pltpu.VMEM((wide, short, long), f32),
            pltpu.VMEM((3, short, long), f32),
            pltpu.VMEM((SUB, LANES), f32),
            pltpu.VMEM(table.shape, f32),
            pltpu.VMEM((nx, ny, nz), f32),
            pltpu.VMEM((2, nx, ny, nz), jnp.int32),
            pltpu.VMEM((2, BOTH, ny, nz), f32),
            pltpu.VMEM((2, BOTH + 2, tall, nz), f32),
            pltpu.VMEM((16 * nx * ny, LANES), f32),
            pltpu.VMEM((2, 1, LANES), f32),
            pltpu.VMEM((plane, 1, LANES), f32),
            pltpu.VMEM((line, 1, LANES), f32),
            pltpu.VMEM((plane * line, 1, LANES), f32),
            pltpu.SemaphoreType.DMA((2,)),
            pltpu.SemaphoreType.DMA((1,)),
            pltpu.SemaphoreType.DMA((3,)),
            pltpu.SemaphoreType.DMA((2,)),
            pltpu.SemaphoreType.DMA((2,)),
            pltpu.SemaphoreType.REGULAR,
            pltpu.SemaphoreType.REGULAR,
        ],
        compiler_params=pltpu.CompilerParams(collective_id=0, has_side_effects=True),
    )(warm, source, category, table, flags)
    return both[0], both[1]


def solution(mesh):
    counts = tuple(mesh.shape[a] for a in AXES)
    spec = P("gx", "gy", "gz")
    return jax.shard_map(
        functools.partial(body, counts),
        mesh=mesh,
        in_specs=(spec, spec, spec, P(), spec),
        out_specs=(spec, spec),
        check_vma=False,
    )
```

```python
import functools

import jax
import jax.numpy as jnp
from jax import lax
from jax.experimental import pallas as pl
from jax.experimental.pallas import tpu as pltpu
from jax.sharding import PartitionSpec as P

ITERS = 4
interval_delta = 2.0
cooling = 3.0

MESH = pl.DeviceIdType.MESH
AXES = ("gx", "gy", "gz")
SUB = 8
REACH = 4
LANES = 128
FIELDS = 4
DEPTH = ITERS + 1
BOTH = 2
MOMENTS = 2 * ITERS
REGIONS = [(a, c) for c in (0, 1, -1) for a in (0, 1, -1)]


def tiles_of(values):
    return [values[r : r + SUB] for r in range(0, values.shape[0], SUB)]


def smooth_y(values):
    tiles = tiles_of(values)
    after = tiles[1:] + [pltpu.roll(tiles[0], SUB - 1, 0)]
    pairs = [a + b for a, b in zip(tiles, after)]
    before = [pltpu.roll(pairs[-1], 1, 0)] + pairs[:-1]
    return jnp.concatenate([a + b for a, b in zip(before, pairs)], axis=0)


def smooth_rows(pieces):
    pairs = [a + b for a, b in zip(pieces, pieces[1:])]
    return jnp.concatenate([a + b for a, b in zip(pairs, pairs[1:])], axis=0)


def smooth_z(values):
    size = values.shape[1]
    return (values + values) + (pltpu.roll(values, 1, 1) + pltpu.roll(values, size - 1, 1))


def smooth_z_own(values):
    size = values.shape[1] // 2
    main, side = values[:, :size], values[:, size:]
    lane = lax.broadcasted_iota(jnp.int32, main.shape, 1)
    before = pltpu.roll(jnp.where(lane == size - 1, side, main), 1, 1)
    after = pltpu.roll(jnp.where(lane == 0, side, main), size - 1, 1)
    return (main + main) + (before + after)


def kernel(
    counts,
    warm_in,
    source_in,
    category_in,
    table_in,
    flags_in,
    both_out,
    pair,
    side_pair,
    push_in,
    cool,
    side_push,
    side_cool,
    basis,
    spread,
    diag,
    couple,
    masks,
    row_mask,
    natural,
    natural_own,
    table,
    table_row,
    source,
    ints,
    edges,
    beside,
    ledger,
    row_out,
    plane_rows,
    line_rows,
    all_rows,
    load_sems,
    halo_send,
    halo_recv,
    row_send,
    row_recv,
    near,
    far,
):
    plane, line = counts[0] * counts[1], counts[2]
    nx, ny, nz = both_out.shape[1:]
    depth = DEPTH
    wide, tall = pair.shape[1:3]
    long = 2 * nz
    short = ny + SUB
    leap = short // SUB
    tail = nx - depth
    direct = max(counts) <= REACH
    here = [lax.axis_index(a) for a in AXES]
    in_plane = here[0] * counts[1] + here[1]

    def exists(offset):
        good = None
        for k in range(3):
            if offset[k] > 0:
                one = here[k] < counts[k] - offset[k]
            elif offset[k] < 0:
                one = here[k] >= -offset[k]
            else:
                continue
            good = one if good is None else jnp.logical_and(good, one)
        return good

    def at(offset):
        return {a: here[k] + offset[k] for k, a in enumerate(AXES)}

    def back(offset):
        return tuple(-o for o in offset)

    def signal(semaphore, offset):
        @pl.when(exists(offset))
        def _():
            pl.semaphore_signal(semaphore, inc=1, device_id=at(offset), device_id_type=MESH)

    def present(offsets):
        return sum(jnp.where(exists(offset), 1, 0) for offset in offsets)

    plane_targets = [
        {"gx": other // counts[1], "gy": other % counts[1], "gz": here[2]}
        for other in [(in_plane + step) % plane for step in range(1, plane)]
    ]
    line_targets = [
        {"gx": here[0], "gy": here[1], "gz": (here[2] + step) % line} for step in range(1, line)
    ]
    def others(k):
        size = counts[k]
        far_side = here[k] >= (size + 1) // 2
        place = jnp.where(far_side, size - 1 - here[k], here[k])
        steps = [(size - 1 - u, size - 1 - u) for u in range(size // 2)]
        spots = [jnp.where(far_side, size - 1 - u, u) for u, _ in steps]
        weights = [w for _, w in steps]
        for step in range(1, size - size // 2):
            u = (place + step) % (size - size // 2)
            spots.append(jnp.where(far_side, size - 1 - u, u))
            weights.append(0.5)
        return list(zip(spots, weights)) + [(here[k], 0)]

    moved_by = [others(k) for k in range(3)]
    links = (0.5, 1.0, 1.0)
    ranked = [
        (sum(g * (m[1] > 0.5 or k > 0) * m[1] for k, (g, m) in enumerate(zip(links, spot))), n, spot)
        for n, spot in enumerate(
            (x, y, z) for x in moved_by[0] for y in moved_by[1] for z in moved_by[2]
        )
        if any(m[1] for m in spot)
    ]
    all_targets = [
        {a: spot[k][0] for k, a in enumerate(AXES)}
        for _, _, spot in sorted(ranked, key=lambda item: (-item[0], item[1]))
    ]

    regions = [r for r in REGIONS if abs(r[0]) < counts[0] and abs(r[1]) < counts[2]]

    def by_class(act):
        if counts[1] == 1:
            act((0,))
            return
        pl.when(here[1] == 0)(lambda: act((0, 1)))
        pl.when(here[1] == counts[1] - 1)(lambda: act((0, -1)))
        if counts[1] > 2:
            inner = jnp.logical_and(here[1] > 0, here[1] < counts[1] - 1)
            pl.when(inner)(lambda: act((0, 1, -1)))

    def guard(region, act):
        if region == (0, 0):
            act()
        else:
            pl.when(exists((region[0], 0, region[1])))(act)

    def ways_of(region, steps):
        ways = [(region[0], step, region[1]) for step in sorted(steps, key=lambda v: -abs(v))]
        return [way for way in ways if any(way)]

    def neighbours():
        total = 0
        for region in regions:
            here_too = 1 if region == (0, 0) else jnp.where(exists((region[0], 0, region[1])), 1, 0)
            beside_y = present([(0, 1, 0), (0, -1, 0)]) if counts[1] > 1 else 0
            total = total + here_too * (beside_y + (0 if region == (0, 0) else 1))
        return total

    def signal_all(semaphore):
        def act(steps):
            for region in sorted(regions, key=lambda r: (-abs(r[0]), -abs(r[1]))):

                def go(region=region):
                    for way in ways_of(region, steps):
                        pl.semaphore_signal(semaphore, inc=1, device_id=at(way), device_id_type=MESH)

                guard(region, go)

        by_class(act)

    barrier = pltpu.get_barrier_semaphore()
    signal_all(barrier)
    if not direct:
        for target in plane_targets + line_targets:
            pl.semaphore_signal(barrier, inc=1, device_id=target, device_id_type=MESH)

    own = (pl.ds(depth, nx), pl.ds(depth, ny))
    loads = [
        pltpu.make_async_copy(table_in, table_row, load_sems.at[0]),
        pltpu.make_async_copy(category_in, ints.at[0], load_sems.at[1]),
        pltpu.make_async_copy(flags_in, ints.at[1], load_sems.at[1]),
        pltpu.make_async_copy(warm_in, pair.at[(0,) + own], load_sems.at[1]),
        pltpu.make_async_copy(source_in, source, load_sems.at[1]),
    ]
    for load in loads:
        load.start()

    def clear(ref, *index):
        shape = ref.at[index].shape
        ref[index] = jnp.zeros(shape, jnp.float32)

    table[...] = jnp.zeros(table.shape, jnp.float32)
    everything = slice(None)
    for way, planes, slots in (
        ((-1, 0, 0), slice(0, depth), 0),
        ((1, 0, 0), slice(depth + nx, wide), 1 + BOTH),
    ):

        @pl.when(jnp.logical_not(exists(way)))
        def _():
            for f in range(2):
                clear(pair, f, planes)
            clear(push_in, planes)
            clear(cool, planes)
            for side in range(2):
                clear(beside, side, slots)

    for way, rows, few in (
        ((0, 1, 0), slice(depth + ny, 2 * depth + ny), slice(ITERS + ny, short)),
        ((0, -1, 0), slice(0, depth), slice(0, ITERS)),
    ):

        @pl.when(jnp.logical_not(exists(way)))
        def _():
            for f in range(2):
                clear(pair, f, everything, rows)
            clear(push_in, everything, few)
            clear(cool, everything, few)
            for side in range(2):
                clear(beside, side, everything, rows)

    for side, way in enumerate(((0, 0, -1), (0, 0, 1))):

        @pl.when(jnp.logical_not(exists(way)))
        def _():
            clear(beside, side)

    row_index = lax.broadcasted_iota(jnp.int32, (short, long), 0)
    y_index = leap * (row_index % SUB) + row_index // SUB - ITERS
    z_index = lax.broadcasted_iota(jnp.int32, (short, long), 1)
    y_low = jnp.logical_or(y_index >= 0, here[1] > 0)
    y_high = jnp.logical_or(y_index < ny, here[1] < counts[1] - 1)
    z_low = jnp.logical_or(z_index < nz + LANES // 2, here[2] > 0)
    z_far = jnp.logical_or(z_index < nz, z_index >= nz + LANES // 2)
    z_high = jnp.logical_or(z_far, here[2] < counts[2] - 1)
    y_good, z_good = jnp.logical_and(y_low, y_high), jnp.logical_and(z_low, z_high)
    within = jnp.where(jnp.logical_and(y_good, z_good), 1.0, 0.0)
    y_own = jnp.logical_and(y_index >= 0, y_index < ny)[:, :nz]
    row_mask[...] = jnp.where(y_own, 1.0, 0.0)
    masks[0] = jnp.where(here[0] > 0, 1.0, 0.0) * within
    masks[1] = within
    masks[2] = jnp.where(here[0] < counts[0] - 1, 1.0, 0.0) * within

    def inside(i):
        return masks[0 if i < depth else 2 if i >= depth + nx else 1]

    loads[0].wait()
    table[0:1, 0 : table_in.shape[1]] = table_row[...]
    most = 7.0 + 24.0 * jnp.max(table[0:1, :], axis=1, keepdims=True)
    high, low = most, jnp.ones_like(most)
    middle = 0.5 * (high + low)
    half = 0.5 * (high - low)
    twice = 2.0 / half
    quarter = 0.125 * interval_delta
    lookup = jnp.broadcast_to(table[0:1, :], (ny, LANES))
    lane = lax.broadcasted_iota(jnp.int32, (ny, LANES), 1)

    every = ledger.at[pl.ds(0, 4 * nx * ny)]
    pltpu.make_async_copy(every, every, load_sems.at[1]).wait()
    packed = [[None, None], [None, None]]
    for i in range(nx):
        cond = jnp.take_along_axis(lookup, ints[0, i], axis=1)
        flag = ints[1, i].astype(jnp.float32)
        warm = pair[0, depth + i, depth : depth + ny, :]
        push = interval_delta * source[i] - (interval_delta * cooling) * flag * warm
        push = twice * push
        pair[1, depth + i, depth : depth + ny, :] = cond
        cool[depth + i, ITERS : ITERS + ny, :] = flag
        push_in[depth + i, ITERS : ITERS + ny, :] = push
        for g, start in enumerate((0, tail)):
            if not 0 <= i - start < depth:
                continue
            for f, piece in enumerate((warm, cond, push, flag)):
                at_lane = ((i - start) * FIELDS + f) * depth
                turned = pltpu.roll(piece, at_lane + depth, 1)
                for side in range(2):
                    old = packed[side][g]
                    if old is not None:
                        turned_in = jnp.where(lane >= at_lane + side * depth, turned, old)
                    else:
                        turned_in = turned
                    packed[side][g] = turned_in
    for side in range(2):
        for g in range(BOTH):
            edges[side, g] = packed[side][g]

    waits = neighbours()
    if not direct:
        waits = waits + (plane + line - 2)
    pl.semaphore_wait(barrier, waits)

    def y_span(step, reach, source_base, base):
        if step == 0:
            return pl.ds(source_base, ny), pl.ds(base, ny)
        if step > 0:
            return pl.ds(source_base + ny - reach, reach), pl.ds(base - reach, reach)
        return pl.ds(source_base, reach), pl.ds(base + ny, reach)

    def x_span(step, reach):
        if step == 0:
            return pl.ds(depth, nx), pl.ds(depth, nx)
        if step > 0:
            return pl.ds(depth + nx - reach, reach), pl.ds(depth - reach, reach)
        return pl.ds(depth, reach), pl.ds(depth + nx, reach)

    def send(src, dst, way, stage):
        pltpu.make_async_remote_copy(
            src_ref=src,
            dst_ref=dst,
            send_sem=halo_send.at[0],
            recv_sem=halo_recv.at[stage],
            device_id=at(way),
            device_id_type=MESH,
        ).start()

    def send_field(ref, way, reach, base, stage):
        src_x, dst_x = x_span(way[0], reach)
        src_y, dst_y = y_span(way[1], reach, base, base)
        send(ref.at[src_x, src_y], ref.at[dst_x, dst_y], way, stage)

    def send_cond(way):
        send_field(pair.at[1], way, depth, depth, 0)

    def send_warm(way):
        send_field(pair.at[0], way, depth, depth, 1)

    def send_rest(way):
        send_field(push_in, way, depth - 1, ITERS, 2)
        send_field(cool, way, depth - 2, ITERS, 2)

    def send_edges(way):
        if way[0] == 0:
            src_x, dst_x = pl.ds(0, BOTH), pl.ds(1, BOTH)
        elif way[0] > 0:
            src_x, dst_x = pl.ds(1, 1), pl.ds(0, 1)
        else:
            src_x, dst_x = pl.ds(0, 1), pl.ds(1 + BOTH, 1)
        src_y, dst_y = y_span(way[1], depth, 0, depth)
        side = 0 if way[2] > 0 else 1
        send(edges.at[side, src_x, src_y], beside.at[side, dst_x, dst_y], way, 0)

    def send_all(steps):
        steps_on = tuple(v for v in steps if v)
        sides = [r for r in regions if r[0] and not r[1]]
        depths = sorted([r for r in regions if r[1]], key=lambda r: -abs(r[0]))
        plan = [(r, steps, (send_edges,)) for r in depths]
        for action in (send_cond, send_warm, send_rest):
            plan += [((0, 0), steps_on, (action,))] + [(r, steps, (action,)) for r in sides]
        for region, some, actions in plan:

            def go(region=region, some=some, actions=actions):
                for action in actions:
                    for way in ways_of(region, some):
                        action(way)

            if ways_of(region, some):
                guard(region, go)

    by_class(send_all)

    def x_rows(step, reach):
        return reach if step else nx

    def y_rows(step, reach):
        return reach if step else ny

    def moved_rows(way, kind):
        if kind == 3:
            return (1 if way[0] else BOTH) * y_rows(way[1], depth)
        reaches = ((depth,), (depth,), (depth - 1, depth - 2))[kind]
        return sum(x_rows(way[0], r) * y_rows(way[1], r) for r in reaches)

    def sides_of(k):
        if counts[k] == 1:
            return [(None, 0)]
        edge = jnp.logical_or(here[k] == 0, here[k] == counts[k] - 1)
        if counts[k] == 2:
            return [(None, 1)]
        return [(edge, 1), (jnp.logical_not(edge), 2)]

    def wait_all(kinds, semaphore, receive):
        def wait(sides):
            rows = 0
            for way in [(a, b, c) for a in (0, 1) for b in (0, 1) for c in (0, 1)]:
                times = 1
                for step, some in zip(way, sides):
                    times = times * (some if step else 1)
                for kind in kinds:
                    if any(way) and (kind == 3) == bool(way[2]):
                        rows = rows + times * moved_rows(way, kind)
            if rows == 0:
                return
            whole = pltpu.make_async_remote_copy(
                src_ref=ledger.at[pl.ds(0, rows)],
                dst_ref=ledger.at[pl.ds(0, rows)],
                send_sem=semaphore,
                recv_sem=semaphore,
                device_id=all_targets[0],
                device_id_type=MESH,
            )
            if receive:
                whole.wait_recv()
            else:
                whole.wait_send()

        for x_good, x_some in sides_of(0):
            for y_good, y_some in sides_of(1):
                for z_good, z_some in sides_of(2):
                    good = None
                    for one in (x_good, y_good, z_good):
                        if one is not None:
                            good = one if good is None else jnp.logical_and(good, one)
                    act = functools.partial(wait, (x_some, y_some, z_some))
                    if good is None:
                        act()
                    else:
                        pl.when(good)(act)

    if direct:
        signal_all(near)
        hops = [(a, 0, c) for a in (0, 2, -2) for c in (0, 2, -2) if a or c]
        hops = [h for h in hops if abs(h[0]) < counts[0] and abs(h[2]) < counts[2]]
        pl.semaphore_wait(near, neighbours())
        for hop in hops:
            signal(far, hop)

    def share(stage, rows_ref, slot, targets):
        for target in targets:
            pltpu.make_async_remote_copy(
                src_ref=row_out.at[stage],
                dst_ref=rows_ref.at[slot],
                send_sem=row_send.at[stage],
                recv_sem=row_recv.at[stage],
                device_id=target,
                device_id_type=MESH,
            ).start()

    def share_wait(stage, rows_ref, targets):
        if targets:
            whole = pltpu.make_async_remote_copy(
                src_ref=rows_ref.at[pl.ds(0, len(targets))],
                dst_ref=rows_ref.at[pl.ds(0, len(targets))],
                send_sem=row_send.at[stage],
                recv_sem=row_recv.at[stage],
                device_id=targets[0],
                device_id_type=MESH,
            )
            whole.wait_send()
            whole.wait_recv()

    wait_all((0, 3), halo_recv.at[0], True)

    tall_lane = lax.broadcasted_iota(jnp.int32, (tall, LANES), 1)

    places = [(0, j) for j in range(depth)]
    places += [(1, p) if p < depth else (2, p - tail) for p in range(nx)]
    places += [(1 + BOTH, j) for j in range(depth)]

    def unpack(fields):
        for i, (g, slot) in enumerate(places):
            for f in fields:
                spare = (0, 0, 1, 2)[f]
                if not spare <= i < wide - spare:
                    continue
                cut = (slot * FIELDS + f + 1) * depth
                if f < 2:
                    kept = jnp.where(tall_lane < cut, beside[0, g], beside[1, g])
                    side_pair[f, i] = pltpu.roll(kept, LANES - cut, 1)
                    continue
                ref = side_push if f == 2 else side_cool
                for t in range(leap):
                    rows = pl.ds(1 + t, SUB, stride=leap)
                    kept = jnp.where(tall_lane[:SUB] < cut, beside[0, g, rows, :], beside[1, g, rows, :])
                    ref[i, t * SUB : (t + 1) * SUB, :] = pltpu.roll(kept, LANES - cut, 1)

    unpack((1, 0))

    def pieces_of(f, i, first, some):
        pieces = []
        for j in range(first, first + some):
            rows = pl.ds(j, SUB, stride=leap)
            pieces.append(jnp.concatenate([pair[f, i, rows, :], side_pair[f, i, rows, :]], axis=1))
        return pieces

    def middle_of(f, i):
        return jnp.concatenate(pieces_of(f, i, 1, leap), axis=0)

    def joined(main, side, i):
        rows = [main[i, pl.ds(t, SUB, stride=leap), :] for t in range(leap)]
        return jnp.concatenate([jnp.concatenate(rows, axis=0), side[i]], axis=1)

    def along_x(least, most, planes_of, use):
        before = sums = None
        for i in range(least, most):
            now = planes_of(i)
            if i > least:
                joined = [a + b for a, b in zip(before, now)]
                if sums is not None:
                    use(i - 1, *[a + b for a, b in zip(sums, joined)])
                sums = joined
            before = now

    def ring_of(i):
        return (smooth_z(smooth_rows(pieces_of(1, i, 0, leap + 2))),)

    def use_ring(i, ring):
        cond = middle_of(1, i)
        base = twice * (8.0 * interval_delta * cond + quarter * ring)
        spread[i] = base
        couple[i] = (quarter * twice) * cond

    along_x(0, wide, ring_of, use_ring)
    unpack((2, 3))

    wait_all((1,), halo_recv.at[1], True)

    totals = [None] * MOMENTS

    def gather(n, a, b):
        part = sum(tiles_of(a * b))
        totals[n] = part if totals[n] is None else totals[n] + part

    def core(v):
        return v[:, :nz]

    def warm_of(i):
        warm = pieces_of(0, i, 0, leap + 2)
        cond = pieces_of(1, i, 0, leap + 2)
        warm_flux = [(quarter * twice) * (a * b) for a, b in zip(warm, cond)]
        return smooth_z(smooth_rows(warm)), smooth_z(smooth_rows(warm_flux))

    def use_warm(i, ring, push):
        edge = couple[i]
        image = spread[i] * middle_of(0, i) - (edge * ring + inside(i) * push)
        basis[0, i] = image

    along_x(0, wide, warm_of, use_warm)

    wait_all((2,), halo_recv.at[2], True)

    for k in range(ITERS - 1):

        def level_of(i, k=k):
            mid = basis[k, i]
            if k == 0:
                mid = joined(push_in, side_push, i) - mid
                basis[0, i] = mid
                if depth <= i < depth + nx:
                    gather(0, row_mask[...] * core(mid), core(mid))
            return smooth_z(smooth_y(mid)), smooth_z(smooth_y(couple[i] * mid))

        def use_level(i, ring, push, k=k):
            edge = couple[i]
            mid = basis[k, i]
            if k == 0:
                main = spread[i] + twice * ((1.0 - middle) + interval_delta * cooling * joined(cool, side_cool, i))
                diag[i] = main
            else:
                main = diag[i]
            fresh = main * mid - (edge * ring + inside(i) * push)
            if k > 0:
                fresh = fresh - basis[k - 1, i]
            basis[k + 1, i] = fresh
            if depth <= i < depth + nx:
                kept = row_mask[...] * core(fresh)
                gather(2 * k + 1, core(mid), kept)
                gather(2 * k + 2, core(fresh), kept)

        along_x(k + 1, wide - k - 1, level_of, use_level)

    k = ITERS - 1

    def last_of(i):
        mid = basis[k, i]
        return smooth_z_own(smooth_y(mid)), smooth_z_own(smooth_y(couple[i] * mid))

    def use_last(i, ring, push):
        mid = core(basis[k, i])
        fresh = core(diag[i]) * mid - (core(couple[i]) * ring + push)
        fresh = fresh - core(basis[k - 1, i])
        basis[k + 1, i, :, 0:nz] = fresh
        gather(2 * k + 1, row_mask[...] * mid, fresh)

    along_x(depth - 1, depth + nx + 1, last_of, use_last)

    diagonal = lax.broadcasted_iota(jnp.int32, (SUB, LANES), 0)
    across = lax.broadcasted_iota(jnp.int32, (SUB, LANES), 1)
    tile = jnp.zeros((SUB, LANES), jnp.float32)
    for n in range(MOMENTS):
        tile = jnp.where(diagonal == n, jnp.sum(totals[n], axis=0, keepdims=True), tile)
    column = jnp.sum(tile, axis=1, keepdims=True)
    row = jnp.sum(jnp.where(across == diagonal, column, 0.0), axis=0, keepdims=True)
    if direct:
        pl.semaphore_wait(far, present(back(h) for h in hops))
    row_out[0] = row

    def settle():
        wait_all((0, 1, 2, 3), halo_send.at[0], False)
        for n in range(ITERS + 1):
            for i in range(nx):
                for t in range(leap):
                    tile = basis[n, depth + i, t * SUB : (t + 1) * SUB, 0:nz]
                    natural[n, i, pl.ds(t, SUB, stride=leap), :] = tile
        for n in range(ITERS + 1):
            for i in range(nx):
                natural_own[n, i] = natural[n, i, ITERS : ITERS + ny, :]
        for i in range(nx):
            natural_own[ITERS + 1, i] = pair[0, depth + i, depth : depth + ny, :]

    if direct:
        mine = in_plane * line + here[2]
        all_rows[mine] = row
        share(0, all_rows, mine, all_targets)
        settle()
        share_wait(0, all_rows, all_targets)
        row = jnp.sum(all_rows[...], axis=0)
    else:
        plane_rows[in_plane] = row
        share(0, plane_rows, in_plane, plane_targets)
        settle()
        share_wait(0, plane_rows, plane_targets)
        row = jnp.sum(plane_rows[...], axis=0)
        row_out[1] = row
        line_rows[here[2]] = row
        share(1, line_rows, here[2], line_targets)
        share_wait(1, line_rows, line_targets)
        row = jnp.sum(line_rows[...], axis=0)
    row_lane = lax.broadcasted_iota(jnp.int32, (1, LANES), 1)
    gram = {}
    for n in range(MOMENTS):
        value = jnp.sum(jnp.where(row_lane == n, row, 0.0), axis=1, keepdims=True)
        gram[n // 2, (n + 1) // 2] = value
    for gap in range(2, ITERS + 1):
        for i in range(ITERS + 1 - gap):
            j = i + gap
            value = gram[i + 1, j - 1] - gram[i, j - 2]
            if i > 0:
                value = value + gram[i - 1, j - 1]
            gram[i, j] = value
    for i, j in list(gram):
        gram[j, i] = gram[i, j]

    def apply(p):
        q = [middle * a for a in p] + [jnp.zeros_like(half)]
        for i, a in enumerate(p):
            q[i + 1] = q[i + 1] + (0.5 * half) * a
            if i > 0:
                q[i - 1] = q[i - 1] + (0.5 * half) * a
        return q

    def product(p, q):
        value = None
        for i, a in enumerate(p):
            inner = None
            for j, b in enumerate(q):
                term = gram[i, j] * b
                inner = term if inner is None else inner + term
            inner = a * inner
            value = inner if value is None else value + inner
        return value

    left = [0.5 * half]
    heading = list(left)
    moved = []
    norm = product(left, left)
    for step in range(ITERS):
        image = apply(heading)
        alpha = norm / product(heading, image)
        moved = [a + alpha * b for a, b in zip(moved, heading)] + [
            alpha * b for b in heading[len(moved) :]
        ]
        left = [a - alpha * b for a, b in zip(left, image)] + [
            -alpha * b for b in image[len(left) :]
        ]
        if step + 1 < ITERS:
            following = product(left, left)
            ratio = following / norm
            heading = [a + ratio * b for a, b in zip(left, heading)] + left[len(heading) :]
            norm = following

    for i in range(nx):
        warm = natural_own[ITERS + 1, i]
        end = jnp.zeros_like(warm)
        for k in range(ITERS + 1):
            value = natural_own[k, i]
            if k < ITERS:
                warm = warm + moved[k] * value
            end = end + left[k] * value
        both_out[0, i] = warm
        both_out[1, i] = end


def body(counts, warm, source, category, table, flags):
    nx, ny, nz = warm.shape
    depth = DEPTH
    plane, line = counts[0] * counts[1], counts[2]
    if nx < depth or nx % 2 or ny % SUB or nz != LANES or table.shape[0] > LANES:
        raise ValueError("block shape")
    if nx > 2 * depth or (FIELDS * depth + 1) * depth > LANES:
        raise ValueError("block shape")
    wide, tall, short, long = nx + 2 * depth, ny + 2 * SUB, ny + SUB, nz + LANES
    table = table[None]
    any_spec = pl.BlockSpec(memory_space=pl.ANY)
    vmem = pl.BlockSpec(memory_space=pltpu.VMEM)
    f32 = jnp.float32
    both = pl.pallas_call(
        functools.partial(kernel, counts),
        out_shape=pltpu.VMEM((2,) + warm.shape, jnp.float32),
        in_specs=[any_spec] * 5,
        out_specs=vmem,
        scratch_shapes=[
            pltpu.VMEM((2, wide, tall, nz), f32),
            pltpu.VMEM((2, wide, tall, nz), f32),
            pltpu.VMEM((wide, short, nz), f32),
            pltpu.VMEM((wide, short, nz), f32),
            pltpu.VMEM((wide, short, nz), f32),
            pltpu.VMEM((wide, short, nz), f32),
            pltpu.VMEM((ITERS + 1, wide, short, long), f32),
            pltpu.VMEM((wide, short, long), f32),
            pltpu.VMEM((wide, short, long), f32),
            pltpu.VMEM((wide, short, long), f32),
            pltpu.VMEM((3, short, long), f32),
            pltpu.VMEM((short, nz), f32),
            pltpu.VMEM((ITERS + 1, nx, short, nz), f32),
            pltpu.VMEM((ITERS + 2, nx, ny, nz), f32),
            pltpu.VMEM((SUB, LANES), f32),
            pltpu.VMEM(table.shape, f32),
            pltpu.VMEM((nx, ny, nz), f32),
            pltpu.VMEM((2, nx, ny, nz), jnp.int32),
            pltpu.VMEM((2, BOTH, ny, nz), f32),
            pltpu.VMEM((2, BOTH + 2, tall, nz), f32),
            pltpu.VMEM((16 * nx * ny, LANES), f32),
            pltpu.VMEM((2, 1, LANES), f32),
            pltpu.VMEM((plane, 1, LANES), f32),
            pltpu.VMEM((line, 1, LANES), f32),
            pltpu.VMEM((plane * line, 1, LANES), f32),
            pltpu.SemaphoreType.DMA((2,)),
            pltpu.SemaphoreType.DMA((1,)),
            pltpu.SemaphoreType.DMA((3,)),
            pltpu.SemaphoreType.DMA((2,)),
            pltpu.SemaphoreType.DMA((2,)),
            pltpu.SemaphoreType.REGULAR,
            pltpu.SemaphoreType.REGULAR,
        ],
        compiler_params=pltpu.CompilerParams(collective_id=0, has_side_effects=True),
    )(warm, source, category, table, flags)
    return both[0], both[1]


def solution(mesh):
    counts = tuple(mesh.shape[a] for a in AXES)
    spec = P("gx", "gy", "gz")
    return jax.shard_map(
        functools.partial(body, counts),
        mesh=mesh,
        in_specs=(spec, spec, spec, P(), spec),
        out_specs=(spec, spec),
        check_vma=False,
    )
```

```python
import functools

import jax
import jax.numpy as jnp
from jax import lax
from jax.experimental import pallas as pl
from jax.experimental.pallas import tpu as pltpu
from jax.sharding import PartitionSpec as P

ITERS = 4
interval_delta = 2.0
cooling = 3.0

MESH = pl.DeviceIdType.MESH
AXES = ("gx", "gy", "gz")
SUB = 8
REACH = 4
LANES = 128
FIELDS = 4
DEPTH = ITERS + 1
BOTH = 2
MOMENTS = 2 * ITERS
REGIONS = [(a, c) for c in (0, 1, -1) for a in (0, 1, -1)]


def tiles_of(values):
    return [values[r : r + SUB] for r in range(0, values.shape[0], SUB)]


def smooth_y(values):
    tiles = tiles_of(values)
    after = tiles[1:] + [pltpu.roll(tiles[0], SUB - 1, 0)]
    pairs = [a + b for a, b in zip(tiles, after)]
    before = [pltpu.roll(pairs[-1], 1, 0)] + pairs[:-1]
    return jnp.concatenate([a + b for a, b in zip(before, pairs)], axis=0)


def smooth_rows(pieces):
    pairs = [a + b for a, b in zip(pieces, pieces[1:])]
    return jnp.concatenate([a + b for a, b in zip(pairs, pairs[1:])], axis=0)


def beside_z(values):
    return pltpu.roll(values, 1, 1), pltpu.roll(values, values.shape[1] - 1, 1)


def beside_z_own(values):
    size = values.shape[1] // 2
    main, side = values[:, :size], values[:, size:]
    lane = lax.broadcasted_iota(jnp.int32, main.shape, 1)
    before = pltpu.roll(jnp.where(lane == size - 1, side, main), 1, 1)
    return before, pltpu.roll(jnp.where(lane == 0, side, main), size - 1, 1)


def smooth_z(values):
    before, after = beside_z(values)
    return (values + values) + (before + after)


def sums_z(values, around, edges):
    before, after = around
    twice = values + values
    own = twice + (before + after)
    return own, edges[0] * twice + (edges[1] * before + edges[2] * after)


def kernel(
    counts,
    warm_in,
    source_in,
    category_in,
    table_in,
    flags_in,
    both_out,
    pair,
    side_pair,
    push_in,
    cool,
    side_push,
    side_cool,
    basis,
    spread,
    diag,
    couples,
    masks,
    row_mask,
    natural,
    natural_own,
    table,
    table_row,
    source,
    ints,
    edges,
    beside,
    ledger,
    row_out,
    plane_rows,
    line_rows,
    all_rows,
    load_sems,
    halo_send,
    halo_recv,
    row_send,
    row_recv,
    near,
    far,
):
    plane, line = counts[0] * counts[1], counts[2]
    nx, ny, nz = both_out.shape[1:]
    depth = DEPTH
    wide, tall = pair.shape[1:3]
    long = 2 * nz
    short = ny + SUB
    leap = short // SUB
    tail = nx - depth
    direct = max(counts) <= REACH
    here = [lax.axis_index(a) for a in AXES]
    in_plane = here[0] * counts[1] + here[1]

    def exists(offset):
        good = None
        for k in range(3):
            if offset[k] > 0:
                one = here[k] < counts[k] - offset[k]
            elif offset[k] < 0:
                one = here[k] >= -offset[k]
            else:
                continue
            good = one if good is None else jnp.logical_and(good, one)
        return good

    def at(offset):
        return {a: here[k] + offset[k] for k, a in enumerate(AXES)}

    def back(offset):
        return tuple(-o for o in offset)

    def signal(semaphore, offset):
        @pl.when(exists(offset))
        def _():
            pl.semaphore_signal(semaphore, inc=1, device_id=at(offset), device_id_type=MESH)

    def present(offsets):
        return sum(jnp.where(exists(offset), 1, 0) for offset in offsets)

    plane_targets = [
        {"gx": other // counts[1], "gy": other % counts[1], "gz": here[2]}
        for other in [(in_plane + step) % plane for step in range(1, plane)]
    ]
    line_targets = [
        {"gx": here[0], "gy": here[1], "gz": (here[2] + step) % line} for step in range(1, line)
    ]
    def others(k):
        size = counts[k]
        far_side = here[k] >= (size + 1) // 2
        place = jnp.where(far_side, size - 1 - here[k], here[k])
        steps = [(size - 1 - u, size - 1 - u) for u in range(size // 2)]
        spots = [jnp.where(far_side, size - 1 - u, u) for u, _ in steps]
        weights = [w for _, w in steps]
        for step in range(1, size - size // 2):
            u = (place + step) % (size - size // 2)
            spots.append(jnp.where(far_side, size - 1 - u, u))
            weights.append(0.5)
        return list(zip(spots, weights)) + [(here[k], 0)]

    moved_by = [others(k) for k in range(3)]
    links = (0.5, 1.0, 1.0)
    ranked = [
        (sum(g * (m[1] > 0.5 or k > 0) * m[1] for k, (g, m) in enumerate(zip(links, spot))), n, spot)
        for n, spot in enumerate(
            (x, y, z) for x in moved_by[0] for y in moved_by[1] for z in moved_by[2]
        )
        if any(m[1] for m in spot)
    ]
    all_targets = [
        {a: spot[k][0] for k, a in enumerate(AXES)}
        for _, _, spot in sorted(ranked, key=lambda item: (-item[0], item[1]))
    ]

    regions = [r for r in REGIONS if abs(r[0]) < counts[0] and abs(r[1]) < counts[2]]

    def by_class(act):
        if counts[1] == 1:
            act((0,))
            return
        pl.when(here[1] == 0)(lambda: act((0, 1)))
        pl.when(here[1] == counts[1] - 1)(lambda: act((0, -1)))
        if counts[1] > 2:
            inner = jnp.logical_and(here[1] > 0, here[1] < counts[1] - 1)
            pl.when(inner)(lambda: act((0, 1, -1)))

    def guard(region, act):
        if region == (0, 0):
            act()
        else:
            pl.when(exists((region[0], 0, region[1])))(act)

    def ways_of(region, steps):
        ways = [(region[0], step, region[1]) for step in sorted(steps, key=lambda v: -abs(v))]
        return [way for way in ways if any(way)]

    def neighbours():
        total = 0
        for region in regions:
            here_too = 1 if region == (0, 0) else jnp.where(exists((region[0], 0, region[1])), 1, 0)
            beside_y = present([(0, 1, 0), (0, -1, 0)]) if counts[1] > 1 else 0
            total = total + here_too * (beside_y + (0 if region == (0, 0) else 1))
        return total

    def signal_all(semaphore):
        def act(steps):
            for region in sorted(regions, key=lambda r: (-abs(r[0]), -abs(r[1]))):

                def go(region=region):
                    for way in ways_of(region, steps):
                        pl.semaphore_signal(semaphore, inc=1, device_id=at(way), device_id_type=MESH)

                guard(region, go)

        by_class(act)

    barrier = pltpu.get_barrier_semaphore()
    signal_all(barrier)
    if not direct:
        for target in plane_targets + line_targets:
            pl.semaphore_signal(barrier, inc=1, device_id=target, device_id_type=MESH)

    own = (pl.ds(depth, nx), pl.ds(depth, ny))
    loads = [
        pltpu.make_async_copy(table_in, table_row, load_sems.at[0]),
        pltpu.make_async_copy(category_in, ints.at[0], load_sems.at[1]),
        pltpu.make_async_copy(flags_in, ints.at[1], load_sems.at[1]),
        pltpu.make_async_copy(warm_in, pair.at[(0,) + own], load_sems.at[1]),
        pltpu.make_async_copy(source_in, source, load_sems.at[1]),
    ]
    for load in loads:
        load.start()

    def clear(ref, *index):
        shape = ref.at[index].shape
        ref[index] = jnp.zeros(shape, jnp.float32)

    table[...] = jnp.zeros(table.shape, jnp.float32)
    everything = slice(None)
    for way, planes, slots in (
        ((-1, 0, 0), slice(0, depth), 0),
        ((1, 0, 0), slice(depth + nx, wide), 1 + BOTH),
    ):

        @pl.when(jnp.logical_not(exists(way)))
        def _():
            for f in range(2):
                clear(pair, f, planes)
            clear(push_in, planes)
            clear(cool, planes)
            for side in range(2):
                clear(beside, side, slots)

    for way, rows, few in (
        ((0, 1, 0), slice(depth + ny, 2 * depth + ny), slice(ITERS + ny, short)),
        ((0, -1, 0), slice(0, depth), slice(0, ITERS)),
    ):

        @pl.when(jnp.logical_not(exists(way)))
        def _():
            for f in range(2):
                clear(pair, f, everything, rows)
            clear(push_in, everything, few)
            clear(cool, everything, few)
            for side in range(2):
                clear(beside, side, everything, rows)

    for side, way in enumerate(((0, 0, -1), (0, 0, 1))):

        @pl.when(jnp.logical_not(exists(way)))
        def _():
            clear(beside, side)

    row_index = lax.broadcasted_iota(jnp.int32, (short, long), 0)
    y_index = leap * (row_index % SUB) + row_index // SUB - ITERS
    z_index = lax.broadcasted_iota(jnp.int32, (short, long), 1)
    y_low = jnp.logical_or(y_index >= 0, here[1] > 0)
    y_high = jnp.logical_or(y_index < ny, here[1] < counts[1] - 1)
    z_low = jnp.logical_or(z_index < nz + LANES // 2, here[2] > 0)
    z_far = jnp.logical_or(z_index < nz, z_index >= nz + LANES // 2)
    z_high = jnp.logical_or(z_far, here[2] < counts[2] - 1)
    y_good, z_good = jnp.logical_and(y_low, y_high), jnp.logical_and(z_low, z_high)
    within = jnp.where(jnp.logical_and(y_good, z_good), 1.0, 0.0)
    y_own = jnp.logical_and(y_index >= 0, y_index < ny)[:, :nz]
    row_mask[...] = jnp.where(y_own, 1.0, 0.0)
    masks[0] = jnp.where(here[0] > 0, 1.0, 0.0) * within
    masks[1] = within
    masks[2] = jnp.where(here[0] < counts[0] - 1, 1.0, 0.0) * within

    def inside(i):
        return masks[0 if i < depth else 2 if i >= depth + nx else 1]

    loads[0].wait()
    table[0:1, 0 : table_in.shape[1]] = table_row[...]
    most = 7.0 + 24.0 * jnp.max(table[0:1, :], axis=1, keepdims=True)
    high, low = most, jnp.ones_like(most)
    middle = 0.5 * (high + low)
    half = 0.5 * (high - low)
    twice = 2.0 / half
    quarter = 0.125 * interval_delta
    lookup = jnp.broadcast_to(table[0:1, :], (ny, LANES))
    lane = lax.broadcasted_iota(jnp.int32, (ny, LANES), 1)

    every = ledger.at[pl.ds(0, 4 * nx * ny)]
    pltpu.make_async_copy(every, every, load_sems.at[1]).wait()
    packed = [[None, None], [None, None]]
    for i in range(nx):
        cond = jnp.take_along_axis(lookup, ints[0, i], axis=1)
        flag = ints[1, i].astype(jnp.float32)
        warm = pair[0, depth + i, depth : depth + ny, :]
        push = interval_delta * source[i] - (interval_delta * cooling) * flag * warm
        push = twice * push
        pair[1, depth + i, depth : depth + ny, :] = cond
        cool[depth + i, ITERS : ITERS + ny, :] = flag
        push_in[depth + i, ITERS : ITERS + ny, :] = push
        for g, start in enumerate((0, tail)):
            if not 0 <= i - start < depth:
                continue
            for f, piece in enumerate((warm, cond, push, flag)):
                at_lane = ((i - start) * FIELDS + f) * depth
                turned = pltpu.roll(piece, at_lane + depth, 1)
                for side in range(2):
                    old = packed[side][g]
                    if old is not None:
                        turned_in = jnp.where(lane >= at_lane + side * depth, turned, old)
                    else:
                        turned_in = turned
                    packed[side][g] = turned_in
    for side in range(2):
        for g in range(BOTH):
            edges[side, g] = packed[side][g]

    waits = neighbours()
    if not direct:
        waits = waits + (plane + line - 2)
    pl.semaphore_wait(barrier, waits)

    def y_span(step, reach, source_base, base):
        if step == 0:
            return pl.ds(source_base, ny), pl.ds(base, ny)
        if step > 0:
            return pl.ds(source_base + ny - reach, reach), pl.ds(base - reach, reach)
        return pl.ds(source_base, reach), pl.ds(base + ny, reach)

    def x_span(step, reach):
        if step == 0:
            return pl.ds(depth, nx), pl.ds(depth, nx)
        if step > 0:
            return pl.ds(depth + nx - reach, reach), pl.ds(depth - reach, reach)
        return pl.ds(depth, reach), pl.ds(depth + nx, reach)

    def send(src, dst, way, stage):
        pltpu.make_async_remote_copy(
            src_ref=src,
            dst_ref=dst,
            send_sem=halo_send.at[0],
            recv_sem=halo_recv.at[stage],
            device_id=at(way),
            device_id_type=MESH,
        ).start()

    def send_field(ref, way, reach, base, stage):
        src_x, dst_x = x_span(way[0], reach)
        src_y, dst_y = y_span(way[1], reach, base, base)
        send(ref.at[src_x, src_y], ref.at[dst_x, dst_y], way, stage)

    def send_cond(way):
        send_field(pair.at[1], way, depth, depth, 0)

    def send_warm(way):
        send_field(pair.at[0], way, depth, depth, 1)

    def send_rest(way):
        send_field(push_in, way, depth - 1, ITERS, 2)
        send_field(cool, way, depth - 2, ITERS, 2)

    def send_edges(way):
        if way[0] == 0:
            src_x, dst_x = pl.ds(0, BOTH), pl.ds(1, BOTH)
        elif way[0] > 0:
            src_x, dst_x = pl.ds(1, 1), pl.ds(0, 1)
        else:
            src_x, dst_x = pl.ds(0, 1), pl.ds(1 + BOTH, 1)
        src_y, dst_y = y_span(way[1], depth, 0, depth)
        side = 0 if way[2] > 0 else 1
        send(edges.at[side, src_x, src_y], beside.at[side, dst_x, dst_y], way, 0)

    def send_all(steps):
        steps_on = tuple(v for v in steps if v)
        sides = [r for r in regions if r[0] and not r[1]]
        depths = sorted([r for r in regions if r[1]], key=lambda r: -abs(r[0]))
        plan = [(r, steps, (send_edges,)) for r in depths]
        for action in (send_cond, send_warm, send_rest):
            plan += [((0, 0), steps_on, (action,))] + [(r, steps, (action,)) for r in sides]
        for region, some, actions in plan:

            def go(region=region, some=some, actions=actions):
                for action in actions:
                    for way in ways_of(region, some):
                        action(way)

            if ways_of(region, some):
                guard(region, go)

    by_class(send_all)

    def x_rows(step, reach):
        return reach if step else nx

    def y_rows(step, reach):
        return reach if step else ny

    def moved_rows(way, kind):
        if kind == 3:
            return (1 if way[0] else BOTH) * y_rows(way[1], depth)
        reaches = ((depth,), (depth,), (depth - 1, depth - 2))[kind]
        return sum(x_rows(way[0], r) * y_rows(way[1], r) for r in reaches)

    def sides_of(k):
        if counts[k] == 1:
            return [(None, 0)]
        edge = jnp.logical_or(here[k] == 0, here[k] == counts[k] - 1)
        if counts[k] == 2:
            return [(None, 1)]
        return [(edge, 1), (jnp.logical_not(edge), 2)]

    def wait_all(kinds, semaphore, receive):
        def wait(sides):
            rows = 0
            for way in [(a, b, c) for a in (0, 1) for b in (0, 1) for c in (0, 1)]:
                times = 1
                for step, some in zip(way, sides):
                    times = times * (some if step else 1)
                for kind in kinds:
                    if any(way) and (kind == 3) == bool(way[2]):
                        rows = rows + times * moved_rows(way, kind)
            if rows == 0:
                return
            whole = pltpu.make_async_remote_copy(
                src_ref=ledger.at[pl.ds(0, rows)],
                dst_ref=ledger.at[pl.ds(0, rows)],
                send_sem=semaphore,
                recv_sem=semaphore,
                device_id=all_targets[0],
                device_id_type=MESH,
            )
            if receive:
                whole.wait_recv()
            else:
                whole.wait_send()

        for x_good, x_some in sides_of(0):
            for y_good, y_some in sides_of(1):
                for z_good, z_some in sides_of(2):
                    good = None
                    for one in (x_good, y_good, z_good):
                        if one is not None:
                            good = one if good is None else jnp.logical_and(good, one)
                    act = functools.partial(wait, (x_some, y_some, z_some))
                    if good is None:
                        act()
                    else:
                        pl.when(good)(act)

    if direct:
        signal_all(near)
        hops = [(a, 0, c) for a in (0, 2, -2) for c in (0, 2, -2) if a or c]
        hops = [h for h in hops if abs(h[0]) < counts[0] and abs(h[2]) < counts[2]]
        pl.semaphore_wait(near, neighbours())
        for hop in hops:
            signal(far, hop)

    def share(stage, rows_ref, slot, targets):
        for target in targets:
            pltpu.make_async_remote_copy(
                src_ref=row_out.at[stage],
                dst_ref=rows_ref.at[slot],
                send_sem=row_send.at[stage],
                recv_sem=row_recv.at[stage],
                device_id=target,
                device_id_type=MESH,
            ).start()

    def share_wait(stage, rows_ref, targets):
        if targets:
            whole = pltpu.make_async_remote_copy(
                src_ref=rows_ref.at[pl.ds(0, len(targets))],
                dst_ref=rows_ref.at[pl.ds(0, len(targets))],
                send_sem=row_send.at[stage],
                recv_sem=row_recv.at[stage],
                device_id=targets[0],
                device_id_type=MESH,
            )
            whole.wait_send()
            whole.wait_recv()

    wait_all((0, 3), halo_recv.at[0], True)

    tall_lane = lax.broadcasted_iota(jnp.int32, (tall, LANES), 1)

    places = [(0, j) for j in range(depth)]
    places += [(1, p) if p < depth else (2, p - tail) for p in range(nx)]
    places += [(1 + BOTH, j) for j in range(depth)]

    def unpack(fields):
        for i, (g, slot) in enumerate(places):
            for f in fields:
                spare = (0, 0, 1, 2)[f]
                if not spare <= i < wide - spare:
                    continue
                cut = (slot * FIELDS + f + 1) * depth
                if f < 2:
                    kept = jnp.where(tall_lane < cut, beside[0, g], beside[1, g])
                    side_pair[f, i] = pltpu.roll(kept, LANES - cut, 1)
                    continue
                ref = side_push if f == 2 else side_cool
                for t in range(leap):
                    rows = pl.ds(1 + t, SUB, stride=leap)
                    kept = jnp.where(tall_lane[:SUB] < cut, beside[0, g, rows, :], beside[1, g, rows, :])
                    ref[i, t * SUB : (t + 1) * SUB, :] = pltpu.roll(kept, LANES - cut, 1)

    unpack((1, 0))

    def pieces_of(f, i, first, some):
        pieces = []
        for j in range(first, first + some):
            rows = pl.ds(j, SUB, stride=leap)
            pieces.append(jnp.concatenate([pair[f, i, rows, :], side_pair[f, i, rows, :]], axis=1))
        return pieces

    def middle_of(f, i):
        return jnp.concatenate(pieces_of(f, i, 1, leap), axis=0)

    def joined(main, side, i):
        rows = [main[i, pl.ds(t, SUB, stride=leap), :] for t in range(leap)]
        return jnp.concatenate([jnp.concatenate(rows, axis=0), side[i]], axis=1)

    def along_x(least, most, planes_of, use):
        before = sums = None
        for i in range(least, most):
            now = planes_of(i)
            if i > least:
                joined = [a + b for a, b in zip(before, now)]
                if sums is not None:
                    use(i - 1, *[a + b for a, b in zip(sums, joined)])
                sums = joined
            before = now

    def ring_of(i):
        edge = (quarter * twice) * jnp.concatenate(pieces_of(1, i, 0, leap + 2), axis=0)
        before, after = beside_z(edge)
        for n, value in enumerate((edge, before, after)):
            couples[n, i] = value[SUB : SUB + short]
        return (smooth_rows(tiles_of((edge + edge) + (before + after))),)

    def use_ring(i, ring):
        spread[i] = (8.0 * interval_delta / quarter) * couples[0, i] + ring

    along_x(0, wide, ring_of, use_ring)
    unpack((2, 3))

    wait_all((1,), halo_recv.at[1], True)

    totals = [None] * MOMENTS

    def gather(n, a, b):
        part = sum(tiles_of(a * b))
        totals[n] = part if totals[n] is None else totals[n] + part

    def core(v):
        return v[:, :nz]

    def warm_of(i):
        warm = pieces_of(0, i, 0, leap + 2)
        cond = pieces_of(1, i, 0, leap + 2)
        warm_flux = [(quarter * twice) * (a * b) for a, b in zip(warm, cond)]
        return smooth_z(smooth_rows(warm)), smooth_z(smooth_rows(warm_flux))

    def use_warm(i, ring, push):
        edge = couples[0, i]
        image = spread[i] * middle_of(0, i) - (edge * ring + inside(i) * push)
        basis[0, i] = image

    along_x(0, wide, warm_of, use_warm)

    wait_all((2,), halo_recv.at[2], True)

    for k in range(ITERS - 1):

        def level_of(i, k=k):
            mid = basis[k, i]
            if k == 0:
                mid = joined(push_in, side_push, i) - mid
                basis[0, i] = mid
                if depth <= i < depth + nx:
                    gather(0, row_mask[...] * core(mid), core(mid))
            sums = sums_z(mid, beside_z(mid), [couples[n, i] for n in range(3)])
            return [smooth_y(value) for value in sums]

        def use_level(i, ring, push, k=k):
            edge = couples[0, i]
            mid = basis[k, i]
            if k == 0:
                main = spread[i] + twice * ((1.0 - middle) + interval_delta * cooling * joined(cool, side_cool, i))
                diag[i] = main
            else:
                main = diag[i]
            fresh = main * mid - (edge * ring + inside(i) * push)
            if k > 0:
                fresh = fresh - basis[k - 1, i]
            basis[k + 1, i] = fresh
            if depth <= i < depth + nx:
                kept = row_mask[...] * core(fresh)
                gather(2 * k + 1, core(mid), kept)
                gather(2 * k + 2, core(fresh), kept)

        along_x(k + 1, wide - k - 1, level_of, use_level)

    k = ITERS - 1

    def last_of(i):
        mid = basis[k, i]
        edges_own = [core(couples[n, i]) for n in range(3)]
        sums = sums_z(core(mid), beside_z_own(mid), edges_own)
        return [smooth_y(value) for value in sums]

    def use_last(i, ring, push):
        mid = core(basis[k, i])
        fresh = core(diag[i]) * mid - (core(couples[0, i]) * ring + push)
        fresh = fresh - core(basis[k - 1, i])
        basis[k + 1, i, :, 0:nz] = fresh
        gather(2 * k + 1, row_mask[...] * mid, fresh)

    along_x(depth - 1, depth + nx + 1, last_of, use_last)

    diagonal = lax.broadcasted_iota(jnp.int32, (SUB, LANES), 0)
    across = lax.broadcasted_iota(jnp.int32, (SUB, LANES), 1)
    tile = jnp.zeros((SUB, LANES), jnp.float32)
    for n in range(MOMENTS):
        tile = jnp.where(diagonal == n, jnp.sum(totals[n], axis=0, keepdims=True), tile)
    column = jnp.sum(tile, axis=1, keepdims=True)
    row = jnp.sum(jnp.where(across == diagonal, column, 0.0), axis=0, keepdims=True)
    if direct:
        pl.semaphore_wait(far, present(back(h) for h in hops))
    row_out[0] = row

    def settle():
        wait_all((0, 1, 2, 3), halo_send.at[0], False)
        for n in range(ITERS + 1):
            for i in range(nx):
                for t in range(leap):
                    tile = basis[n, depth + i, t * SUB : (t + 1) * SUB, 0:nz]
                    natural[n, i, pl.ds(t, SUB, stride=leap), :] = tile
        for n in range(ITERS + 1):
            for i in range(nx):
                natural_own[n, i] = natural[n, i, ITERS : ITERS + ny, :]
        for i in range(nx):
            natural_own[ITERS + 1, i] = pair[0, depth + i, depth : depth + ny, :]

    if direct:
        mine = in_plane * line + here[2]
        all_rows[mine] = row
        share(0, all_rows, mine, all_targets)
        settle()
        share_wait(0, all_rows, all_targets)
        row = jnp.sum(all_rows[...], axis=0)
    else:
        plane_rows[in_plane] = row
        share(0, plane_rows, in_plane, plane_targets)
        settle()
        share_wait(0, plane_rows, plane_targets)
        row = jnp.sum(plane_rows[...], axis=0)
        row_out[1] = row
        line_rows[here[2]] = row
        share(1, line_rows, here[2], line_targets)
        share_wait(1, line_rows, line_targets)
        row = jnp.sum(line_rows[...], axis=0)
    row_lane = lax.broadcasted_iota(jnp.int32, (1, LANES), 1)
    gram = {}
    for n in range(MOMENTS):
        value = jnp.sum(jnp.where(row_lane == n, row, 0.0), axis=1, keepdims=True)
        gram[n // 2, (n + 1) // 2] = value
    for gap in range(2, ITERS + 1):
        for i in range(ITERS + 1 - gap):
            j = i + gap
            value = gram[i + 1, j - 1] - gram[i, j - 2]
            if i > 0:
                value = value + gram[i - 1, j - 1]
            gram[i, j] = value
    for i, j in list(gram):
        gram[j, i] = gram[i, j]

    def apply(p):
        q = [middle * a for a in p] + [jnp.zeros_like(half)]
        for i, a in enumerate(p):
            q[i + 1] = q[i + 1] + (0.5 * half) * a
            if i > 0:
                q[i - 1] = q[i - 1] + (0.5 * half) * a
        return q

    def product(p, q):
        value = None
        for i, a in enumerate(p):
            inner = None
            for j, b in enumerate(q):
                term = gram[i, j] * b
                inner = term if inner is None else inner + term
            inner = a * inner
            value = inner if value is None else value + inner
        return value

    left = [0.5 * half]
    heading = list(left)
    moved = []
    norm = product(left, left)
    for step in range(ITERS):
        image = apply(heading)
        alpha = norm / product(heading, image)
        moved = [a + alpha * b for a, b in zip(moved, heading)] + [
            alpha * b for b in heading[len(moved) :]
        ]
        left = [a - alpha * b for a, b in zip(left, image)] + [
            -alpha * b for b in image[len(left) :]
        ]
        if step + 1 < ITERS:
            following = product(left, left)
            ratio = following / norm
            heading = [a + ratio * b for a, b in zip(left, heading)] + left[len(heading) :]
            norm = following

    for i in range(nx):
        warm = natural_own[ITERS + 1, i]
        end = jnp.zeros_like(warm)
        for k in range(ITERS + 1):
            value = natural_own[k, i]
            if k < ITERS:
                warm = warm + moved[k] * value
            end = end + left[k] * value
        both_out[0, i] = warm
        both_out[1, i] = end


def body(counts, warm, source, category, table, flags):
    nx, ny, nz = warm.shape
    depth = DEPTH
    plane, line = counts[0] * counts[1], counts[2]
    if nx < depth or nx % 2 or ny % SUB or nz != LANES or table.shape[0] > LANES:
        raise ValueError("block shape")
    if nx > 2 * depth or (FIELDS * depth + 1) * depth > LANES:
        raise ValueError("block shape")
    wide, tall, short, long = nx + 2 * depth, ny + 2 * SUB, ny + SUB, nz + LANES
    table = table[None]
    any_spec = pl.BlockSpec(memory_space=pl.ANY)
    vmem = pl.BlockSpec(memory_space=pltpu.VMEM)
    f32 = jnp.float32
    both = pl.pallas_call(
        functools.partial(kernel, counts),
        out_shape=pltpu.VMEM((2,) + warm.shape, jnp.float32),
        in_specs=[any_spec] * 5,
        out_specs=vmem,
        scratch_shapes=[
            pltpu.VMEM((2, wide, tall, nz), f32),
            pltpu.VMEM((2, wide, tall, nz), f32),
            pltpu.VMEM((wide, short, nz), f32),
            pltpu.VMEM((wide, short, nz), f32),
            pltpu.VMEM((wide, short, nz), f32),
            pltpu.VMEM((wide, short, nz), f32),
            pltpu.VMEM((ITERS + 1, wide, short, long), f32),
            pltpu.VMEM((wide, short, long), f32),
            pltpu.VMEM((wide, short, long), f32),
            pltpu.VMEM((3, wide, short, long), f32),
            pltpu.VMEM((3, short, long), f32),
            pltpu.VMEM((short, nz), f32),
            pltpu.VMEM((ITERS + 1, nx, short, nz), f32),
            pltpu.VMEM((ITERS + 2, nx, ny, nz), f32),
            pltpu.VMEM((SUB, LANES), f32),
            pltpu.VMEM(table.shape, f32),
            pltpu.VMEM((nx, ny, nz), f32),
            pltpu.VMEM((2, nx, ny, nz), jnp.int32),
            pltpu.VMEM((2, BOTH, ny, nz), f32),
            pltpu.VMEM((2, BOTH + 2, tall, nz), f32),
            pltpu.VMEM((16 * nx * ny, LANES), f32),
            pltpu.VMEM((2, 1, LANES), f32),
            pltpu.VMEM((plane, 1, LANES), f32),
            pltpu.VMEM((line, 1, LANES), f32),
            pltpu.VMEM((plane * line, 1, LANES), f32),
            pltpu.SemaphoreType.DMA((2,)),
            pltpu.SemaphoreType.DMA((1,)),
            pltpu.SemaphoreType.DMA((3,)),
            pltpu.SemaphoreType.DMA((2,)),
            pltpu.SemaphoreType.DMA((2,)),
            pltpu.SemaphoreType.REGULAR,
            pltpu.SemaphoreType.REGULAR,
        ],
        compiler_params=pltpu.CompilerParams(collective_id=0, has_side_effects=True),
    )(warm, source, category, table, flags)
    return both[0], both[1]


def solution(mesh):
    counts = tuple(mesh.shape[a] for a in AXES)
    spec = P("gx", "gy", "gz")
    return jax.shard_map(
        functools.partial(body, counts),
        mesh=mesh,
        in_specs=(spec, spec, spec, P(), spec),
        out_specs=(spec, spec),
        check_vma=False,
    )
```

```python
import functools

import jax
import jax.numpy as jnp
from jax import lax
from jax.experimental import pallas as pl
from jax.experimental.pallas import tpu as pltpu
from jax.sharding import PartitionSpec as P

ITERS = 4
interval_delta = 2.0
cooling = 3.0

MESH = pl.DeviceIdType.MESH
AXES = ("gx", "gy", "gz")
SUB = 8
REACH = 4
LANES = 128
FIELDS = 4
DEPTH = ITERS + 1
BOTH = 2
MOMENTS = 2 * ITERS
REGIONS = [(a, c) for c in (0, 1, -1) for a in (0, 1, -1)]


def tiles_of(values):
    return [values[r : r + SUB] for r in range(0, values.shape[0], SUB)]


def smooth_y(values):
    tiles = tiles_of(values)
    after = tiles[1:] + [pltpu.roll(tiles[0], SUB - 1, 0)]
    pairs = [a + b for a, b in zip(tiles, after)]
    before = [pltpu.roll(pairs[-1], 1, 0)] + pairs[:-1]
    return jnp.concatenate([a + b for a, b in zip(before, pairs)], axis=0)


def smooth_rows(pieces):
    pairs = [a + b for a, b in zip(pieces, pieces[1:])]
    return jnp.concatenate([a + b for a, b in zip(pairs, pairs[1:])], axis=0)


def beside_z(values):
    return pltpu.roll(values, 1, 1), pltpu.roll(values, values.shape[1] - 1, 1)


def beside_z_own(values):
    size = values.shape[1] // 2
    main, side = values[:, :size], values[:, size:]
    lane = lax.broadcasted_iota(jnp.int32, main.shape, 1)
    before = pltpu.roll(jnp.where(lane == size - 1, side, main), 1, 1)
    return before, pltpu.roll(jnp.where(lane == 0, side, main), size - 1, 1)


def smooth_z(values):
    before, after = beside_z(values)
    return (values + values) + (before + after)


def smooth_z_two(first, second, bands):
    rows = first.shape[0]
    both = jnp.concatenate([first, second], axis=0)
    coarse = both.astype(jnp.bfloat16)
    fine = (both - coarse.astype(jnp.float32)).astype(jnp.bfloat16)
    parts = jnp.concatenate([coarse, fine], axis=0)
    sums = jnp.dot(parts, bands[...], preferred_element_type=jnp.float32)
    sums = sums[: 2 * rows] + sums[2 * rows :]
    return sums[:rows], sums[rows:]


def sums_z(values, around, edges):
    before, after = around
    twice = values + values
    own = twice + (before + after)
    return own, edges[0] * twice + (edges[1] * before + edges[2] * after)


def kernel(
    counts,
    warm_in,
    source_in,
    category_in,
    table_in,
    flags_in,
    both_out,
    pair,
    side_pair,
    push_in,
    cool,
    side_push,
    side_cool,
    basis,
    spread,
    diag,
    couples,
    masks,
    row_mask,
    bands,
    natural,
    natural_own,
    table,
    table_row,
    source,
    ints,
    edges,
    beside,
    ledger,
    row_out,
    plane_rows,
    line_rows,
    all_rows,
    load_sems,
    halo_send,
    halo_recv,
    row_send,
    row_recv,
    near,
    far,
):
    plane, line = counts[0] * counts[1], counts[2]
    nx, ny, nz = both_out.shape[1:]
    depth = DEPTH
    wide, tall = pair.shape[1:3]
    long = 2 * nz
    short = ny + SUB
    leap = short // SUB
    tail = nx - depth
    direct = max(counts) <= REACH
    here = [lax.axis_index(a) for a in AXES]
    in_plane = here[0] * counts[1] + here[1]

    def exists(offset):
        good = None
        for k in range(3):
            if offset[k] > 0:
                one = here[k] < counts[k] - offset[k]
            elif offset[k] < 0:
                one = here[k] >= -offset[k]
            else:
                continue
            good = one if good is None else jnp.logical_and(good, one)
        return good

    def at(offset):
        return {a: here[k] + offset[k] for k, a in enumerate(AXES)}

    def back(offset):
        return tuple(-o for o in offset)

    def signal(semaphore, offset):
        @pl.when(exists(offset))
        def _():
            pl.semaphore_signal(semaphore, inc=1, device_id=at(offset), device_id_type=MESH)

    def present(offsets):
        return sum(jnp.where(exists(offset), 1, 0) for offset in offsets)

    plane_targets = [
        {"gx": other // counts[1], "gy": other % counts[1], "gz": here[2]}
        for other in [(in_plane + step) % plane for step in range(1, plane)]
    ]
    line_targets = [
        {"gx": here[0], "gy": here[1], "gz": (here[2] + step) % line} for step in range(1, line)
    ]
    def others(k):
        size = counts[k]
        far_side = here[k] >= (size + 1) // 2
        place = jnp.where(far_side, size - 1 - here[k], here[k])
        steps = [(size - 1 - u, size - 1 - u) for u in range(size // 2)]
        spots = [jnp.where(far_side, size - 1 - u, u) for u, _ in steps]
        weights = [w for _, w in steps]
        for step in range(1, size - size // 2):
            u = (place + step) % (size - size // 2)
            spots.append(jnp.where(far_side, size - 1 - u, u))
            weights.append(0.5)
        return list(zip(spots, weights)) + [(here[k], 0)]

    moved_by = [others(k) for k in range(3)]
    links = (0.5, 1.0, 1.0)
    ranked = [
        (sum(g * (m[1] > 0.5 or k > 0) * m[1] for k, (g, m) in enumerate(zip(links, spot))), n, spot)
        for n, spot in enumerate(
            (x, y, z) for x in moved_by[0] for y in moved_by[1] for z in moved_by[2]
        )
        if any(m[1] for m in spot)
    ]
    all_targets = [
        {a: spot[k][0] for k, a in enumerate(AXES)}
        for _, _, spot in sorted(ranked, key=lambda item: (-item[0], item[1]))
    ]

    regions = [r for r in REGIONS if abs(r[0]) < counts[0] and abs(r[1]) < counts[2]]

    def by_class(act):
        if counts[1] == 1:
            act((0,))
            return
        pl.when(here[1] == 0)(lambda: act((0, 1)))
        pl.when(here[1] == counts[1] - 1)(lambda: act((0, -1)))
        if counts[1] > 2:
            inner = jnp.logical_and(here[1] > 0, here[1] < counts[1] - 1)
            pl.when(inner)(lambda: act((0, 1, -1)))

    def guard(region, act):
        if region == (0, 0):
            act()
        else:
            pl.when(exists((region[0], 0, region[1])))(act)

    def ways_of(region, steps):
        ways = [(region[0], step, region[1]) for step in sorted(steps, key=lambda v: -abs(v))]
        return [way for way in ways if any(way)]

    def neighbours():
        total = 0
        for region in regions:
            here_too = 1 if region == (0, 0) else jnp.where(exists((region[0], 0, region[1])), 1, 0)
            beside_y = present([(0, 1, 0), (0, -1, 0)]) if counts[1] > 1 else 0
            total = total + here_too * (beside_y + (0 if region == (0, 0) else 1))
        return total

    def signal_all(semaphore):
        def act(steps):
            for region in sorted(regions, key=lambda r: (-abs(r[0]), -abs(r[1]))):

                def go(region=region):
                    for way in ways_of(region, steps):
                        pl.semaphore_signal(semaphore, inc=1, device_id=at(way), device_id_type=MESH)

                guard(region, go)

        by_class(act)

    barrier = pltpu.get_barrier_semaphore()
    signal_all(barrier)
    if not direct:
        for target in plane_targets + line_targets:
            pl.semaphore_signal(barrier, inc=1, device_id=target, device_id_type=MESH)

    own = (pl.ds(depth, nx), pl.ds(depth, ny))
    loads = [
        pltpu.make_async_copy(table_in, table_row, load_sems.at[0]),
        pltpu.make_async_copy(category_in, ints.at[0], load_sems.at[1]),
        pltpu.make_async_copy(flags_in, ints.at[1], load_sems.at[1]),
        pltpu.make_async_copy(warm_in, pair.at[(0,) + own], load_sems.at[1]),
        pltpu.make_async_copy(source_in, source, load_sems.at[1]),
    ]
    for load in loads:
        load.start()

    def clear(ref, *index):
        shape = ref.at[index].shape
        ref[index] = jnp.zeros(shape, jnp.float32)

    table[...] = jnp.zeros(table.shape, jnp.float32)
    everything = slice(None)
    for way, planes, slots in (
        ((-1, 0, 0), slice(0, depth), 0),
        ((1, 0, 0), slice(depth + nx, wide), 1 + BOTH),
    ):

        @pl.when(jnp.logical_not(exists(way)))
        def _():
            for f in range(2):
                clear(pair, f, planes)
            clear(push_in, planes)
            clear(cool, planes)
            for side in range(2):
                clear(beside, side, slots)

    for way, rows, few in (
        ((0, 1, 0), slice(depth + ny, 2 * depth + ny), slice(ITERS + ny, short)),
        ((0, -1, 0), slice(0, depth), slice(0, ITERS)),
    ):

        @pl.when(jnp.logical_not(exists(way)))
        def _():
            for f in range(2):
                clear(pair, f, everything, rows)
            clear(push_in, everything, few)
            clear(cool, everything, few)
            for side in range(2):
                clear(beside, side, everything, rows)

    for side, way in enumerate(((0, 0, -1), (0, 0, 1))):

        @pl.when(jnp.logical_not(exists(way)))
        def _():
            clear(beside, side)

    row_index = lax.broadcasted_iota(jnp.int32, (short, long), 0)
    y_index = leap * (row_index % SUB) + row_index // SUB - ITERS
    z_index = lax.broadcasted_iota(jnp.int32, (short, long), 1)
    y_low = jnp.logical_or(y_index >= 0, here[1] > 0)
    y_high = jnp.logical_or(y_index < ny, here[1] < counts[1] - 1)
    z_low = jnp.logical_or(z_index < nz + LANES // 2, here[2] > 0)
    z_far = jnp.logical_or(z_index < nz, z_index >= nz + LANES // 2)
    z_high = jnp.logical_or(z_far, here[2] < counts[2] - 1)
    y_good, z_good = jnp.logical_and(y_low, y_high), jnp.logical_and(z_low, z_high)
    within = jnp.where(jnp.logical_and(y_good, z_good), 1.0, 0.0)
    y_own = jnp.logical_and(y_index >= 0, y_index < ny)[:, :nz]
    row_mask[...] = jnp.where(y_own, 1.0, 0.0)
    masks[0] = jnp.where(here[0] > 0, 1.0, 0.0) * within
    masks[1] = within
    masks[2] = jnp.where(here[0] < counts[0] - 1, 1.0, 0.0) * within

    def inside(i):
        return masks[0 if i < depth else 2 if i >= depth + nx else 1]

    from_lane = lax.broadcasted_iota(jnp.int32, (long, long), 0)
    to_lane = lax.broadcasted_iota(jnp.int32, (long, long), 1)
    gap = jnp.abs(from_lane - to_lane)
    near_lane = jnp.logical_or(gap == 1, gap == long - 1)
    bands[...] = jnp.where(gap == 0, 2.0, jnp.where(near_lane, 1.0, 0.0)).astype(jnp.bfloat16)

    loads[0].wait()
    table[0:1, 0 : table_in.shape[1]] = table_row[...]
    most = 7.0 + 24.0 * jnp.max(table[0:1, :], axis=1, keepdims=True)
    high, low = most, jnp.ones_like(most)
    middle = 0.5 * (high + low)
    half = 0.5 * (high - low)
    twice = 2.0 / half
    quarter = 0.125 * interval_delta
    lookup = jnp.broadcast_to(table[0:1, :], (ny, LANES))
    lane = lax.broadcasted_iota(jnp.int32, (ny, LANES), 1)

    every = ledger.at[pl.ds(0, 4 * nx * ny)]
    pltpu.make_async_copy(every, every, load_sems.at[1]).wait()
    packed = [[None, None], [None, None]]
    for i in range(nx):
        cond = jnp.take_along_axis(lookup, ints[0, i], axis=1)
        flag = ints[1, i].astype(jnp.float32)
        warm = pair[0, depth + i, depth : depth + ny, :]
        push = interval_delta * source[i] - (interval_delta * cooling) * flag * warm
        push = twice * push
        pair[1, depth + i, depth : depth + ny, :] = cond
        cool[depth + i, ITERS : ITERS + ny, :] = flag
        push_in[depth + i, ITERS : ITERS + ny, :] = push
        for g, start in enumerate((0, tail)):
            if not 0 <= i - start < depth:
                continue
            for f, piece in enumerate((warm, cond, push, flag)):
                at_lane = ((i - start) * FIELDS + f) * depth
                turned = pltpu.roll(piece, at_lane + depth, 1)
                for side in range(2):
                    old = packed[side][g]
                    if old is not None:
                        turned_in = jnp.where(lane >= at_lane + side * depth, turned, old)
                    else:
                        turned_in = turned
                    packed[side][g] = turned_in
    for side in range(2):
        for g in range(BOTH):
            edges[side, g] = packed[side][g]

    waits = neighbours()
    if not direct:
        waits = waits + (plane + line - 2)
    pl.semaphore_wait(barrier, waits)

    def y_span(step, reach, source_base, base):
        if step == 0:
            return pl.ds(source_base, ny), pl.ds(base, ny)
        if step > 0:
            return pl.ds(source_base + ny - reach, reach), pl.ds(base - reach, reach)
        return pl.ds(source_base, reach), pl.ds(base + ny, reach)

    def x_span(step, reach):
        if step == 0:
            return pl.ds(depth, nx), pl.ds(depth, nx)
        if step > 0:
            return pl.ds(depth + nx - reach, reach), pl.ds(depth - reach, reach)
        return pl.ds(depth, reach), pl.ds(depth + nx, reach)

    def send(src, dst, way, stage):
        pltpu.make_async_remote_copy(
            src_ref=src,
            dst_ref=dst,
            send_sem=halo_send.at[0],
            recv_sem=halo_recv.at[stage],
            device_id=at(way),
            device_id_type=MESH,
        ).start()

    def send_field(ref, way, reach, base, stage):
        src_x, dst_x = x_span(way[0], reach)
        src_y, dst_y = y_span(way[1], reach, base, base)
        send(ref.at[src_x, src_y], ref.at[dst_x, dst_y], way, stage)

    def send_cond(way):
        send_field(pair.at[1], way, depth, depth, 0)

    def send_warm(way):
        send_field(pair.at[0], way, depth, depth, 1)

    def send_rest(way):
        send_field(push_in, way, depth - 1, ITERS, 2)
        send_field(cool, way, depth - 2, ITERS, 2)

    def send_edges(way):
        if way[0] == 0:
            src_x, dst_x = pl.ds(0, BOTH), pl.ds(1, BOTH)
        elif way[0] > 0:
            src_x, dst_x = pl.ds(1, 1), pl.ds(0, 1)
        else:
            src_x, dst_x = pl.ds(0, 1), pl.ds(1 + BOTH, 1)
        src_y, dst_y = y_span(way[1], depth, 0, depth)
        side = 0 if way[2] > 0 else 1
        send(edges.at[side, src_x, src_y], beside.at[side, dst_x, dst_y], way, 0)

    def send_all(steps):
        steps_on = tuple(v for v in steps if v)
        sides = [r for r in regions if r[0] and not r[1]]
        depths = sorted([r for r in regions if r[1]], key=lambda r: -abs(r[0]))
        plan = [(r, steps, (send_edges,)) for r in depths]
        for action in (send_cond, send_warm, send_rest):
            plan += [((0, 0), steps_on, (action,))] + [(r, steps, (action,)) for r in sides]
        for region, some, actions in plan:

            def go(region=region, some=some, actions=actions):
                for action in actions:
                    for way in ways_of(region, some):
                        action(way)

            if ways_of(region, some):
                guard(region, go)

    by_class(send_all)

    def x_rows(step, reach):
        return reach if step else nx

    def y_rows(step, reach):
        return reach if step else ny

    def moved_rows(way, kind):
        if kind == 3:
            return (1 if way[0] else BOTH) * y_rows(way[1], depth)
        reaches = ((depth,), (depth,), (depth - 1, depth - 2))[kind]
        return sum(x_rows(way[0], r) * y_rows(way[1], r) for r in reaches)

    def sides_of(k):
        if counts[k] == 1:
            return [(None, 0)]
        edge = jnp.logical_or(here[k] == 0, here[k] == counts[k] - 1)
        if counts[k] == 2:
            return [(None, 1)]
        return [(edge, 1), (jnp.logical_not(edge), 2)]

    def wait_all(kinds, semaphore, receive):
        def wait(sides):
            rows = 0
            for way in [(a, b, c) for a in (0, 1) for b in (0, 1) for c in (0, 1)]:
                times = 1
                for step, some in zip(way, sides):
                    times = times * (some if step else 1)
                for kind in kinds:
                    if any(way) and (kind == 3) == bool(way[2]):
                        rows = rows + times * moved_rows(way, kind)
            if rows == 0:
                return
            whole = pltpu.make_async_remote_copy(
                src_ref=ledger.at[pl.ds(0, rows)],
                dst_ref=ledger.at[pl.ds(0, rows)],
                send_sem=semaphore,
                recv_sem=semaphore,
                device_id=all_targets[0],
                device_id_type=MESH,
            )
            if receive:
                whole.wait_recv()
            else:
                whole.wait_send()

        for x_good, x_some in sides_of(0):
            for y_good, y_some in sides_of(1):
                for z_good, z_some in sides_of(2):
                    good = None
                    for one in (x_good, y_good, z_good):
                        if one is not None:
                            good = one if good is None else jnp.logical_and(good, one)
                    act = functools.partial(wait, (x_some, y_some, z_some))
                    if good is None:
                        act()
                    else:
                        pl.when(good)(act)

    if direct:
        signal_all(near)
        hops = [(a, 0, c) for a in (0, 2, -2) for c in (0, 2, -2) if a or c]
        hops = [h for h in hops if abs(h[0]) < counts[0] and abs(h[2]) < counts[2]]
        pl.semaphore_wait(near, neighbours())
        for hop in hops:
            signal(far, hop)

    def share(stage, rows_ref, slot, targets):
        for target in targets:
            pltpu.make_async_remote_copy(
                src_ref=row_out.at[stage],
                dst_ref=rows_ref.at[slot],
                send_sem=row_send.at[stage],
                recv_sem=row_recv.at[stage],
                device_id=target,
                device_id_type=MESH,
            ).start()

    def share_wait(stage, rows_ref, targets):
        if targets:
            whole = pltpu.make_async_remote_copy(
                src_ref=rows_ref.at[pl.ds(0, len(targets))],
                dst_ref=rows_ref.at[pl.ds(0, len(targets))],
                send_sem=row_send.at[stage],
                recv_sem=row_recv.at[stage],
                device_id=targets[0],
                device_id_type=MESH,
            )
            whole.wait_send()
            whole.wait_recv()

    wait_all((0, 3), halo_recv.at[0], True)

    tall_lane = lax.broadcasted_iota(jnp.int32, (tall, LANES), 1)

    places = [(0, j) for j in range(depth)]
    places += [(1, p) if p < depth else (2, p - tail) for p in range(nx)]
    places += [(1 + BOTH, j) for j in range(depth)]

    def unpack(fields):
        for i, (g, slot) in enumerate(places):
            for f in fields:
                spare = (0, 0, 1, 2)[f]
                if not spare <= i < wide - spare:
                    continue
                cut = (slot * FIELDS + f + 1) * depth
                if f < 2:
                    kept = jnp.where(tall_lane < cut, beside[0, g], beside[1, g])
                    side_pair[f, i] = pltpu.roll(kept, LANES - cut, 1)
                    continue
                ref = side_push if f == 2 else side_cool
                for t in range(leap):
                    rows = pl.ds(1 + t, SUB, stride=leap)
                    kept = jnp.where(tall_lane[:SUB] < cut, beside[0, g, rows, :], beside[1, g, rows, :])
                    ref[i, t * SUB : (t + 1) * SUB, :] = pltpu.roll(kept, LANES - cut, 1)

    unpack((1, 0))

    def pieces_of(f, i, first, some):
        pieces = []
        for j in range(first, first + some):
            rows = pl.ds(j, SUB, stride=leap)
            pieces.append(jnp.concatenate([pair[f, i, rows, :], side_pair[f, i, rows, :]], axis=1))
        return pieces

    def middle_of(f, i):
        return jnp.concatenate(pieces_of(f, i, 1, leap), axis=0)

    def joined(main, side, i):
        rows = [main[i, pl.ds(t, SUB, stride=leap), :] for t in range(leap)]
        return jnp.concatenate([jnp.concatenate(rows, axis=0), side[i]], axis=1)

    def along_x(least, most, planes_of, use):
        before = sums = None
        for i in range(least, most):
            now = planes_of(i)
            if i > least:
                joined = [a + b for a, b in zip(before, now)]
                if sums is not None:
                    use(i - 1, *[a + b for a, b in zip(sums, joined)])
                sums = joined
            before = now

    def ring_of(i):
        edge = (quarter * twice) * jnp.concatenate(pieces_of(1, i, 0, leap + 2), axis=0)
        before, after = beside_z(edge)
        for n, value in enumerate((edge, before, after)):
            couples[n, i] = value[SUB : SUB + short]
        return (smooth_rows(tiles_of((edge + edge) + (before + after))),)

    def use_ring(i, ring):
        spread[i] = (8.0 * interval_delta / quarter) * couples[0, i] + ring

    along_x(0, wide, ring_of, use_ring)
    unpack((2, 3))

    wait_all((1,), halo_recv.at[1], True)

    totals = [None] * MOMENTS

    def gather(n, a, b):
        part = sum(tiles_of(a * b))
        totals[n] = part if totals[n] is None else totals[n] + part

    def core(v):
        return v[:, :nz]

    pushes = {}

    def flux_rows(i):
        warm = pieces_of(0, i, 0, leap + 2)
        cond = pieces_of(1, i, 0, leap + 2)
        return smooth_rows([(quarter * twice) * (a * b) for a, b in zip(warm, cond)])

    def warm_of(i):
        if i % 2 == 0:
            pushes[i], pushes[i + 1] = smooth_z_two(flux_rows(i), flux_rows(i + 1), bands)
        return smooth_z(smooth_rows(pieces_of(0, i, 0, leap + 2))), pushes.pop(i)

    def use_warm(i, ring, push):
        edge = couples[0, i]
        image = spread[i] * middle_of(0, i) - (edge * ring + inside(i) * push)
        basis[0, i] = image

    along_x(0, wide, warm_of, use_warm)

    wait_all((2,), halo_recv.at[2], True)

    for k in range(ITERS - 1):

        def level_of(i, k=k):
            mid = basis[k, i]
            if k == 0:
                mid = joined(push_in, side_push, i) - mid
                basis[0, i] = mid
                if depth <= i < depth + nx:
                    gather(0, row_mask[...] * core(mid), core(mid))
            sums = sums_z(mid, beside_z(mid), [couples[n, i] for n in range(3)])
            return [smooth_y(value) for value in sums]

        def use_level(i, ring, push, k=k):
            edge = couples[0, i]
            mid = basis[k, i]
            if k == 0:
                main = spread[i] + twice * ((1.0 - middle) + interval_delta * cooling * joined(cool, side_cool, i))
                diag[i] = main
            else:
                main = diag[i]
            fresh = main * mid - (edge * ring + inside(i) * push)
            if k > 0:
                fresh = fresh - basis[k - 1, i]
            basis[k + 1, i] = fresh
            if depth <= i < depth + nx:
                kept = row_mask[...] * core(fresh)
                gather(2 * k + 1, core(mid), kept)
                gather(2 * k + 2, core(fresh), kept)

        along_x(k + 1, wide - k - 1, level_of, use_level)

    k = ITERS - 1

    def last_of(i):
        mid = basis[k, i]
        edges_own = [core(couples[n, i]) for n in range(3)]
        sums = sums_z(core(mid), beside_z_own(mid), edges_own)
        return [smooth_y(value) for value in sums]

    def use_last(i, ring, push):
        mid = core(basis[k, i])
        fresh = core(diag[i]) * mid - (core(couples[0, i]) * ring + push)
        fresh = fresh - core(basis[k - 1, i])
        basis[k + 1, i, :, 0:nz] = fresh
        gather(2 * k + 1, row_mask[...] * mid, fresh)

    along_x(depth - 1, depth + nx + 1, last_of, use_last)

    diagonal = lax.broadcasted_iota(jnp.int32, (SUB, LANES), 0)
    across = lax.broadcasted_iota(jnp.int32, (SUB, LANES), 1)
    tile = jnp.zeros((SUB, LANES), jnp.float32)
    for n in range(MOMENTS):
        tile = jnp.where(diagonal == n, jnp.sum(totals[n], axis=0, keepdims=True), tile)
    column = jnp.sum(tile, axis=1, keepdims=True)
    row = jnp.sum(jnp.where(across == diagonal, column, 0.0), axis=0, keepdims=True)
    if direct:
        pl.semaphore_wait(far, present(back(h) for h in hops))
    row_out[0] = row

    def settle():
        wait_all((0, 1, 2, 3), halo_send.at[0], False)
        for n in range(ITERS + 1):
            for i in range(nx):
                for t in range(leap):
                    tile = basis[n, depth + i, t * SUB : (t + 1) * SUB, 0:nz]
                    natural[n, i, pl.ds(t, SUB, stride=leap), :] = tile
        for n in range(ITERS + 1):
            for i in range(nx):
                natural_own[n, i] = natural[n, i, ITERS : ITERS + ny, :]
        for i in range(nx):
            natural_own[ITERS + 1, i] = pair[0, depth + i, depth : depth + ny, :]

    if direct:
        mine = in_plane * line + here[2]
        all_rows[mine] = row
        share(0, all_rows, mine, all_targets)
        settle()
        share_wait(0, all_rows, all_targets)
        row = jnp.sum(all_rows[...], axis=0)
    else:
        plane_rows[in_plane] = row
        share(0, plane_rows, in_plane, plane_targets)
        settle()
        share_wait(0, plane_rows, plane_targets)
        row = jnp.sum(plane_rows[...], axis=0)
        row_out[1] = row
        line_rows[here[2]] = row
        share(1, line_rows, here[2], line_targets)
        share_wait(1, line_rows, line_targets)
        row = jnp.sum(line_rows[...], axis=0)
    row_lane = lax.broadcasted_iota(jnp.int32, (1, LANES), 1)
    gram = {}
    for n in range(MOMENTS):
        value = jnp.sum(jnp.where(row_lane == n, row, 0.0), axis=1, keepdims=True)
        gram[n // 2, (n + 1) // 2] = value
    for gap in range(2, ITERS + 1):
        for i in range(ITERS + 1 - gap):
            j = i + gap
            value = gram[i + 1, j - 1] - gram[i, j - 2]
            if i > 0:
                value = value + gram[i - 1, j - 1]
            gram[i, j] = value
    for i, j in list(gram):
        gram[j, i] = gram[i, j]

    def apply(p):
        q = [middle * a for a in p] + [jnp.zeros_like(half)]
        for i, a in enumerate(p):
            q[i + 1] = q[i + 1] + (0.5 * half) * a
            if i > 0:
                q[i - 1] = q[i - 1] + (0.5 * half) * a
        return q

    def product(p, q):
        value = None
        for i, a in enumerate(p):
            inner = None
            for j, b in enumerate(q):
                term = gram[i, j] * b
                inner = term if inner is None else inner + term
            inner = a * inner
            value = inner if value is None else value + inner
        return value

    left = [0.5 * half]
    heading = list(left)
    moved = []
    norm = product(left, left)
    for step in range(ITERS):
        image = apply(heading)
        alpha = norm / product(heading, image)
        moved = [a + alpha * b for a, b in zip(moved, heading)] + [
            alpha * b for b in heading[len(moved) :]
        ]
        left = [a - alpha * b for a, b in zip(left, image)] + [
            -alpha * b for b in image[len(left) :]
        ]
        if step + 1 < ITERS:
            following = product(left, left)
            ratio = following / norm
            heading = [a + ratio * b for a, b in zip(left, heading)] + left[len(heading) :]
            norm = following

    for i in range(nx):
        warm = natural_own[ITERS + 1, i]
        end = jnp.zeros_like(warm)
        for k in range(ITERS + 1):
            value = natural_own[k, i]
            if k < ITERS:
                warm = warm + moved[k] * value
            end = end + left[k] * value
        both_out[0, i] = warm
        both_out[1, i] = end


def body(counts, warm, source, category, table, flags):
    nx, ny, nz = warm.shape
    depth = DEPTH
    plane, line = counts[0] * counts[1], counts[2]
    if nx < depth or nx % 2 or ny % SUB or nz != LANES or table.shape[0] > LANES:
        raise ValueError("block shape")
    if nx > 2 * depth or (FIELDS * depth + 1) * depth > LANES:
        raise ValueError("block shape")
    wide, tall, short, long = nx + 2 * depth, ny + 2 * SUB, ny + SUB, nz + LANES
    table = table[None]
    any_spec = pl.BlockSpec(memory_space=pl.ANY)
    vmem = pl.BlockSpec(memory_space=pltpu.VMEM)
    f32 = jnp.float32
    both = pl.pallas_call(
        functools.partial(kernel, counts),
        out_shape=pltpu.VMEM((2,) + warm.shape, jnp.float32),
        in_specs=[any_spec] * 5,
        out_specs=vmem,
        scratch_shapes=[
            pltpu.VMEM((2, wide, tall, nz), f32),
            pltpu.VMEM((2, wide, tall, nz), f32),
            pltpu.VMEM((wide, short, nz), f32),
            pltpu.VMEM((wide, short, nz), f32),
            pltpu.VMEM((wide, short, nz), f32),
            pltpu.VMEM((wide, short, nz), f32),
            pltpu.VMEM((ITERS + 1, wide, short, long), f32),
            pltpu.VMEM((wide, short, long), f32),
            pltpu.VMEM((wide, short, long), f32),
            pltpu.VMEM((3, wide, short, long), f32),
            pltpu.VMEM((3, short, long), f32),
            pltpu.VMEM((short, nz), f32),
            pltpu.VMEM((long, long), jnp.bfloat16),
            pltpu.VMEM((ITERS + 1, nx, short, nz), f32),
            pltpu.VMEM((ITERS + 2, nx, ny, nz), f32),
            pltpu.VMEM((SUB, LANES), f32),
            pltpu.VMEM(table.shape, f32),
            pltpu.VMEM((nx, ny, nz), f32),
            pltpu.VMEM((2, nx, ny, nz), jnp.int32),
            pltpu.VMEM((2, BOTH, ny, nz), f32),
            pltpu.VMEM((2, BOTH + 2, tall, nz), f32),
            pltpu.VMEM((16 * nx * ny, LANES), f32),
            pltpu.VMEM((2, 1, LANES), f32),
            pltpu.VMEM((plane, 1, LANES), f32),
            pltpu.VMEM((line, 1, LANES), f32),
            pltpu.VMEM((plane * line, 1, LANES), f32),
            pltpu.SemaphoreType.DMA((2,)),
            pltpu.SemaphoreType.DMA((1,)),
            pltpu.SemaphoreType.DMA((3,)),
            pltpu.SemaphoreType.DMA((2,)),
            pltpu.SemaphoreType.DMA((2,)),
            pltpu.SemaphoreType.REGULAR,
            pltpu.SemaphoreType.REGULAR,
        ],
        compiler_params=pltpu.CompilerParams(collective_id=0, has_side_effects=True),
    )(warm, source, category, table, flags)
    return both[0], both[1]


def solution(mesh):
    counts = tuple(mesh.shape[a] for a in AXES)
    spec = P("gx", "gy", "gz")
    return jax.shard_map(
        functools.partial(body, counts),
        mesh=mesh,
        in_specs=(spec, spec, spec, P(), spec),
        out_specs=(spec, spec),
        check_vma=False,
    )
```

```python
import functools

import jax
import jax.numpy as jnp
from jax import lax
from jax.experimental import pallas as pl
from jax.experimental.pallas import tpu as pltpu
from jax.sharding import PartitionSpec as P

ITERS = 4
interval_delta = 2.0
cooling = 3.0

MESH = pl.DeviceIdType.MESH
AXES = ("gx", "gy", "gz")
SUB = 8
REACH = 4
LANES = 128
FIELDS = 4
DEPTH = ITERS + 1
BOTH = 2
MOMENTS = 2 * ITERS
REGIONS = [(a, c) for c in (0, 1, -1) for a in (0, 1, -1)]


def tiles_of(values):
    return [values[r : r + SUB] for r in range(0, values.shape[0], SUB)]


def smooth_y(values):
    tiles = tiles_of(values)
    after = tiles[1:] + [pltpu.roll(tiles[0], SUB - 1, 0)]
    pairs = [a + b for a, b in zip(tiles, after)]
    before = [pltpu.roll(pairs[-1], 1, 0)] + pairs[:-1]
    return jnp.concatenate([a + b for a, b in zip(before, pairs)], axis=0)


def smooth_rows(pieces):
    pairs = [a + b for a, b in zip(pieces, pieces[1:])]
    return jnp.concatenate([a + b for a, b in zip(pairs, pairs[1:])], axis=0)


def beside_z(values):
    return pltpu.roll(values, 1, 1), pltpu.roll(values, values.shape[1] - 1, 1)


def beside_z_own(values):
    size = values.shape[1] // 2
    main, side = values[:, :size], values[:, size:]
    lane = lax.broadcasted_iota(jnp.int32, main.shape, 1)
    before = pltpu.roll(jnp.where(lane == size - 1, side, main), 1, 1)
    return before, pltpu.roll(jnp.where(lane == 0, side, main), size - 1, 1)


def smooth_z(values):
    before, after = beside_z(values)
    return (values + values) + (before + after)


def smooth_z_two(first, second, bands):
    rows = first.shape[0]
    both = jnp.concatenate([first, second], axis=0)
    coarse = both.astype(jnp.bfloat16)
    fine = (both - coarse.astype(jnp.float32)).astype(jnp.bfloat16)
    parts = jnp.concatenate([coarse, fine], axis=0)
    sums = jnp.dot(parts, bands[...], preferred_element_type=jnp.float32)
    sums = sums[: 2 * rows] + sums[2 * rows :]
    return sums[:rows], sums[rows:]


def sums_z(values, around, edges):
    before, after = around
    twice = values + values
    own = twice + (before + after)
    return own, edges[0] * twice + (edges[1] * before + edges[2] * after)


def kernel(
    counts,
    warm_in,
    source_in,
    category_in,
    table_in,
    flags_in,
    both_out,
    pair,
    side_pair,
    push_in,
    cool,
    side_push,
    side_cool,
    basis,
    spread,
    diag,
    couples,
    masks,
    row_mask,
    bands,
    natural,
    natural_own,
    table,
    table_row,
    source,
    ints,
    edges,
    beside,
    ledger,
    row_out,
    plane_rows,
    line_rows,
    plane_bounds,
    line_bounds,
    all_rows,
    load_sems,
    halo_send,
    halo_recv,
    row_send,
    row_recv,
    near,
    far,
):
    plane, line = counts[0] * counts[1], counts[2]
    nx, ny, nz = both_out.shape[1:]
    depth = DEPTH
    wide, tall = pair.shape[1:3]
    long = 2 * nz
    short = ny + SUB
    leap = short // SUB
    tail = nx - depth
    direct = max(counts) <= REACH
    here = [lax.axis_index(a) for a in AXES]
    in_plane = here[0] * counts[1] + here[1]

    def exists(offset):
        good = None
        for k in range(3):
            if offset[k] > 0:
                one = here[k] < counts[k] - offset[k]
            elif offset[k] < 0:
                one = here[k] >= -offset[k]
            else:
                continue
            good = one if good is None else jnp.logical_and(good, one)
        return good

    def at(offset):
        return {a: here[k] + offset[k] for k, a in enumerate(AXES)}

    def back(offset):
        return tuple(-o for o in offset)

    def signal(semaphore, offset):
        @pl.when(exists(offset))
        def _():
            pl.semaphore_signal(semaphore, inc=1, device_id=at(offset), device_id_type=MESH)

    def present(offsets):
        return sum(jnp.where(exists(offset), 1, 0) for offset in offsets)

    plane_targets = [
        {"gx": other // counts[1], "gy": other % counts[1], "gz": here[2]}
        for other in [(in_plane + step) % plane for step in range(1, plane)]
    ]
    line_targets = [
        {"gx": here[0], "gy": here[1], "gz": (here[2] + step) % line} for step in range(1, line)
    ]
    def others(k):
        size = counts[k]
        far_side = here[k] >= (size + 1) // 2
        place = jnp.where(far_side, size - 1 - here[k], here[k])
        steps = [(size - 1 - u, size - 1 - u) for u in range(size // 2)]
        spots = [jnp.where(far_side, size - 1 - u, u) for u, _ in steps]
        weights = [w for _, w in steps]
        for step in range(1, size - size // 2):
            u = (place + step) % (size - size // 2)
            spots.append(jnp.where(far_side, size - 1 - u, u))
            weights.append(0.5)
        return list(zip(spots, weights)) + [(here[k], 0)]

    moved_by = [others(k) for k in range(3)]
    links = (0.5, 1.0, 1.0)
    ranked = [
        (sum(g * (m[1] > 0.5 or k > 0) * m[1] for k, (g, m) in enumerate(zip(links, spot))), n, spot)
        for n, spot in enumerate(
            (x, y, z) for x in moved_by[0] for y in moved_by[1] for z in moved_by[2]
        )
        if any(m[1] for m in spot)
    ]
    all_targets = [
        {a: spot[k][0] for k, a in enumerate(AXES)}
        for _, _, spot in sorted(ranked, key=lambda item: (-item[0], item[1]))
    ]

    regions = [r for r in REGIONS if abs(r[0]) < counts[0] and abs(r[1]) < counts[2]]

    def by_class(act):
        if counts[1] == 1:
            act((0,))
            return
        pl.when(here[1] == 0)(lambda: act((0, 1)))
        pl.when(here[1] == counts[1] - 1)(lambda: act((0, -1)))
        if counts[1] > 2:
            inner = jnp.logical_and(here[1] > 0, here[1] < counts[1] - 1)
            pl.when(inner)(lambda: act((0, 1, -1)))

    def guard(region, act):
        if region == (0, 0):
            act()
        else:
            pl.when(exists((region[0], 0, region[1])))(act)

    def ways_of(region, steps):
        ways = [(region[0], step, region[1]) for step in sorted(steps, key=lambda v: -abs(v))]
        return [way for way in ways if any(way)]

    def neighbours():
        total = 0
        for region in regions:
            here_too = 1 if region == (0, 0) else jnp.where(exists((region[0], 0, region[1])), 1, 0)
            beside_y = present([(0, 1, 0), (0, -1, 0)]) if counts[1] > 1 else 0
            total = total + here_too * (beside_y + (0 if region == (0, 0) else 1))
        return total

    def signal_all(semaphore):
        def act(steps):
            for region in sorted(regions, key=lambda r: (-abs(r[0]), -abs(r[1]))):

                def go(region=region):
                    for way in ways_of(region, steps):
                        pl.semaphore_signal(semaphore, inc=1, device_id=at(way), device_id_type=MESH)

                guard(region, go)

        by_class(act)

    barrier = pltpu.get_barrier_semaphore()
    signal_all(barrier)
    for target in plane_targets + line_targets:
        pl.semaphore_signal(barrier, inc=1, device_id=target, device_id_type=MESH)

    own = (pl.ds(depth, nx), pl.ds(depth, ny))
    loads = [
        pltpu.make_async_copy(table_in, table_row, load_sems.at[0]),
        pltpu.make_async_copy(category_in, ints.at[0], load_sems.at[1]),
        pltpu.make_async_copy(flags_in, ints.at[1], load_sems.at[1]),
        pltpu.make_async_copy(warm_in, pair.at[(0,) + own], load_sems.at[1]),
        pltpu.make_async_copy(source_in, source, load_sems.at[1]),
    ]
    for load in loads:
        load.start()

    def clear(ref, *index):
        shape = ref.at[index].shape
        ref[index] = jnp.zeros(shape, jnp.float32)

    table[...] = jnp.zeros(table.shape, jnp.float32)
    everything = slice(None)
    for way, planes, slots in (
        ((-1, 0, 0), slice(0, depth), 0),
        ((1, 0, 0), slice(depth + nx, wide), 1 + BOTH),
    ):

        @pl.when(jnp.logical_not(exists(way)))
        def _():
            for f in range(2):
                clear(pair, f, planes)
            clear(push_in, planes)
            clear(cool, planes)
            for side in range(2):
                clear(beside, side, slots)

    for way, rows, few in (
        ((0, 1, 0), slice(depth + ny, 2 * depth + ny), slice(ITERS + ny, short)),
        ((0, -1, 0), slice(0, depth), slice(0, ITERS)),
    ):

        @pl.when(jnp.logical_not(exists(way)))
        def _():
            for f in range(2):
                clear(pair, f, everything, rows)
            clear(push_in, everything, few)
            clear(cool, everything, few)
            for side in range(2):
                clear(beside, side, everything, rows)

    for side, way in enumerate(((0, 0, -1), (0, 0, 1))):

        @pl.when(jnp.logical_not(exists(way)))
        def _():
            clear(beside, side)

    row_index = lax.broadcasted_iota(jnp.int32, (short, long), 0)
    y_index = leap * (row_index % SUB) + row_index // SUB - ITERS
    z_index = lax.broadcasted_iota(jnp.int32, (short, long), 1)
    y_low = jnp.logical_or(y_index >= 0, here[1] > 0)
    y_high = jnp.logical_or(y_index < ny, here[1] < counts[1] - 1)
    z_low = jnp.logical_or(z_index < nz + LANES // 2, here[2] > 0)
    z_far = jnp.logical_or(z_index < nz, z_index >= nz + LANES // 2)
    z_high = jnp.logical_or(z_far, here[2] < counts[2] - 1)
    y_good, z_good = jnp.logical_and(y_low, y_high), jnp.logical_and(z_low, z_high)
    within = jnp.where(jnp.logical_and(y_good, z_good), 1.0, 0.0)
    y_own = jnp.logical_and(y_index >= 0, y_index < ny)[:, :nz]
    row_mask[...] = jnp.where(y_own, 1.0, 0.0)
    masks[0] = jnp.where(here[0] > 0, 1.0, 0.0) * within
    masks[1] = within
    masks[2] = jnp.where(here[0] < counts[0] - 1, 1.0, 0.0) * within

    def inside(i):
        return masks[0 if i < depth else 2 if i >= depth + nx else 1]

    from_lane = lax.broadcasted_iota(jnp.int32, (long, long), 0)
    to_lane = lax.broadcasted_iota(jnp.int32, (long, long), 1)
    gap = jnp.abs(from_lane - to_lane)
    near_lane = jnp.logical_or(gap == 1, gap == long - 1)
    bands[...] = jnp.where(gap == 0, 2.0, jnp.where(near_lane, 1.0, 0.0)).astype(jnp.bfloat16)

    loads[0].wait()
    table[0:1, 0 : table_in.shape[1]] = table_row[...]
    quarter = 0.125 * interval_delta
    lookup = jnp.broadcast_to(table[0:1, :], (ny, LANES))
    lane = lax.broadcasted_iota(jnp.int32, (ny, LANES), 1)

    every = ledger.at[pl.ds(0, 4 * nx * ny)]
    pltpu.make_async_copy(every, every, load_sems.at[1]).wait()
    packed = [[None, None], [None, None]]
    for i in range(nx):
        cond = jnp.take_along_axis(lookup, ints[0, i], axis=1)
        flag = ints[1, i].astype(jnp.float32)
        warm = pair[0, depth + i, depth : depth + ny, :]
        push = interval_delta * source[i] - (interval_delta * cooling) * flag * warm
        tops = (cond, cond, flag, flag) if i == 0 else (
            jnp.maximum(tops[0], cond), tops[1] + cond, jnp.maximum(tops[2], flag), jnp.minimum(tops[3], flag)
        )
        pair[1, depth + i, depth : depth + ny, :] = cond
        cool[depth + i, ITERS : ITERS + ny, :] = flag
        push_in[depth + i, ITERS : ITERS + ny, :] = push
        for g, start in enumerate((0, tail)):
            if not 0 <= i - start < depth:
                continue
            for f, piece in enumerate((warm, cond, push, flag)):
                at_lane = ((i - start) * FIELDS + f) * depth
                turned = pltpu.roll(piece, at_lane + depth, 1)
                for side in range(2):
                    old = packed[side][g]
                    if old is not None:
                        turned_in = jnp.where(lane >= at_lane + side * depth, turned, old)
                    else:
                        turned_in = turned
                    packed[side][g] = turned_in
    for side in range(2):
        for g in range(BOTH):
            edges[side, g] = packed[side][g]

    shrink = lambda op, v: op(op(v, axis=0, keepdims=True), axis=1, keepdims=True)
    mean = shrink(jnp.sum, tops[1]) * (1.0 / (nx * ny * nz))
    high = 1.0 + interval_delta * cooling * shrink(jnp.max, tops[2])
    high = high + 8.0 * interval_delta * (shrink(jnp.max, tops[0]) + mean)
    low = 1.0 + interval_delta * cooling * shrink(jnp.min, tops[3])
    row_lane = lax.broadcasted_iota(jnp.int32, (1, LANES), 1)
    bound = jnp.where(row_lane == 0, high, -low)
    row_out[2] = bound
    plane_bounds[in_plane] = bound

    waits = neighbours()
    waits = waits + (plane + line - 2)
    pl.semaphore_wait(barrier, waits)

    def share(stage, rows_ref, slot, targets):
        for target in targets:
            pltpu.make_async_remote_copy(
                src_ref=row_out.at[stage],
                dst_ref=rows_ref.at[slot],
                send_sem=row_send.at[stage],
                recv_sem=row_recv.at[stage],
                device_id=target,
                device_id_type=MESH,
            ).start()

    def share_wait(stage, rows_ref, targets):
        if targets:
            whole = pltpu.make_async_remote_copy(
                src_ref=rows_ref.at[pl.ds(0, len(targets))],
                dst_ref=rows_ref.at[pl.ds(0, len(targets))],
                send_sem=row_send.at[stage],
                recv_sem=row_recv.at[stage],
                device_id=targets[0],
                device_id_type=MESH,
            )
            whole.wait_send()
            whole.wait_recv()

    share(2, plane_bounds, in_plane, plane_targets)

    def y_span(step, reach, source_base, base):
        if step == 0:
            return pl.ds(source_base, ny), pl.ds(base, ny)
        if step > 0:
            return pl.ds(source_base + ny - reach, reach), pl.ds(base - reach, reach)
        return pl.ds(source_base, reach), pl.ds(base + ny, reach)

    def x_span(step, reach):
        if step == 0:
            return pl.ds(depth, nx), pl.ds(depth, nx)
        if step > 0:
            return pl.ds(depth + nx - reach, reach), pl.ds(depth - reach, reach)
        return pl.ds(depth, reach), pl.ds(depth + nx, reach)

    def send(src, dst, way, stage):
        pltpu.make_async_remote_copy(
            src_ref=src,
            dst_ref=dst,
            send_sem=halo_send.at[0],
            recv_sem=halo_recv.at[stage],
            device_id=at(way),
            device_id_type=MESH,
        ).start()

    def send_field(ref, way, reach, base, stage):
        src_x, dst_x = x_span(way[0], reach)
        src_y, dst_y = y_span(way[1], reach, base, base)
        send(ref.at[src_x, src_y], ref.at[dst_x, dst_y], way, stage)

    def send_cond(way):
        send_field(pair.at[1], way, depth, depth, 0)

    def send_warm(way):
        send_field(pair.at[0], way, depth, depth, 1)

    def send_rest(way):
        send_field(push_in, way, depth - 1, ITERS, 2)
        send_field(cool, way, depth - 2, ITERS, 2)

    def send_edges(way):
        if way[0] == 0:
            src_x, dst_x = pl.ds(0, BOTH), pl.ds(1, BOTH)
        elif way[0] > 0:
            src_x, dst_x = pl.ds(1, 1), pl.ds(0, 1)
        else:
            src_x, dst_x = pl.ds(0, 1), pl.ds(1 + BOTH, 1)
        src_y, dst_y = y_span(way[1], depth, 0, depth)
        side = 0 if way[2] > 0 else 1
        send(edges.at[side, src_x, src_y], beside.at[side, dst_x, dst_y], way, 0)

    def send_all(steps):
        steps_on = tuple(v for v in steps if v)
        sides = [r for r in regions if r[0] and not r[1]]
        depths = sorted([r for r in regions if r[1]], key=lambda r: -abs(r[0]))
        plan = [(r, steps, (send_edges,)) for r in depths]
        for action in (send_cond, send_warm, send_rest):
            plan += [((0, 0), steps_on, (action,))] + [(r, steps, (action,)) for r in sides]
        for region, some, actions in plan:

            def go(region=region, some=some, actions=actions):
                for action in actions:
                    for way in ways_of(region, some):
                        action(way)

            if ways_of(region, some):
                guard(region, go)

    by_class(send_all)

    def x_rows(step, reach):
        return reach if step else nx

    def y_rows(step, reach):
        return reach if step else ny

    def moved_rows(way, kind):
        if kind == 3:
            return (1 if way[0] else BOTH) * y_rows(way[1], depth)
        reaches = ((depth,), (depth,), (depth - 1, depth - 2))[kind]
        return sum(x_rows(way[0], r) * y_rows(way[1], r) for r in reaches)

    def sides_of(k):
        if counts[k] == 1:
            return [(None, 0)]
        edge = jnp.logical_or(here[k] == 0, here[k] == counts[k] - 1)
        if counts[k] == 2:
            return [(None, 1)]
        return [(edge, 1), (jnp.logical_not(edge), 2)]

    def wait_all(kinds, semaphore, receive):
        def wait(sides):
            rows = 0
            for way in [(a, b, c) for a in (0, 1) for b in (0, 1) for c in (0, 1)]:
                times = 1
                for step, some in zip(way, sides):
                    times = times * (some if step else 1)
                for kind in kinds:
                    if any(way) and (kind == 3) == bool(way[2]):
                        rows = rows + times * moved_rows(way, kind)
            if rows == 0:
                return
            whole = pltpu.make_async_remote_copy(
                src_ref=ledger.at[pl.ds(0, rows)],
                dst_ref=ledger.at[pl.ds(0, rows)],
                send_sem=semaphore,
                recv_sem=semaphore,
                device_id=all_targets[0],
                device_id_type=MESH,
            )
            if receive:
                whole.wait_recv()
            else:
                whole.wait_send()

        for x_good, x_some in sides_of(0):
            for y_good, y_some in sides_of(1):
                for z_good, z_some in sides_of(2):
                    good = None
                    for one in (x_good, y_good, z_good):
                        if one is not None:
                            good = one if good is None else jnp.logical_and(good, one)
                    act = functools.partial(wait, (x_some, y_some, z_some))
                    if good is None:
                        act()
                    else:
                        pl.when(good)(act)

    if direct:
        signal_all(near)
        hops = [(a, 0, c) for a in (0, 2, -2) for c in (0, 2, -2) if a or c]
        hops = [h for h in hops if abs(h[0]) < counts[0] and abs(h[2]) < counts[2]]
        pl.semaphore_wait(near, neighbours())
        for hop in hops:
            signal(far, hop)

    share_wait(2, plane_bounds, plane_targets)
    bound = jnp.max(plane_bounds[...], axis=0)
    row_out[3] = bound
    line_bounds[here[2]] = bound
    share(3, line_bounds, here[2], line_targets)

    wait_all((0, 3), halo_recv.at[0], True)

    tall_lane = lax.broadcasted_iota(jnp.int32, (tall, LANES), 1)

    places = [(0, j) for j in range(depth)]
    places += [(1, p) if p < depth else (2, p - tail) for p in range(nx)]
    places += [(1 + BOTH, j) for j in range(depth)]

    def unpack(fields):
        for i, (g, slot) in enumerate(places):
            for f in fields:
                spare = (0, 0, 1, 2)[f]
                if not spare <= i < wide - spare:
                    continue
                cut = (slot * FIELDS + f + 1) * depth
                if f < 2:
                    kept = jnp.where(tall_lane < cut, beside[0, g], beside[1, g])
                    side_pair[f, i] = pltpu.roll(kept, LANES - cut, 1)
                    continue
                ref = side_push if f == 2 else side_cool
                for t in range(leap):
                    rows = pl.ds(1 + t, SUB, stride=leap)
                    kept = jnp.where(tall_lane[:SUB] < cut, beside[0, g, rows, :], beside[1, g, rows, :])
                    ref[i, t * SUB : (t + 1) * SUB, :] = pltpu.roll(kept, LANES - cut, 1)

    unpack((1, 0))

    def pieces_of(f, i, first, some):
        pieces = []
        for j in range(first, first + some):
            rows = pl.ds(j, SUB, stride=leap)
            pieces.append(jnp.concatenate([pair[f, i, rows, :], side_pair[f, i, rows, :]], axis=1))
        return pieces

    def middle_of(f, i):
        return jnp.concatenate(pieces_of(f, i, 1, leap), axis=0)

    def joined(main, side, i):
        rows = [main[i, pl.ds(t, SUB, stride=leap), :] for t in range(leap)]
        return jnp.concatenate([jnp.concatenate(rows, axis=0), side[i]], axis=1)

    def along_x(least, most, planes_of, use):
        before = sums = None
        for i in range(least, most):
            now = planes_of(i)
            if i > least:
                joined = [a + b for a, b in zip(before, now)]
                if sums is not None:
                    use(i - 1, *[a + b for a, b in zip(sums, joined)])
                sums = joined
            before = now

    def ring_of(i):
        edge = quarter * jnp.concatenate(pieces_of(1, i, 0, leap + 2), axis=0)
        before, after = beside_z(edge)
        for n, value in enumerate((edge, before, after)):
            couples[n, i] = value[SUB : SUB + short]
        return (smooth_rows(tiles_of((edge + edge) + (before + after))),)

    def use_ring(i, ring):
        spread[i] = (8.0 * interval_delta / quarter) * couples[0, i] + ring

    along_x(0, wide, ring_of, use_ring)
    unpack((2, 3))

    wait_all((1,), halo_recv.at[1], True)

    totals = [None] * MOMENTS

    def gather(n, a, b):
        part = sum(tiles_of(a * b))
        totals[n] = part if totals[n] is None else totals[n] + part

    def core(v):
        return v[:, :nz]

    pushes = {}

    def flux_rows(i):
        warm = pieces_of(0, i, 0, leap + 2)
        cond = pieces_of(1, i, 0, leap + 2)
        return smooth_rows([quarter * (a * b) for a, b in zip(warm, cond)])

    def warm_of(i):
        if i % 2 == 0:
            pushes[i], pushes[i + 1] = smooth_z_two(flux_rows(i), flux_rows(i + 1), bands)
        return smooth_z(smooth_rows(pieces_of(0, i, 0, leap + 2))), pushes.pop(i)

    def use_warm(i, ring, push):
        edge = couples[0, i]
        image = spread[i] * middle_of(0, i) - (edge * ring + inside(i) * push)
        basis[0, i] = image

    along_x(0, wide, warm_of, use_warm)

    wait_all((2,), halo_recv.at[2], True)

    share_wait(3, line_bounds, line_targets)
    bound = jnp.max(line_bounds[...], axis=0)
    pick_one = lambda v, n: jnp.sum(jnp.where(row_lane == n, v, 0.0), axis=1, keepdims=True)
    high, low = pick_one(bound, 0), -pick_one(bound, 1)
    middle = 0.5 * (high + low)
    half = 0.5 * (high - low)
    twice = 2.0 / half

    for k in range(ITERS - 1):

        def level_of(i, k=k):
            mid = basis[k, i]
            if k == 0:
                mid = joined(push_in, side_push, i) - mid
                basis[0, i] = mid
                if depth <= i < depth + nx:
                    gather(0, row_mask[...] * core(mid), core(mid))
            sums = sums_z(mid, beside_z(mid), [couples[n, i] for n in range(3)])
            return [smooth_y(value) for value in sums]

        def use_level(i, ring, push, k=k):
            edge = couples[0, i]
            mid = basis[k, i]
            if k == 0:
                main = spread[i] + ((1.0 - middle) + interval_delta * cooling * joined(cool, side_cool, i))
                diag[i] = main
            else:
                main = diag[i]
            fresh = twice * (main * mid - (edge * ring + inside(i) * push))
            if k > 0:
                fresh = fresh - basis[k - 1, i]
            basis[k + 1, i] = fresh
            if depth <= i < depth + nx:
                kept = row_mask[...] * core(fresh)
                gather(2 * k + 1, core(mid), kept)
                gather(2 * k + 2, core(fresh), kept)

        along_x(k + 1, wide - k - 1, level_of, use_level)

    k = ITERS - 1

    def last_of(i):
        mid = basis[k, i]
        edges_own = [core(couples[n, i]) for n in range(3)]
        sums = sums_z(core(mid), beside_z_own(mid), edges_own)
        return [smooth_y(value) for value in sums]

    def use_last(i, ring, push):
        mid = core(basis[k, i])
        fresh = twice * (core(diag[i]) * mid - (core(couples[0, i]) * ring + push))
        fresh = fresh - core(basis[k - 1, i])
        basis[k + 1, i, :, 0:nz] = fresh
        gather(2 * k + 1, row_mask[...] * mid, fresh)

    along_x(depth - 1, depth + nx + 1, last_of, use_last)

    diagonal = lax.broadcasted_iota(jnp.int32, (SUB, LANES), 0)
    across = lax.broadcasted_iota(jnp.int32, (SUB, LANES), 1)
    tile = jnp.zeros((SUB, LANES), jnp.float32)
    for n in range(MOMENTS):
        tile = jnp.where(diagonal == n, jnp.sum(totals[n], axis=0, keepdims=True), tile)
    column = jnp.sum(tile, axis=1, keepdims=True)
    row = jnp.sum(jnp.where(across == diagonal, column, 0.0), axis=0, keepdims=True)
    if direct:
        pl.semaphore_wait(far, present(back(h) for h in hops))
    row_out[0] = row

    def settle():
        wait_all((0, 1, 2, 3), halo_send.at[0], False)
        for n in range(ITERS + 1):
            for i in range(nx):
                for t in range(leap):
                    tile = basis[n, depth + i, t * SUB : (t + 1) * SUB, 0:nz]
                    natural[n, i, pl.ds(t, SUB, stride=leap), :] = tile
        for n in range(ITERS + 1):
            for i in range(nx):
                natural_own[n, i] = natural[n, i, ITERS : ITERS + ny, :]
        for i in range(nx):
            natural_own[ITERS + 1, i] = pair[0, depth + i, depth : depth + ny, :]

    if direct:
        mine = in_plane * line + here[2]
        all_rows[mine] = row
        share(0, all_rows, mine, all_targets)
        settle()
        share_wait(0, all_rows, all_targets)
        row = jnp.sum(all_rows[...], axis=0)
    else:
        plane_rows[in_plane] = row
        share(0, plane_rows, in_plane, plane_targets)
        settle()
        share_wait(0, plane_rows, plane_targets)
        row = jnp.sum(plane_rows[...], axis=0)
        row_out[1] = row
        line_rows[here[2]] = row
        share(1, line_rows, here[2], line_targets)
        share_wait(1, line_rows, line_targets)
        row = jnp.sum(line_rows[...], axis=0)
    row_lane = lax.broadcasted_iota(jnp.int32, (1, LANES), 1)
    gram = {}
    for n in range(MOMENTS):
        value = jnp.sum(jnp.where(row_lane == n, row, 0.0), axis=1, keepdims=True)
        gram[n // 2, (n + 1) // 2] = value
    for gap in range(2, ITERS + 1):
        for i in range(ITERS + 1 - gap):
            j = i + gap
            value = gram[i + 1, j - 1] - gram[i, j - 2]
            if i > 0:
                value = value + gram[i - 1, j - 1]
            gram[i, j] = value
    for i, j in list(gram):
        gram[j, i] = gram[i, j]

    def apply(p):
        q = [middle * a for a in p] + [jnp.zeros_like(half)]
        for i, a in enumerate(p):
            q[i + 1] = q[i + 1] + (0.5 * half) * a
            if i > 0:
                q[i - 1] = q[i - 1] + (0.5 * half) * a
        return q

    def product(p, q):
        value = None
        for i, a in enumerate(p):
            inner = None
            for j, b in enumerate(q):
                term = gram[i, j] * b
                inner = term if inner is None else inner + term
            inner = a * inner
            value = inner if value is None else value + inner
        return value

    left = [jnp.ones_like(half)]
    heading = list(left)
    moved = []
    norm = product(left, left)
    for step in range(ITERS):
        image = apply(heading)
        alpha = norm / product(heading, image)
        moved = [a + alpha * b for a, b in zip(moved, heading)] + [
            alpha * b for b in heading[len(moved) :]
        ]
        left = [a - alpha * b for a, b in zip(left, image)] + [
            -alpha * b for b in image[len(left) :]
        ]
        if step + 1 < ITERS:
            following = product(left, left)
            ratio = following / norm
            heading = [a + ratio * b for a, b in zip(left, heading)] + left[len(heading) :]
            norm = following

    for i in range(nx):
        warm = natural_own[ITERS + 1, i]
        end = jnp.zeros_like(warm)
        for k in range(ITERS + 1):
            value = natural_own[k, i]
            if k < ITERS:
                warm = warm + moved[k] * value
            end = end + left[k] * value
        both_out[0, i] = warm
        both_out[1, i] = end


def body(counts, warm, source, category, table, flags):
    nx, ny, nz = warm.shape
    depth = DEPTH
    plane, line = counts[0] * counts[1], counts[2]
    if nx < depth or nx % 2 or ny % SUB or nz != LANES or table.shape[0] > LANES:
        raise ValueError("block shape")
    if nx > 2 * depth or (FIELDS * depth + 1) * depth > LANES:
        raise ValueError("block shape")
    wide, tall, short, long = nx + 2 * depth, ny + 2 * SUB, ny + SUB, nz + LANES
    table = table[None]
    any_spec = pl.BlockSpec(memory_space=pl.ANY)
    vmem = pl.BlockSpec(memory_space=pltpu.VMEM)
    f32 = jnp.float32
    both = pl.pallas_call(
        functools.partial(kernel, counts),
        out_shape=pltpu.VMEM((2,) + warm.shape, jnp.float32),
        in_specs=[any_spec] * 5,
        out_specs=vmem,
        scratch_shapes=[
            pltpu.VMEM((2, wide, tall, nz), f32),
            pltpu.VMEM((2, wide, tall, nz), f32),
            pltpu.VMEM((wide, short, nz), f32),
            pltpu.VMEM((wide, short, nz), f32),
            pltpu.VMEM((wide, short, nz), f32),
            pltpu.VMEM((wide, short, nz), f32),
            pltpu.VMEM((ITERS + 1, wide, short, long), f32),
            pltpu.VMEM((wide, short, long), f32),
            pltpu.VMEM((wide, short, long), f32),
            pltpu.VMEM((3, wide, short, long), f32),
            pltpu.VMEM((3, short, long), f32),
            pltpu.VMEM((short, nz), f32),
            pltpu.VMEM((long, long), jnp.bfloat16),
            pltpu.VMEM((ITERS + 1, nx, short, nz), f32),
            pltpu.VMEM((ITERS + 2, nx, ny, nz), f32),
            pltpu.VMEM((SUB, LANES), f32),
            pltpu.VMEM(table.shape, f32),
            pltpu.VMEM((nx, ny, nz), f32),
            pltpu.VMEM((2, nx, ny, nz), jnp.int32),
            pltpu.VMEM((2, BOTH, ny, nz), f32),
            pltpu.VMEM((2, BOTH + 2, tall, nz), f32),
            pltpu.VMEM((16 * nx * ny, LANES), f32),
            pltpu.VMEM((4, 1, LANES), f32),
            pltpu.VMEM((plane, 1, LANES), f32),
            pltpu.VMEM((line, 1, LANES), f32),
            pltpu.VMEM((plane, 1, LANES), f32),
            pltpu.VMEM((line, 1, LANES), f32),
            pltpu.VMEM((plane * line, 1, LANES), f32),
            pltpu.SemaphoreType.DMA((2,)),
            pltpu.SemaphoreType.DMA((1,)),
            pltpu.SemaphoreType.DMA((3,)),
            pltpu.SemaphoreType.DMA((4,)),
            pltpu.SemaphoreType.DMA((4,)),
            pltpu.SemaphoreType.REGULAR,
            pltpu.SemaphoreType.REGULAR,
        ],
        compiler_params=pltpu.CompilerParams(collective_id=0, has_side_effects=True),
    )(warm, source, category, table, flags)
    return both[0], both[1]


def solution(mesh):
    counts = tuple(mesh.shape[a] for a in AXES)
    spec = P("gx", "gy", "gz")
    return jax.shard_map(
        functools.partial(body, counts),
        mesh=mesh,
        in_specs=(spec, spec, spec, P(), spec),
        out_specs=(spec, spec),
        check_vma=False,
    )
```
